128 devices in a mesh: grp: 4 (over z), dev: 32 (over y, x, core).
Axes of the slice: x: 4, y: 4, z: 4, core: 2. Of those that a mesh axis runs over, the one named last changes fastest.
Arguments:
- old_state: float32 [32768, 4, 512], P(('grp', 'dev')), may hold values from -6 to 6
- dest_row: int32 [32768], P(('grp', 'dev')), may hold values from -1 to 16383, as said below
- neighbours: int32 [6, 16384], P(None, ('grp', 'dev')), may hold values from 0 to 16383, as said below
- orientation: int32 [6, 16384], P(None, ('grp', 'dev')), may hold values from 0 to 7
- wall_flags: int32 [6, 16384], P(None, ('grp', 'dev')), may hold values from 0 to 1, as said below
- bulk_modulus: float32 [16384], P(('grp', 'dev')), may hold values from 0.5 to 2
- density: float32 [16384], P(('grp', 'dev')), may hold values from 0.5 to 2
Outputs:
- tendency: float32 [16384, 4, 512], P(('grp', 'dev'))
The draws below stay inside these ranges and needn't reach their ends.
Inputs may be any that keep to these rules, and one draw needn't show every extreme that they name: `dest_row`: each of the 16384 new rows appears exactly once. On half of the devices every slot is used, on the others every slot is -1. The slots of one device whose new rows lie on one device number either 0 or 8. The elements form a grid of 16 x 32 x 32 cubes along x, y, z, cut into blocks of 4 x 4 x 8, faces 0 to 5 looking to -x, +x, -y, +y, -z, +z; a face on the grid's outside has the row itself as neighbour. If neighbours[f, r] = m differs from r then neighbours[f xor 1, m] = r. Each device holds the rows of one whole block, in rows 128 * i to 128 * (i + 1) - 1 for device index i = g * 32 + d (g of grp, d of dev); which block lies on which device is arbitrary. One device's rows and faces have at most 32 neighbours on any one other device. wall_flags[f, r] is 1 exactly where neighbours[f, r] = r.
All inputs are finite; a program needn't handle non-finite values.
Results may differ from the reference program's by a relative error of at most 0.0001.
Values sent between devices are 32-bit elements; how exact they have to be, the bound alone decides.
A program may use at most 128 MiB of HBM per device.

```python
import math
import jax
import jax.numpy as jnp
import numpy as np
from jax import lax

NP = 8
BX = 4
BY = 4
BZ = 8
PZ = 4
PIECES = 16
NODES = 512
PX = 4
PY = 8
ELEM_DEV = 128
ELEMS = 16384
CAP = 8
OLD_CAP = 256
OLD_ALL = 32768


def grid_rows(key):
    device_count = PX * PY * PZ
    key_list = jax.random.split(jax.random.fold_in(key, 11), device_count)
    box_orders = jax.vmap(lambda sub_key: jax.random.permutation(sub_key, ELEM_DEV))(key_list)
    block_order = jax.random.permutation(jax.random.fold_in(key, 14), device_count)
    coord_x, coord_y, coord_z = jnp.meshgrid(jnp.arange(BX * PX), jnp.arange(BY * PY), jnp.arange(BZ * PZ), indexing='ij')
    block_id = coord_x // BX * (PY * PZ) + coord_y // BY * PZ + coord_z // BZ
    owner_dev = block_order[block_id]
    local_id = coord_x % BX * (BY * BZ) + coord_y % BY * BZ + coord_z % BZ
    row_grid = owner_dev * ELEM_DEV + box_orders[owner_dev, local_id]
    return row_grid.astype(jnp.int32)


def face_shift(row_grid, face_id):
    axis_id = face_id // 2
    extent = row_grid.shape[axis_id]
    position = lax.broadcasted_iota(jnp.int32, row_grid.shape, axis_id)
    if face_id % 2 == 0:
        first_slab = lax.slice_in_dim(row_grid, 0, 1, axis=axis_id)
        rest_slab = lax.slice_in_dim(row_grid, 0, extent - 1, axis=axis_id)
        shifted = jnp.concatenate([first_slab, rest_slab], axis=axis_id)
        at_edge = position == 0
    else:
        rest_slab = lax.slice_in_dim(row_grid, 1, extent, axis=axis_id)
        first_slab = lax.slice_in_dim(row_grid, extent - 1, extent, axis=axis_id)
        shifted = jnp.concatenate([rest_slab, first_slab], axis=axis_id)
        at_edge = position == extent - 1
    return (shifted, at_edge)


def draw_neighbours(key, part):
    row_grid = grid_rows(key)
    result = jnp.zeros((6, ELEM_DEV * PX * PY * PZ), jnp.int32)
    for face_id in range(6):
        shifted, at_edge = face_shift(row_grid, face_id)
        result = result.at[face_id, row_grid.reshape(-1)].set(shifted.reshape(-1))
    return result


def draw_wall_flags(key, part):
    row_grid = grid_rows(key)
    result = jnp.zeros((6, ELEM_DEV * PX * PY * PZ), jnp.int32)
    for face_id in range(6):
        shifted, at_edge = face_shift(row_grid, face_id)
        result = result.at[face_id, row_grid.reshape(-1)].set(at_edge.reshape(-1).astype(jnp.int32))
    return result


def draw_dest_row(key, part):
    device_count = PX * PY * PZ
    source_order = jax.random.permutation(jax.random.fold_in(key, 12), device_count)
    heavy_src = source_order[:device_count // 2]
    run_length = 2 * PIECES
    piece_ids = jnp.arange(device_count * PIECES)
    sources = jnp.repeat(heavy_src, run_length, total_repeat_length=device_count * PIECES)
    target_dev = piece_ids % device_count
    piece_number = piece_ids // device_count
    within = piece_ids % run_length
    slot_keys = jax.random.split(jax.random.fold_in(key, 13), device_count)
    slot_orders = jax.vmap(lambda sub_key: jax.random.permutation(sub_key, OLD_CAP))(slot_keys)
    offsets = jnp.arange(CAP)
    new_rows = target_dev[:, None] * ELEM_DEV + piece_number[:, None] * CAP + offsets[None, :]
    old_rows = sources[:, None] * OLD_CAP + slot_orders[sources[:, None], within[:, None] * CAP + offsets[None, :]]
    empty_rows = jnp.full((device_count * OLD_CAP,), -1, jnp.int32)
    return empty_rows.at[old_rows.reshape(-1)].set(new_rows.reshape(-1).astype(jnp.int32))


def with_ends(array, key, least, top_value):
    longest = array.shape.index(max(array.shape))
    spots = []
    for shift in (0, 1):
        where = [jax.random.randint(jax.random.fold_in(key, axis), (), 0, length) for axis, length in enumerate(array.shape)]
        where[longest] = (where[longest] + shift) % array.shape[longest]
        spots.append(tuple(where))
    return array.at[spots[0]].set(least).at[spots[1]].set(top_value)


def levels(key, shape, cuts, smallest, largest):
    def one(axis_at, blocks):
        heights = jax.random.uniform(jax.random.fold_in(jax.random.fold_in(key, 6), axis_at), (blocks,), jnp.float32, smallest / len(cuts), largest / len(cuts))
        return jnp.repeat(jnp.exp(heights), shape[axis_at] // blocks).reshape((-1,) + (1,) * (len(shape) - axis_at - 1))

    level = one(*cuts[0])
    for cut in cuts[1:]:
        level = level * one(*cut)
    return level


def centred(rng, shape, spread, most, shards=(), kind=jnp.bfloat16):
    values = spread * jax.random.normal(rng, shape, jnp.float32)
    if shards:
        values = values * levels(rng, shape, shards, -0.22, 0.18)
    return jnp.clip(values, -most, most).astype(kind)


def setup_inputs(seed: int = 0) -> dict:
    splits = jax.random.split(jax.random.key(seed), 8)
    old_state = centred(splits[0], (OLD_ALL, 4, NODES), 1.0, 6.0, ((0, 128),), jnp.float32)
    dest_row = draw_dest_row(jax.random.fold_in(splits[7], 71), 0)
    neighbours = draw_neighbours(jax.random.fold_in(splits[7], 71), 0)
    orientation = with_ends(jax.random.randint(splits[3], (6, ELEMS), 0, 8), jax.random.fold_in(splits[3], 1), 0, 7).astype(jnp.int32)
    wall_flags = draw_wall_flags(jax.random.fold_in(splits[7], 71), 0)
    bulk_modulus = jnp.clip(jnp.exp(math.log(2.0) - 1.3862944 * jax.random.uniform(splits[5], (ELEMS,), jnp.float32) ** levels(splits[5], (ELEMS,), ((0, 128),), -0.2, 0.2)), 0.5, 2.0)
    density = jnp.clip(jnp.exp(math.log(2.0) - 1.3862944 * jax.random.uniform(splits[6], (ELEMS,), jnp.float32) ** levels(splits[6], (ELEMS,), ((0, 128),), -0.2, 0.2)), 0.5, 2.0)
    return {"old_state": old_state, "dest_row": dest_row, "neighbours": neighbours, "orientation": orientation, "wall_flags": wall_flags, "bulk_modulus": bulk_modulus, "density": density}


metric_scale = 0.25

def gll_tables(poly_order):
    num_points = poly_order + 1
    points = -np.cos(np.pi * np.arange(num_points) / poly_order)
    legendre = np.zeros((num_points, num_points))
    for sweeps in range(101):
        legendre[:, 0] = 1.0
        legendre[:, 1] = points
        for degree in range(2, num_points):
            legendre[:, degree] = ((2 * degree - 1) * points * legendre[:, degree - 1] - (degree - 1) * legendre[:, degree - 2]) / degree
        if sweeps < 100:
            points = points - (points * legendre[:, poly_order] - legendre[:, poly_order - 1]) / (num_points * legendre[:, poly_order])
    end_values = legendre[:, poly_order]
    weights = 2.0 / (poly_order * num_points * end_values ** 2)
    distance = points[:, None] - points[None, :] + np.eye(num_points)
    derivative = end_values[:, None] / end_values[None, :] / distance
    derivative = derivative * (1.0 - np.eye(num_points))
    derivative[0, 0] = -poly_order * num_points / 4.0
    derivative[poly_order, poly_order] = poly_order * num_points / 4.0
    return (points, weights, derivative)

def face_index(face_id):
    picked = [slice(None), slice(None), slice(None)]
    picked[face_id // 2] = 0 if face_id % 2 == 0 else NP - 1
    return tuple(picked)

def face_traces(volume):
    return jnp.stack([volume[(slice(None), slice(None)) + face_index(face_id)] for face_id in range(6)])

def orient_trace(values, orient_code):
    shaped = orient_code[:, None, None, None]
    values = jnp.where(shaped % 2 == 1, values[:, :, ::-1, :], values)
    values = jnp.where(shaped // 2 % 2 == 1, values[:, :, :, ::-1], values)
    return jnp.where(shaped >= 4, jnp.swapaxes(values, 2, 3), values)

def derivative_along(scalar_field, matrix, axis_id):
    einsum_forms = ['ai,eijk->eajk', 'aj,eijk->eiak', 'ak,eijk->eija']
    return jnp.einsum(einsum_forms[axis_id], matrix, scalar_field, precision=lax.Precision.HIGHEST)

def right_side(volume, inner_faces, outer_faces, outer_impedance, orientation, wall_flags, bulk_modulus, density):
    points, weights, derivative = gll_tables(NP - 1)
    matrix = jnp.asarray(derivative, jnp.float32)
    lift_factor = metric_scale / float(weights[0])
    bulk_vol = bulk_modulus[:, None, None, None]
    dens_vol = density[:, None, None, None]
    divergence = derivative_along(volume[:, 1], matrix, 0) + derivative_along(volume[:, 2], matrix, 1) + derivative_along(volume[:, 3], matrix, 2)
    pieces_list = [-metric_scale * bulk_vol * divergence]
    for axis_id in range(3):
        pieces_list.append(-(metric_scale / dens_vol) * derivative_along(volume[:, 0], matrix, axis_id))
    result = jnp.stack(pieces_list, axis=1)
    inner_impedance = jnp.sqrt(bulk_modulus * density)
    for face_id in range(6):
        axis_id = face_id // 2
        normal_sign = 2.0 * (face_id % 2) - 1.0
        own_face = inner_faces[face_id]
        far_face = orient_trace(outer_faces[face_id], orientation[face_id])
        is_wall = wall_flags[face_id] == 1
        wall_face = is_wall[:, None, None]
        press_in = own_face[:, 0]
        normal_in = normal_sign * own_face[:, 1 + axis_id]
        press_out = jnp.where(wall_face, press_in, far_face[:, 0])
        normal_out = jnp.where(wall_face, -normal_in, normal_sign * far_face[:, 1 + axis_id])
        imped_in = inner_impedance[:, None, None]
        imped_out = jnp.where(is_wall, inner_impedance, outer_impedance[face_id])[:, None, None]
        imped_sum = imped_in + imped_out
        press_star = (imped_out * press_in + imped_in * press_out + imped_in * imped_out * (normal_in - normal_out)) / imped_sum
        normal_star = (imped_in * normal_in + imped_out * normal_out + press_in - press_out) / imped_sum
        result = result.at[(slice(None), 0) + face_index(face_id)].add(-lift_factor * bulk_modulus[:, None, None] * (normal_star - normal_in))
        result = result.at[(slice(None), 1 + axis_id) + face_index(face_id)].add(-(normal_sign * lift_factor) * (press_star - press_in) / density[:, None, None])
    return result.reshape(result.shape[0], 4, -1)

def reference(old_state, dest_row, neighbours, orientation, wall_flags, bulk_modulus, density):
    elem_count = bulk_modulus.shape[0]
    target = jnp.where(dest_row >= 0, dest_row, elem_count)
    new_state = jnp.zeros((elem_count, 4, old_state.shape[2]), jnp.float32).at[target].set(old_state, mode='drop')
    volume = new_state.reshape(elem_count, 4, NP, NP, NP)
    inner_faces = face_traces(volume)
    outer_faces = jnp.stack([inner_faces[face_id ^ 1][neighbours[face_id]] for face_id in range(6)])
    impedance = jnp.sqrt(bulk_modulus * density)
    outer_impedance = impedance[neighbours]
    return right_side(volume, inner_faces, outer_faces, outer_impedance, orientation, wall_flags, bulk_modulus, density)
```

```python
import functools

import jax
import jax.numpy as jnp
import numpy as np
from jax import lax
from jax.experimental import pallas as pl
from jax.experimental.pallas import tpu as pltpu
from jax.sharding import PartitionSpec as P

NP = 8
HCAP = 32
MESH = pl.DeviceIdType.MESH
HIGHEST = lax.Precision.HIGHEST

metric_scale = 0.25


def gll_tables(poly_order):
    num_points = poly_order + 1
    points = -np.cos(np.pi * np.arange(num_points) / poly_order)
    legendre = np.zeros((num_points, num_points))
    for sweeps in range(101):
        legendre[:, 0] = 1.0
        legendre[:, 1] = points
        for degree in range(2, num_points):
            legendre[:, degree] = (
                (2 * degree - 1) * points * legendre[:, degree - 1]
                - (degree - 1) * legendre[:, degree - 2]
            ) / degree
        if sweeps < 100:
            points = points - (points * legendre[:, poly_order] - legendre[:, poly_order - 1]) / (
                num_points * legendre[:, poly_order]
            )
    end_values = legendre[:, poly_order]
    weights = 2.0 / (poly_order * num_points * end_values**2)
    distance = points[:, None] - points[None, :] + np.eye(num_points)
    derivative = end_values[:, None] / end_values[None, :] / distance
    derivative = derivative * (1.0 - np.eye(num_points))
    derivative[0, 0] = -poly_order * num_points / 4.0
    derivative[poly_order, poly_order] = poly_order * num_points / 4.0
    return (points, weights, derivative)


def face_index(face_id):
    picked = [slice(None), slice(None), slice(None)]
    picked[face_id // 2] = 0 if face_id % 2 == 0 else NP - 1
    return tuple(picked)


def face_traces(volume):
    return jnp.stack(
        [volume[(slice(None), slice(None)) + face_index(face_id)] for face_id in range(6)]
    )


def orient_trace(values, orient_code):
    shaped = orient_code[:, None, None, None]
    values = jnp.where(shaped % 2 == 1, values[:, :, ::-1, :], values)
    values = jnp.where(shaped // 2 % 2 == 1, values[:, :, :, ::-1], values)
    return jnp.where(shaped >= 4, jnp.swapaxes(values, 2, 3), values)


def derivative_along(scalar_field, matrix, axis_id):
    einsum_forms = ["ai,eijk->eajk", "aj,eijk->eiak", "ak,eijk->eija"]
    return jnp.einsum(einsum_forms[axis_id], matrix, scalar_field, precision=lax.Precision.HIGHEST)


def right_side(
    volume,
    inner_faces,
    outer_faces,
    outer_impedance,
    orientation,
    wall_flags,
    bulk_modulus,
    density,
):
    points, weights, derivative = gll_tables(NP - 1)
    matrix = jnp.asarray(derivative, jnp.float32)
    lift_factor = metric_scale / float(weights[0])
    bulk_vol = bulk_modulus[:, None, None, None]
    dens_vol = density[:, None, None, None]
    divergence = (
        derivative_along(volume[:, 1], matrix, 0)
        + derivative_along(volume[:, 2], matrix, 1)
        + derivative_along(volume[:, 3], matrix, 2)
    )
    pieces_list = [-metric_scale * bulk_vol * divergence]
    for axis_id in range(3):
        pieces_list.append(
            -(metric_scale / dens_vol) * derivative_along(volume[:, 0], matrix, axis_id)
        )
    result = jnp.stack(pieces_list, axis=1)
    inner_impedance = jnp.sqrt(bulk_modulus * density)
    for face_id in range(6):
        axis_id = face_id // 2
        normal_sign = 2.0 * (face_id % 2) - 1.0
        own_face = inner_faces[face_id]
        far_face = orient_trace(outer_faces[face_id], orientation[face_id])
        is_wall = wall_flags[face_id] == 1
        wall_face = is_wall[:, None, None]
        press_in = own_face[:, 0]
        normal_in = normal_sign * own_face[:, 1 + axis_id]
        press_out = jnp.where(wall_face, press_in, far_face[:, 0])
        normal_out = jnp.where(wall_face, -normal_in, normal_sign * far_face[:, 1 + axis_id])
        imped_in = inner_impedance[:, None, None]
        imped_out = jnp.where(is_wall, inner_impedance, outer_impedance[face_id])[:, None, None]
        imped_sum = imped_in + imped_out
        press_star = (
            imped_out * press_in
            + imped_in * press_out
            + imped_in * imped_out * (normal_in - normal_out)
        ) / imped_sum
        normal_star = (
            imped_in * normal_in + imped_out * normal_out + press_in - press_out
        ) / imped_sum
        result = result.at[(slice(None), 0) + face_index(face_id)].add(
            -lift_factor * bulk_modulus[:, None, None] * (normal_star - normal_in)
        )
        result = result.at[(slice(None), 1 + axis_id) + face_index(face_id)].add(
            -(normal_sign * lift_factor) * (press_star - press_in) / density[:, None, None]
        )
    return result.reshape(result.shape[0], 4, -1)


def my_place():
    group = lax.axis_index("grp")
    member = lax.axis_index("dev")
    return group, member // 8, (member // 2) % 4, member % 2


def chip_at(place, step):
    z_at, y_at, x_at, _ = place
    x_to = (x_at + step) % 4
    y_to = (y_at + step // 4 + step) % 4
    z_to = (z_at + step // 16 + step // 4 + step) % 4
    return z_to, y_to * 4 + x_to


def permute_kernel(place_ref, state_ref, send_ref, sem):
    def one(slot, carry):
        at = place_ref[slot]
        pltpu.make_async_copy(
            state_ref.at[slot], send_ref.at[pl.ds((at % 8) * 16, 16), at // 8], sem
        ).start()
        return carry

    lax.fori_loop(0, 256, one, 0, unroll=8)
    pltpu.make_async_copy(state_ref, state_ref, sem).wait()


def exchange_kernel(
    note_ref, send_ref, out_ref, notes, first, second, third, table, index, perm, sems
):
    place = my_place()
    mine = place[0] * 32 + lax.axis_index("dev")
    core = place[3]
    barrier = pltpu.get_barrier_semaphore()

    def other(step):
        group, chip = chip_at(place, step // 2)
        member = chip * 2 + (core + step) % 2
        return group, member

    def greet(step, carry):
        group, member = other(step)
        pl.semaphore_signal(barrier, inc=1, device_id=(group, member), device_id_type=MESH)
        return carry

    lax.fori_loop(1, 128, greet, 0)
    pl.semaphore_wait(barrier, 127)

    def copy(source, target, phase, group, member):
        pltpu.make_async_remote_copy(
            src_ref=source,
            dst_ref=target,
            send_sem=sems.at[2 * phase],
            recv_sem=sems.at[2 * phase + 1],
            device_id=(group, member),
            device_id_type=MESH,
        ).start()

    def finish(buffer, rows, which):
        view = buffer.at[pl.ds(0, rows)]
        pltpu.make_async_copy(view, view, sems.at[which]).wait()

    def tell(step, carry):
        group, member = other(step)
        copy(note_ref.at[pl.ds(group * 32 + member, 1)], notes.at[pl.ds(mine, 1)], 0, group, member)
        return carry

    lax.fori_loop(1, 128, tell, 0)

    def spread(group, member):
        copy(send_ref.at[group * 32 + member], first.at[pl.ds(mine * 32, 32)], 1, group, member)

    spread(place[0], lax.axis_index("dev") + 1 - 2 * core)
    for side in range(2):

        def spread_step(step, carry):
            group, chip = chip_at(place, step)
            spread(group, chip * 2 + side)
            return carry

        lax.fori_loop(1, 64, spread_step, 0)
    notes[pl.ds(mine, 1)] = note_ref[pl.ds(mine, 1)]
    first[pl.ds(mine * 32, 32)] = send_ref[mine]

    finish(notes, 127, 1)
    note = notes.reshape(128, 128)[...]
    lane = lax.broadcasted_iota(jnp.int32, (128, 128), 1)
    sub = lax.broadcasted_iota(jnp.int32, (128, 128), 0)
    lower = (lane < sub).astype(jnp.float32)
    piece = jnp.zeros((128, 128), jnp.int32)
    for k in range(32):
        piece = piece + jnp.where(note[:, 32 + k : 33 + k] == lane, k + 1, 0)
    valid = piece > 0
    rank = jnp.dot(lower, valid.astype(jnp.float32), preferred_element_type=jnp.float32)
    rank = rank.astype(jnp.int32)
    entry = sub * 32 + piece - 1
    for j in range(16):
        table[j : j + 1, :] = jnp.sum(
            jnp.where(valid & (rank == j), entry, 0), axis=0, keepdims=True
        )
    to_scalar = pltpu.make_async_copy(table, index, sems.at[8])
    to_scalar.start()
    has = jnp.broadcast_to(note[:, 0:1] > 0, (128, 128))
    order = jnp.dot(lower, has.astype(jnp.float32), preferred_element_type=jnp.float32)
    slot = jnp.where(has & (order.astype(jnp.int32) == lane), 1.0, 0.0)[:, :16]
    rows = []
    for i in range(8):
        is_row = (note[:, i : i + 1] - 1 == lane).astype(jnp.float32)
        rows.append(
            lax.dot_general(
                slot, is_row, (((0,), (0,)), ((), ())), preferred_element_type=jnp.float32
            )
        )
    perm[...] = jnp.concatenate(rows, axis=0).T
    to_scalar.wait()

    finish(first, 127 * 32, 3)

    def pick(target, base, at):
        for j in range(16):
            target[pl.ds(base + j, 1)] = first[pl.ds(index[j, at], 1)]

    pick(third, mine * 16, mine)

    def forward(step):
        group, member = other(step)
        at = group * 32 + member
        copy(
            second.at[pl.ds(at * 16, 16)], third.at[pl.ds(mine * 16, 16)], 2, group, member
        )

    def pick_step(step, carry):
        group, member = other(step)
        at = group * 32 + member
        pick(second, at * 16, at)

        @pl.when(step > 1)
        def _():
            forward(step - 1)

        return carry

    lax.fori_loop(1, 128, pick_step, 0)
    forward(127)
    finish(third, 127 * 16, 5)

    arrived = third.reshape(8, 16, 16, 128)
    for part in range(16):
        block = arrived[:, part].reshape(128, 128)
        out_ref[pl.ds(part, 128, stride=16), :] = jnp.dot(
            perm[...], block, precision=HIGHEST, preferred_element_type=jnp.float32
        )
    finish(notes, 127, 0)
    finish(first, 127 * 32, 2)
    finish(third, 127 * 16, 4)


def move_state(old_state, dest_row):
    below = dest_row[None, :] < dest_row[:, None]
    tie = (dest_row[None, :] == dest_row[:, None]) & (
        jnp.arange(256)[None, :] < jnp.arange(256)[:, None]
    )
    position = jnp.sum((below | tie).astype(jnp.int32), axis=1)
    ordered = jnp.sum(
        jnp.where(position[:, None] == jnp.arange(256)[None, :], dest_row[:, None], 0), axis=0
    )
    pieces = ordered.reshape(32, 8)
    targets = pieces[:, 0] // 128
    row_ids = jnp.sum(
        jnp.where(
            targets[None, :, None] == jnp.arange(128)[:, None, None], pieces[None] % 128 + 1, 0
        ),
        axis=1,
    )
    note = jnp.concatenate(
        [
            row_ids,
            jnp.zeros((128, 24), jnp.int32),
            jnp.broadcast_to(targets[None, :], (128, 32)),
            jnp.zeros((128, 64), jnp.int32),
        ],
        axis=1,
    )[:, None, :]
    view = old_state.reshape(256, 4, 4, 128).transpose(0, 2, 1, 3).reshape(256, 16, 1, 128)
    whole = pl.BlockSpec(memory_space=pltpu.VMEM)
    sends = pl.pallas_call(
        permute_kernel,
        out_shape=jax.ShapeDtypeStruct((128, 32, 1, 128), jnp.float32),
        in_specs=[pl.BlockSpec(memory_space=pltpu.SMEM), pl.BlockSpec(memory_space=pl.ANY)],
        out_specs=whole,
        scratch_shapes=[pltpu.SemaphoreType.DMA],
    )(position, view)
    moved = pl.pallas_call(
        exchange_kernel,
        out_shape=jax.ShapeDtypeStruct((2048, 128), jnp.float32),
        in_specs=[whole, whole],
        out_specs=whole,
        scratch_shapes=[
            pltpu.VMEM((128, 1, 128), jnp.int32),
            pltpu.VMEM((4096, 1, 128), jnp.float32),
            pltpu.VMEM((2048, 1, 128), jnp.float32),
            pltpu.VMEM((2048, 1, 128), jnp.float32),
            pltpu.VMEM((16, 128), jnp.int32),
            pltpu.SMEM((16, 128), jnp.int32),
            pltpu.VMEM((128, 128), jnp.float32),
            pltpu.SemaphoreType.DMA((9,)),
        ],
        compiler_params=pltpu.CompilerParams(collective_id=0, has_side_effects=True),
    )(note, sends)
    return moved.reshape(128, 4, 4, 128).transpose(0, 2, 1, 3).reshape(128, 4, 512)


def body(old_state, dest_row, neighbours, orientation, wall_flags, bulk_modulus, density):
    elem_dev = bulk_modulus.shape[0]
    members = lax.axis_size("dev")
    devices = 128
    new_state = move_state(old_state, dest_row)
    volume = new_state.reshape(elem_dev, 4, NP, NP, NP)
    inner_faces = face_traces(volume)
    flat_inner = inner_faces.reshape(6, elem_dev, 4 * NP * NP)
    face_width = flat_inner.shape[2]
    impedance = jnp.sqrt(bulk_modulus * density)
    my_index = lax.axis_index("grp") * members + lax.axis_index("dev")
    owner_dev = neighbours // elem_dev
    local_row = neighbours - owner_dev * elem_dev
    remote = (owner_dev != my_index) & (wall_flags == 0)
    near_row = jnp.where(remote, 0, local_row)
    outer_faces = jnp.stack([flat_inner[face_id ^ 1][near_row[face_id]] for face_id in range(6)])
    outer_impedance = impedance[near_row]
    slot_count = HCAP
    remote_flat = remote.reshape(-1)
    owner_flat = owner_dev.reshape(-1)
    match_owner = (
        (owner_flat[:, None] == jnp.arange(devices)[None, :]) & remote_flat[:, None]
    ).astype(jnp.int32)
    owner_before = jnp.cumsum(match_owner, axis=0) - match_owner
    owner_rank = jnp.sum(owner_before * match_owner, axis=1)
    ask_slot = jnp.where(remote_flat, owner_flat * slot_count + owner_rank, devices * slot_count)
    ask_value = ((jnp.arange(6) ^ 1)[:, None] * elem_dev + local_row).reshape(-1) + 1
    requests_out = (
        jnp.zeros((devices * slot_count,), jnp.int32).at[ask_slot].set(ask_value, mode="drop")
    )
    trace_table = flat_inner.reshape(6 * elem_dev, face_width)
    incoming = lax.all_to_all(requests_out, ("grp", "dev"), split_axis=0, concat_axis=0, tiled=True)
    serve_at = jnp.maximum(incoming - 1, 0)
    asked = (incoming > 0).astype(jnp.float32)
    answer = trace_table[serve_at] * asked[:, None]
    answer_imped = impedance[serve_at % elem_dev] * asked
    back_trace, back_imped = (
        lax.all_to_all(answer, ("grp", "dev"), split_axis=0, concat_axis=0, tiled=True),
        lax.all_to_all(answer_imped, ("grp", "dev"), split_axis=0, concat_axis=0, tiled=True),
    )
    take_at = jnp.minimum(ask_slot, devices * slot_count - 1)
    outer_faces = jnp.where(
        remote[:, :, None], back_trace[take_at].reshape(6, elem_dev, face_width), outer_faces
    )
    outer_impedance = jnp.where(remote, back_imped[take_at].reshape(6, elem_dev), outer_impedance)
    outer_shaped = outer_faces.reshape(6, elem_dev, 4, NP, NP)
    return right_side(
        volume,
        inner_faces,
        outer_shaped,
        outer_impedance,
        orientation,
        wall_flags,
        bulk_modulus,
        density,
    )


def solution(mesh):
    in_specs = (
        P(("grp", "dev"), None, None),
        P(("grp", "dev")),
        P(None, ("grp", "dev")),
        P(None, ("grp", "dev")),
        P(None, ("grp", "dev")),
        P(("grp", "dev")),
        P(("grp", "dev")),
    )
    out_specs = P(("grp", "dev"), None, None)
    return jax.shard_map(body, mesh=mesh, in_specs=in_specs, out_specs=out_specs, check_vma=False)
```

```python
import functools

import jax
import jax.numpy as jnp
import numpy as np
from jax import lax
from jax.experimental import pallas as pl
from jax.experimental.pallas import tpu as pltpu
from jax.sharding import PartitionSpec as P

NP = 8
HCAP = 32
MESH = pl.DeviceIdType.MESH
HIGHEST = lax.Precision.HIGHEST

metric_scale = 0.25


def gll_tables(poly_order):
    num_points = poly_order + 1
    points = -np.cos(np.pi * np.arange(num_points) / poly_order)
    legendre = np.zeros((num_points, num_points))
    for sweeps in range(101):
        legendre[:, 0] = 1.0
        legendre[:, 1] = points
        for degree in range(2, num_points):
            legendre[:, degree] = (
                (2 * degree - 1) * points * legendre[:, degree - 1]
                - (degree - 1) * legendre[:, degree - 2]
            ) / degree
        if sweeps < 100:
            points = points - (points * legendre[:, poly_order] - legendre[:, poly_order - 1]) / (
                num_points * legendre[:, poly_order]
            )
    end_values = legendre[:, poly_order]
    weights = 2.0 / (poly_order * num_points * end_values**2)
    distance = points[:, None] - points[None, :] + np.eye(num_points)
    derivative = end_values[:, None] / end_values[None, :] / distance
    derivative = derivative * (1.0 - np.eye(num_points))
    derivative[0, 0] = -poly_order * num_points / 4.0
    derivative[poly_order, poly_order] = poly_order * num_points / 4.0
    return (points, weights, derivative)


def fixed_tables():
    derivative = gll_tables(NP - 1)[2]
    take = np.zeros((2, 4, 128, 128))
    for end in range(2):
        for first in range(8):
            for second in range(8):
                face_lane = 64 * end + 8 * first + second
                half, chunk = 64 * (first % 2), first // 2
                take[0, chunk, half + 56 * end + second, face_lane] = 1.0
                take[1, chunk, half + 8 * second + 7 * end, face_lane] = 1.0
    turns = np.zeros((3, 128, 128))
    for end in range(2):
        for first in range(8):
            for second in range(8):
                to = 64 * end + 8 * first + second
                turns[0, 64 * end + 8 * (7 - first) + second, to] = 1.0
                turns[1, 64 * end + 8 * first + 7 - second, to] = 1.0
                turns[2, 64 * end + 8 * second + first, to] = 1.0
    eye2, eye8 = np.eye(2), np.eye(8)
    inside = [
        np.kron(eye2, np.kron(derivative.T, eye8)),
        np.kron(eye2, np.kron(eye8, derivative.T)),
    ]
    lift = np.swapaxes(take, 2, 3)
    stack = [take.reshape(8, 128, 128), lift.reshape(8, 128, 128), turns, np.stack(inside)]
    return np.concatenate(stack).astype(np.float32)


TAKE, LIFT, TURN, INSIDE, TABLES = 0, 8, 16, 19, 21
NEAR, FAR, GIVE, CODE, WALL, Z_IN, BULK, THIN, KEPT = 0, 6, 12, 18, 21, 24, 25, 26, 27

def my_place():
    group = lax.axis_index("grp")
    member = lax.axis_index("dev")
    return group, member // 8, (member // 2) % 4, member % 2


def chip_at(place, step):
    z_at, y_at, x_at, _ = place
    x_to = (x_at + step) % 4
    y_to = (y_at + step // 4 + step) % 4
    z_to = (z_at + step // 16 + step // 4 + step) % 4
    return z_to, y_to * 4 + x_to


def permute_kernel(place_ref, state_ref, send_ref, sem):
    def one(slot, carry):
        at = place_ref[slot]
        pltpu.make_async_copy(
            state_ref.at[slot], send_ref.at[pl.ds((at % 8) * 16, 16), at // 8], sem
        ).start()
        return carry

    lax.fori_loop(0, 256, one, 0, unroll=8)
    pltpu.make_async_copy(state_ref, state_ref, sem).wait()


def exact(left, right):
    return jnp.dot(left, right, precision=HIGHEST, preferred_element_type=jnp.float32)


def prepare(mine, near_ref, turn_ref, wall_ref, bulk_ref, dens_ref, stack, kept, lane, sub):
    near_rows = near_ref[...]
    wall_rows = wall_ref[...]
    away_rows = jnp.where((near_rows // 128 != mine) & (wall_rows == 0), 1.0, 0.0)
    stack[...] = jnp.zeros((128, 128), jnp.float32)
    stack[0:6, :] = near_rows.astype(jnp.float32)
    stack[8:14, :] = turn_ref[...].astype(jnp.float32)
    stack[16:22, :] = wall_rows.astype(jnp.float32)
    stack[24:25, :] = bulk_ref[...]
    stack[25:26, :] = dens_ref[...]
    stack[26:32, :] = away_rows
    columns = stack[...].T
    away_all = stack[...]
    upper = (sub < lane).astype(jnp.float32)
    give_rank = jnp.dot(away_all, upper, preferred_element_type=jnp.float32)
    base = (mine * 128).astype(jnp.float32)
    lane_f = lane.astype(jnp.float32)
    sub_f = sub.astype(jnp.float32)
    for face in range(6):
        near = columns[:, face : face + 1]
        away = columns[:, 26 + face : 27 + face]
        away_row = away_rows[face : face + 1, :]
        kept[NEAR + face] = jnp.where((near - base == lane_f) & (away == 0.0), 1.0, 0.0)
        before = jnp.where((near_rows[face : face + 1, :].astype(jnp.float32) < near), away_row, 0.0)
        take_rank = jnp.sum(before, axis=1, keepdims=True)
        kept[FAR + face] = jnp.where((take_rank == lane_f) & (away > 0.0), 1.0, 0.0)
        row_rank = give_rank[26 + face : 27 + face, :]
        kept[GIVE + face] = jnp.where((row_rank == sub_f) & (away_row > 0.0), 1.0, 0.0)
    low = lane < 64
    for axis in range(3):
        kept[CODE + axis] = jnp.where(
            low, columns[:, 8 + 2 * axis : 9 + 2 * axis], columns[:, 9 + 2 * axis : 10 + 2 * axis]
        )
        kept[WALL + axis] = jnp.where(
            low, columns[:, 16 + 2 * axis : 17 + 2 * axis], columns[:, 17 + 2 * axis : 18 + 2 * axis]
        )
    bulk = jnp.broadcast_to(columns[:, 24:25], (128, 128))
    dens = jnp.broadcast_to(columns[:, 25:26], (128, 128))
    kept[Z_IN] = jnp.sqrt(bulk * dens)
    kept[BULK] = bulk
    kept[THIN] = 1.0 / dens


def exchange_kernel(
    note_ref,
    send_ref,
    near_ref,
    turn_ref,
    wall_ref,
    bulk_ref,
    dens_ref,
    fixed_ref,
    out_ref,
    notes,
    first,
    second,
    third,
    table,
    index,
    perm,
    fixed,
    stack,
    facing,
    kept,
    field,
    traces,
    ask,
    ask_in,
    answer,
    answer_in,
    total,
    sems,
):
    load_fixed = pltpu.make_async_copy(fixed_ref, fixed, sems.at[14])
    load_fixed.start()
    place = my_place()
    mine = place[0] * 32 + lax.axis_index("dev")
    core = place[3]
    barrier = pltpu.get_barrier_semaphore()

    def other(step):
        group, chip = chip_at(place, step // 2)
        member = chip * 2 + (core + step) % 2
        return group, member

    def greet(step, carry):
        group, member = other(step)
        pl.semaphore_signal(barrier, inc=1, device_id=(group, member), device_id_type=MESH)
        return carry

    lax.fori_loop(1, 128, greet, 0)
    pl.semaphore_wait(barrier, 127)

    def copy(source, target, phase, group, member):
        pltpu.make_async_remote_copy(
            src_ref=source,
            dst_ref=target,
            send_sem=sems.at[2 * phase],
            recv_sem=sems.at[2 * phase + 1],
            device_id=(group, member),
            device_id_type=MESH,
        ).start()

    def finish(buffer, rows, which):
        view = buffer.at[pl.ds(0, rows)]
        pltpu.make_async_copy(view, view, sems.at[which]).wait()

    def tell(step, carry):
        group, member = other(step)
        copy(note_ref.at[pl.ds(group * 32 + member, 1)], notes.at[pl.ds(mine, 1)], 0, group, member)
        return carry

    lax.fori_loop(1, 128, tell, 0)

    def spread(group, member):
        copy(send_ref.at[group * 32 + member], first.at[pl.ds(mine * 32, 32)], 1, group, member)

    spread(place[0], lax.axis_index("dev") + 1 - 2 * core)
    for side in range(2):

        def spread_step(step, carry):
            group, chip = chip_at(place, step)
            spread(group, chip * 2 + side)
            return carry

        lax.fori_loop(1, 64, spread_step, 0)
    notes[pl.ds(mine, 1)] = note_ref[pl.ds(mine, 1)]
    first[pl.ds(mine * 32, 32)] = send_ref[mine]

    finish(notes, 127, 1)
    note = notes.reshape(128, 128)[...]
    lane = lax.broadcasted_iota(jnp.int32, (128, 128), 1)
    sub = lax.broadcasted_iota(jnp.int32, (128, 128), 0)
    lower = (lane < sub).astype(jnp.float32)
    piece = jnp.zeros((128, 128), jnp.int32)
    for k in range(32):
        piece = piece + jnp.where(note[:, 32 + k : 33 + k] == lane, k + 1, 0)
    valid = piece > 0
    rank = jnp.dot(lower, valid.astype(jnp.float32), preferred_element_type=jnp.float32)
    rank = rank.astype(jnp.int32)
    entry = sub * 32 + piece - 1
    for j in range(16):
        table[j : j + 1, :] = jnp.sum(
            jnp.where(valid & (rank == j), entry, 0), axis=0, keepdims=True
        )
    to_scalar = pltpu.make_async_copy(table, index, sems.at[8])
    to_scalar.start()
    has = jnp.broadcast_to(note[:, 0:1] > 0, (128, 128))
    order = jnp.dot(lower, has.astype(jnp.float32), preferred_element_type=jnp.float32)
    slot = jnp.where(has & (order.astype(jnp.int32) == lane), 1.0, 0.0)[:, :16]
    rows = []
    for i in range(8):
        is_row = (note[:, i : i + 1] - 1 == lane).astype(jnp.float32)
        rows.append(
            lax.dot_general(
                slot, is_row, (((0,), (0,)), ((), ())), preferred_element_type=jnp.float32
            )
        )
    perm[...] = jnp.concatenate(rows, axis=0).T
    facing[...] = note.astype(jnp.float32).T
    prepare(mine, near_ref, turn_ref, wall_ref, bulk_ref, dens_ref, stack, kept, lane, sub)
    ask[...] = jnp.zeros((256, 1, 128), jnp.float32)
    load_fixed.wait()
    to_scalar.wait()

    finish(first, 127 * 32, 3)

    def pick(target, base, at):
        for j in range(16):
            target[pl.ds(base + j, 1)] = first[pl.ds(index[j, at], 1)]

    pick(third, mine * 16, mine)

    def forward(step):
        group, member = other(step)
        at = group * 32 + member
        copy(
            second.at[pl.ds(at * 16, 16)], third.at[pl.ds(mine * 16, 16)], 2, group, member
        )

    def pick_step(step, carry):
        group, member = other(step)
        at = group * 32 + member
        pick(second, at * 16, at)

        @pl.when(step > 1)
        def _():
            forward(step - 1)

        return carry

    lax.fori_loop(1, 128, pick_step, 0)
    forward(127)
    finish(third, 127 * 16, 5)

    arrived = third.reshape(8, 16, 16, 128)
    for part in range(16):
        field[part] = exact(perm[...], arrived[:, part].reshape(128, 128))

    low = lane < 64
    sign = jnp.where(low, -1.0, 1.0)
    z_in = kept[Z_IN]

    def pair(axis, which):
        if axis == 0:
            return jnp.where(low, field[which], field[12 + which])
        found = exact(field[which], fixed[TAKE + 4 * (axis - 1)])
        for q in range(1, 4):
            found = found + exact(field[4 * q + which], fixed[TAKE + 4 * (axis - 1) + q])
        return found

    for axis in range(3):
        pressure = pair(axis, 0)
        normal = sign * pair(axis, 1 + axis)
        traces[6 + 2 * axis] = pressure
        traces[7 + 2 * axis] = normal
        turned = pltpu.roll(pressure + z_in * normal, 64, 1)
        traces[2 * axis] = jnp.where(low, z_in, turned)
        traces[2 * axis + 1] = jnp.where(low, turned, z_in)

    ask_rows = ask.reshape(256, 128)
    for face in range(6):
        if face < 4:
            ask_rows[pl.ds(64 * face, 32, stride=2), :] = exact(
                kept[GIVE + face][:32], traces[face]
            )
        else:
            ask_rows[pl.ds(128 * (face - 4) + 1, 16, stride=8), :] = exact(
                kept[GIVE + face][:16], traces[face]
            )

    def swap(source, target, phase):
        def one(step, carry):
            group, member = other(step)
            copy(
                source.at[pl.ds((group * 32 + member) * 2, 2)],
                target.at[pl.ds(mine * 2, 2)],
                phase,
                group,
                member,
            )
            return carry

        lax.fori_loop(1, 128, one, 0)
        target[pl.ds(mine * 2, 2)] = source[pl.ds(mine * 2, 2)]

    swap(ask, ask_in, 4 + 1)

    scale = jnp.float32(-metric_scale) * kept[BULK]
    thin = jnp.float32(-metric_scale) * kept[THIN]
    derivative = gll_tables(NP - 1)[2]

    def along_x(which):
        straight = [field[4 * q + which] for q in range(4)]
        crossed = [pltpu.roll(part, 64, 1) for part in straight]
        sums = []
        for q in range(4):
            found = None
            for b in range(4):
                one = jnp.where(low, derivative[2 * q, 2 * b], derivative[2 * q + 1, 2 * b + 1])
                two = jnp.where(low, derivative[2 * q, 2 * b + 1], derivative[2 * q + 1, 2 * b])
                term = one.astype(jnp.float32) * straight[b] + two.astype(jnp.float32) * crossed[b]
                found = term if found is None else found + term
            sums.append(found)
        return sums

    side_x = along_x(1)
    grad_x = along_x(0)
    for q in range(4):
        side = side_x[q] + exact(field[4 * q + 2], fixed[INSIDE])
        side = side + exact(field[4 * q + 3], fixed[INSIDE + 1])
        total[4 * q] = scale * side
        total[4 * q + 1] = thin * grad_x[q]
        total[4 * q + 2] = thin * exact(field[4 * q], fixed[INSIDE])
        total[4 * q + 3] = thin * exact(field[4 * q], fixed[INSIDE + 1])

    finish(ask_in, 254, 11)
    asked = ask_in.reshape(256, 128)
    answer_rows = answer.reshape(256, 128)
    sub_f = sub.astype(jnp.float32)
    for spot in range(2):
        face = mine // 32 if spot == 0 else 4 + mine // 64
        to = facing[pl.ds(8 + face, 1), :] - 1.0
        chosen = (to == sub_f).astype(jnp.float32)
        answer_rows[pl.ds(spot, 128, stride=2), :] = exact(
            chosen, asked[pl.ds(spot, 128, stride=2), :]
        )
    swap(answer, answer_in, 4 + 2)

    outside = [exact(kept[NEAR + face], traces[face ^ 1]) for face in range(6)]

    finish(answer_in, 254, 13)
    answers = answer_in.reshape(256, 128)
    for face in range(6):
        if face < 4:
            brought = answers[pl.ds(64 * (face ^ 1), 32, stride=2), :]
            picked = exact(kept[FAR + face][:, :32], brought)
        else:
            brought = answers[pl.ds(128 * ((face ^ 1) - 4) + 1, 16, stride=8), :]
            picked = exact(kept[FAR + face][:, :16], brought)
        outside[face] = outside[face] + picked
    lift = jnp.float32(metric_scale / float(gll_tables(NP - 1)[1][0]))
    gain_p = []
    gain_u = []
    for axis in range(3):
        even, odd = outside[2 * axis], outside[2 * axis + 1]
        coming = jnp.where(low, even, odd)
        z_out = pltpu.roll(jnp.where(low, odd, even), 64, 1)
        code = kept[CODE + axis].astype(jnp.int32)
        coming = jnp.where(code % 2 == 1, exact(coming, fixed[TURN]), coming)
        coming = jnp.where(code // 2 % 2 == 1, exact(coming, fixed[TURN + 1]), coming)
        coming = jnp.where(code >= 4, exact(coming, fixed[TURN + 2]), coming)
        is_wall = kept[WALL + axis] == 1.0
        pressure = traces[6 + 2 * axis]
        normal = traces[7 + 2 * axis]
        z_out = jnp.where(is_wall, z_in, z_out)
        jump = jnp.where(is_wall, 2.0 * z_in * normal, coming - pressure + z_out * normal)
        jump = lift * jump / (z_in + z_out)
        gain_p.append(kept[BULK] * jump)
        gain_u.append(-sign * kept[THIN] * z_in * jump)
    for q in range(4):
        for which in range(4):
            part = total[4 * q + which]
            for axis in range(3):
                if which == 0:
                    gain = gain_p[axis]
                elif which == 1 + axis:
                    gain = gain_u[axis]
                else:
                    continue
                if axis > 0:
                    part = part + exact(gain, fixed[LIFT + 4 * (axis - 1) + q])
                elif q == 0:
                    part = part + jnp.where(low, gain, 0.0)
                elif q == 3:
                    part = part + jnp.where(low, 0.0, gain)
            out_ref[pl.ds(4 * q + which, 128, stride=16), :] = part
    finish(notes, 127, 0)
    finish(first, 127 * 32, 2)
    finish(third, 127 * 16, 4)
    finish(ask_in, 254, 10)
    finish(answer_in, 254, 12)


def body(old_state, dest_row, neighbours, orientation, wall_flags, bulk_modulus, density):
    mine = lax.axis_index("grp") * 32 + lax.axis_index("dev")
    below = dest_row[None, :] < dest_row[:, None]
    tie = (dest_row[None, :] == dest_row[:, None]) & (
        jnp.arange(256)[None, :] < jnp.arange(256)[:, None]
    )
    position = jnp.sum((below | tie).astype(jnp.int32), axis=1)
    ordered = jnp.sum(
        jnp.where(position[:, None] == jnp.arange(256)[None, :], dest_row[:, None], 0), axis=0
    )
    pieces = ordered.reshape(32, 8)
    targets = pieces[:, 0] // 128
    row_ids = jnp.sum(
        jnp.where(
            targets[None, :, None] == jnp.arange(128)[:, None, None], pieces[None] % 128 + 1, 0
        ),
        axis=1,
    )
    owners = neighbours // 128
    beside = jnp.max(jnp.where((owners != mine) & (wall_flags == 0), owners + 1, 0), axis=1)
    note = jnp.concatenate(
        [
            row_ids,
            jnp.broadcast_to(beside[None, :], (128, 6)),
            jnp.zeros((128, 18), jnp.int32),
            jnp.broadcast_to(targets[None, :], (128, 32)),
            jnp.zeros((128, 64), jnp.int32),
        ],
        axis=1,
    )[:, None, :]
    view = old_state.reshape(256, 4, 4, 128).transpose(0, 2, 1, 3).reshape(256, 16, 1, 128)
    whole = pl.BlockSpec(memory_space=pltpu.VMEM)
    sends = pl.pallas_call(
        permute_kernel,
        out_shape=jax.ShapeDtypeStruct((128, 32, 1, 128), jnp.float32),
        in_specs=[pl.BlockSpec(memory_space=pltpu.SMEM), pl.BlockSpec(memory_space=pl.ANY)],
        out_specs=whole,
        scratch_shapes=[pltpu.SemaphoreType.DMA],
    )(position, view)
    small = pltpu.VMEM((256, 1, 128), jnp.float32)
    result = pl.pallas_call(
        exchange_kernel,
        out_shape=jax.ShapeDtypeStruct((2048, 128), jnp.float32),
        in_specs=[whole] * 7 + [pl.BlockSpec(memory_space=pl.ANY)],
        out_specs=whole,
        scratch_shapes=[
            pltpu.VMEM((128, 1, 128), jnp.int32),
            pltpu.VMEM((4096, 1, 128), jnp.float32),
            pltpu.VMEM((2048, 1, 128), jnp.float32),
            pltpu.VMEM((2048, 1, 128), jnp.float32),
            pltpu.VMEM((16, 128), jnp.int32),
            pltpu.SMEM((16, 128), jnp.int32),
            pltpu.VMEM((128, 128), jnp.float32),
            pltpu.VMEM((TABLES, 128, 128), jnp.float32),
            pltpu.VMEM((128, 128), jnp.float32),
            pltpu.VMEM((128, 128), jnp.float32),
            pltpu.VMEM((KEPT, 128, 128), jnp.float32),
            pltpu.VMEM((16, 128, 128), jnp.float32),
            pltpu.VMEM((12, 128, 128), jnp.float32),
            small,
            small,
            small,
            small,
            pltpu.VMEM((16, 128, 128), jnp.float32),
            pltpu.SemaphoreType.DMA((15,)),
        ],
        compiler_params=pltpu.CompilerParams(collective_id=0, has_side_effects=True),
    )(
        note,
        sends,
        neighbours,
        orientation,
        wall_flags,
        bulk_modulus[None, :],
        density[None, :],
        jnp.asarray(fixed_tables()),
    )
    return result.reshape(128, 4, 4, 128).transpose(0, 2, 1, 3).reshape(128, 4, 512)


def solution(mesh):
    in_specs = (
        P(("grp", "dev"), None, None),
        P(("grp", "dev")),
        P(None, ("grp", "dev")),
        P(None, ("grp", "dev")),
        P(None, ("grp", "dev")),
        P(("grp", "dev")),
        P(("grp", "dev")),
    )
    out_specs = P(("grp", "dev"), None, None)
    return jax.shard_map(body, mesh=mesh, in_specs=in_specs, out_specs=out_specs, check_vma=False)
```

```python
import jax
import jax.numpy as jnp
import numpy as np
from jax import lax
from jax.experimental import pallas as pl
from jax.experimental.pallas import tpu as pltpu
from jax.sharding import PartitionSpec as P

NP = 8
MESH = pl.DeviceIdType.MESH
HIGHEST = lax.Precision.HIGHEST

metric_scale = 0.25


def gll_tables(poly_order):
    num_points = poly_order + 1
    points = -np.cos(np.pi * np.arange(num_points) / poly_order)
    legendre = np.zeros((num_points, num_points))
    for sweeps in range(101):
        legendre[:, 0] = 1.0
        legendre[:, 1] = points
        for degree in range(2, num_points):
            legendre[:, degree] = (
                (2 * degree - 1) * points * legendre[:, degree - 1]
                - (degree - 1) * legendre[:, degree - 2]
            ) / degree
        if sweeps < 100:
            points = points - (points * legendre[:, poly_order] - legendre[:, poly_order - 1]) / (
                num_points * legendre[:, poly_order]
            )
    end_values = legendre[:, poly_order]
    weights = 2.0 / (poly_order * num_points * end_values**2)
    distance = points[:, None] - points[None, :] + np.eye(num_points)
    derivative = end_values[:, None] / end_values[None, :] / distance
    derivative = derivative * (1.0 - np.eye(num_points))
    derivative[0, 0] = -poly_order * num_points / 4.0
    derivative[poly_order, poly_order] = poly_order * num_points / 4.0
    return (points, weights, derivative)


def fixed_tables():
    derivative = gll_tables(NP - 1)[2]
    take = np.zeros((2, 4, 128, 128))
    for end in range(2):
        for first in range(8):
            for second in range(8):
                face_lane = 64 * end + 8 * first + second
                half, chunk = 64 * (first % 2), first // 2
                take[0, chunk, half + 56 * end + second, face_lane] = 1.0
                take[1, chunk, half + 8 * second + 7 * end, face_lane] = 1.0
    turns = np.zeros((3, 128, 128))
    for end in range(2):
        for first in range(8):
            for second in range(8):
                to = 64 * end + 8 * first + second
                turns[0, 64 * end + 8 * (7 - first) + second, to] = 1.0
                turns[1, 64 * end + 8 * first + 7 - second, to] = 1.0
                turns[2, 64 * end + 8 * second + first, to] = 1.0
    eye2, eye8 = np.eye(2), np.eye(8)
    inside = [
        np.kron(eye2, np.kron(derivative.T, eye8)),
        np.kron(eye2, np.kron(eye8, derivative.T)),
    ]
    lift = np.swapaxes(take, 2, 3)
    stack = [take.reshape(8, 128, 128), lift.reshape(8, 128, 128), turns]
    return np.concatenate(stack), np.stack(inside).astype(np.float32)


TAKE, LIFT, TURN = 0, 8, 16
NEAR, FAR, GIVE = 0, 6, 12
CODE, WALL, Z_IN, BULK, THIN, KEPT = 0, 3, 6, 7, 8, 9

STEPS = sorted(
    [(a, b, c, d) for a in range(4) for b in range(4) for c in range(4) for d in range(2)][1:],
    key=lambda step: -sum(min(part, 4 - part) for part in step[:3]),
)


def my_place():
    group = lax.axis_index("grp")
    member = lax.axis_index("dev")
    return group, member // 8, (member // 2) % 4, member % 2


def chip_at(place, step):
    z_at, y_at, x_at, _ = place
    x_to = (x_at + step) % 4
    y_to = (y_at + step // 4 + step) % 4
    z_to = (z_at + step // 16 + step // 4 + step) % 4
    return z_to, y_to * 4 + x_to


def split3(value):
    high = value.astype(jnp.bfloat16)
    rest = value - high.astype(jnp.float32)
    middle = rest.astype(jnp.bfloat16)
    low = (rest - middle.astype(jnp.float32)).astype(jnp.bfloat16)
    return high, middle, low


def pick_rows(chosen, value):
    wide = value.shape[1]
    parts = jnp.concatenate(split3(value), axis=1)
    found = jnp.dot(chosen, parts, preferred_element_type=jnp.float32)
    return found[:, :wide] + found[:, wide : 2 * wide] + found[:, 2 * wide :]


def pick_lanes(value, chosen):
    tall = value.shape[0]
    parts = jnp.concatenate(split3(value), axis=0)
    found = jnp.dot(parts, chosen, preferred_element_type=jnp.float32)
    return found[:tall] + found[tall : 2 * tall] + found[2 * tall :]


def exact(left, right):
    return jnp.dot(left, right, precision=HIGHEST, preferred_element_type=jnp.float32)


def count(left, right):
    return jnp.dot(
        left.astype(jnp.bfloat16), right.astype(jnp.bfloat16), preferred_element_type=jnp.float32
    )


def order_slots(dest_row, stack, ranks):
    lane = lax.broadcasted_iota(jnp.int32, (128, 128), 1)
    sub = lax.broadcasted_iota(jnp.int32, (128, 128), 0)
    value = dest_row.astype(jnp.float32)
    stack[0:2, :] = value
    columns = stack[...].T
    rows = [value[0:1, :], value[1:2, :]]
    slots = []
    for half in range(2):
        mine = columns[:, half : half + 1]
        below = jnp.zeros((128, 128), jnp.float32)
        for other in range(2):
            tied = rows[other] == mine
            if other > half:
                less = rows[other] < mine
            elif other < half:
                less = (rows[other] < mine) | tied
            else:
                less = (rows[other] < mine) | (tied & (lane < sub))
            below = below + jnp.where(less, 1.0, 0.0)
        slots.append((mine, jnp.sum(below, axis=1, keepdims=True)))
    lane_f = lane.astype(jnp.float32)
    sub_f = sub.astype(jnp.float32)
    for half in range(2):
        found = jnp.zeros((1, 128), jnp.float32)
        for part in range(2):
            is_it = slots[part][1] == lane_f + 128.0 * half
            found = found + jnp.sum(
                jnp.where(is_it, sub_f + 128.0 * part, 0.0), axis=0, keepdims=True
            )
        ranks[half : half + 1, :] = jnp.clip(found.astype(jnp.int32), 0, 255)
    return rows, slots


def write_notes(rows, slots, near_rows, wall_rows, mine, note_out):
    lane = lax.broadcasted_iota(jnp.int32, (128, 128), 1)
    sub = lax.broadcasted_iota(jnp.int32, (128, 128), 0)
    lane_f = lane.astype(jnp.float32)
    sub_f = sub.astype(jnp.float32)
    note = jnp.zeros((128, 128), jnp.float32)
    heads = jnp.zeros((1, 128), jnp.float32)
    for half in range(2):
        row = rows[half].astype(jnp.int32)
        owner_row = jnp.where(row >= 0, row // 128, -1)
        to = jnp.where(owner_row == sub, 1.0, 0.0)
        mine_f, rank = slots[half]
        column = mine_f.astype(jnp.int32)
        rank_i = rank.astype(jnp.int32)
        owner = jnp.where(column >= 0, column // 128, -1).astype(jnp.float32)
        inside = (column % 128 + 1).astype(jnp.float32)
        ids = jnp.where((rank_i % 8) == lane, inside, 0.0)
        note = note + count(to, ids)
        heads = heads + jnp.sum(
            jnp.where(rank_i == 8 * (lane - 32), owner, 0.0), axis=0, keepdims=True
        )
    owners = near_rows // 128
    beside = jnp.where((owners != mine) & (wall_rows == 0), owners + 1, 0).astype(jnp.float32)
    beside = jnp.max(beside, axis=1, keepdims=True)
    beside = jnp.sum(
        jnp.where(lane_f[:6] == sub_f[:6] + 8.0, beside, 0.0), axis=0, keepdims=True
    )
    heads = jnp.where((lane[:1] >= 32) & (lane[:1] < 64), heads, 0.0)
    note_out.reshape(128, 128)[...] = (note + heads + beside).astype(jnp.int32)


def prepare(mine, near_rows, turn_rows, wall_rows, bulk_row, dens_row, stack, moves, kept):
    lane = lax.broadcasted_iota(jnp.int32, (128, 128), 1)
    sub = lax.broadcasted_iota(jnp.int32, (128, 128), 0)
    away_rows = jnp.where((near_rows // 128 != mine) & (wall_rows == 0), 1.0, 0.0)
    stack[0:6, :] = near_rows.astype(jnp.float32)
    stack[8:14, :] = turn_rows.astype(jnp.float32)
    stack[16:22, :] = wall_rows.astype(jnp.float32)
    stack[24:25, :] = bulk_row
    stack[25:26, :] = dens_row
    stack[26:32, :] = away_rows
    columns = stack[...].T
    give_rank = count(stack[24:32, :], (sub < lane).astype(jnp.float32))
    base = (mine * 128).astype(jnp.float32)
    lane_f = lane.astype(jnp.float32)
    sub_f = sub.astype(jnp.float32)
    for face in range(6):
        near = columns[:, face : face + 1]
        away = columns[:, 26 + face : 27 + face]
        away_row = away_rows[face : face + 1, :]
        is_near = (near - base == lane_f) & (away == 0.0)
        before = jnp.where((near_rows[face : face + 1, :].astype(jnp.float32) < near), away_row, 0.0)
        take_rank = jnp.sum(before, axis=1, keepdims=True)
        is_far = (take_rank == lane_f) & (away > 0.0)
        is_given = (give_rank[2 + face : 3 + face, :] == sub_f) & (away_row > 0.0)
        moves[NEAR + face] = jnp.where(is_near, 1.0, 0.0).astype(jnp.bfloat16)
        moves[FAR + face] = jnp.where(is_far, 1.0, 0.0).astype(jnp.bfloat16)
        moves[GIVE + face] = jnp.where(is_given, 1.0, 0.0).astype(jnp.bfloat16)
    low = lane < 64
    for axis in range(3):
        kept[CODE + axis] = jnp.where(
            low, columns[:, 8 + 2 * axis : 9 + 2 * axis], columns[:, 9 + 2 * axis : 10 + 2 * axis]
        )
        kept[WALL + axis] = jnp.where(
            low, columns[:, 16 + 2 * axis : 17 + 2 * axis], columns[:, 17 + 2 * axis : 18 + 2 * axis]
        )
    bulk = jnp.broadcast_to(columns[:, 24:25], (128, 128))
    dens = jnp.broadcast_to(columns[:, 25:26], (128, 128))
    kept[Z_IN] = jnp.sqrt(bulk * dens)
    kept[BULK] = bulk
    kept[THIN] = 1.0 / dens


def exchange_kernel(
    state_ref, dest_ref, near_ref, turn_ref, wall_ref, bulk_ref, dens_ref, fixed_ref, inside_ref,
    out_ref, state, dest, near, turn, wall, bulk, dens, fixed, inside, ranks, slot_of, note_out,
    notes, sends, first, second, third, table, index, perm, stack, facing, moves, kept, field,
    traces, ask, ask_in, answer, answer_in, total, sems, loads, met_y, met_z,
):
    place = my_place()
    z_at, y_at, x_at, core = place
    member_here = lax.axis_index("dev")
    mine = z_at * 32 + member_here
    barrier = pltpu.get_barrier_semaphore()

    def signal(sem, group, y_to, x_to, core_to):
        pl.semaphore_signal(
            sem, inc=1, device_id=(group, (y_to * 4 + x_to) * 2 + core_to), device_id_type=MESH
        )

    for step in range(1, 8):
        signal(barrier, z_at, y_at, (x_at + step // 2) % 4, (core + step) % 2)
    for step in range(1, 4):
        signal(barrier, z_at, (y_at + step) % 4, x_at, core)
        signal(barrier, (z_at + step) % 4, y_at, x_at, core)

    pairs = [
        (dest_ref, dest), (near_ref, near), (wall_ref, wall), (turn_ref, turn),
        (bulk_ref, bulk), (dens_ref, dens), (state_ref, state), (fixed_ref, fixed),
        (inside_ref, inside),
    ]
    local = [pltpu.make_async_copy(a, b, loads.at[n]) for n, (a, b) in enumerate(pairs)]
    for one in local:
        one.start()
    stack[...] = jnp.zeros((128, 128), jnp.float32)
    local[0].wait()
    rows, slots = order_slots(dest[...], stack, ranks)
    to_slots = pltpu.make_async_copy(ranks, slot_of, loads.at[9])
    to_slots.start()
    pl.semaphore_wait(barrier, 13)
    for step in range(1, 4):
        signal(met_y, z_at, (y_at + step) % 4, x_at, core)
    local[1].wait()
    local[2].wait()
    write_notes(rows, slots, near[...], wall[...], mine, note_out)
    pl.semaphore_wait(met_y, 3)
    for step in range(1, 4):
        signal(met_z, (z_at + step) % 4, y_at, x_at, core)
    to_slots.wait()
    local[6].wait()

    def gather_first(target, base, at):
        row, chunk = at // 16, at % 16
        found = []
        for k in range(32):
            slot = slot_of[k // 16, (k % 16) * 8 + row]
            found.append(state[pl.ds(slot * 16 + chunk, 1)])
        for k in range(32):
            target[pl.ds(base + k, 1)] = found[k]

    def to_device(step):
        chip_step = jnp.where(step > 63, step - 63, step)
        side = jnp.where(step == 0, 1 - core, step // 64)
        group, chip = chip_at(place, chip_step)
        return group, chip * 2 + side

    def copy(source, target, phase, group, member):
        pltpu.make_async_remote_copy(
            src_ref=source,
            dst_ref=target,
            send_sem=sems.at[2 * phase],
            recv_sem=sems.at[2 * phase + 1],
            device_id=(group, member),
            device_id_type=MESH,
        ).start()

    def finish(buffer, rows, which):
        view = buffer.at[pl.ds(0, rows)]
        pltpu.make_async_copy(view, view, sems.at[which]).wait()

    def fetch(step):
        group, member = to_device(step)
        at = group * 32 + member
        gather_first(sends, at * 32, at)

    def spread(step):
        group, member = to_device(step)
        at = group * 32 + member
        copy(sends.at[pl.ds(at * 32, 32)], first.at[pl.ds(mine * 32, 32)], 1, group, member)

    def tell(group, member):
        at = group * 32 + member
        copy(note_out.at[pl.ds(at, 1)], notes.at[pl.ds(mine, 1)], 0, group, member)

    fetch(0)
    fetch(1)
    pl.semaphore_wait(met_z, 3)
    spread(0)
    tell(z_at, member_here + 1 - 2 * core)

    def early(step, carry):
        fetch(step + 1)
        spread(step)
        group, chip = chip_at(place, step)
        tell(group, chip * 2)
        tell(group, chip * 2 + 1)
        return carry

    lax.fori_loop(1, 64, early, 0)

    def late(step, carry):
        fetch(step + 1)
        spread(step)
        return carry

    lax.fori_loop(64, 126, late, 0)
    spread(126)
    gather_first(first, mine * 32, mine)
    notes[pl.ds(mine, 1)] = note_out[pl.ds(mine, 1)]

    local[3].wait()
    local[4].wait()
    local[5].wait()
    prepare(
        mine, near[...], turn[...], wall[...], bulk[...], dens[...], stack, moves, kept
    )
    ask[...] = jnp.zeros((256, 1, 128), jnp.float32)
    finish(notes, 127, 1)
    note = notes.reshape(128, 128)[...]
    lane = lax.broadcasted_iota(jnp.int32, (128, 128), 1)
    sub = lax.broadcasted_iota(jnp.int32, (128, 128), 0)
    lower = (lane < sub).astype(jnp.float32)
    piece = jnp.zeros((128, 128), jnp.int32)
    for k in range(32):
        piece = piece + jnp.where(note[:, 32 + k : 33 + k] == lane, k + 1, 0)
    valid = piece > 0
    rank = count(lower, valid.astype(jnp.float32)).astype(jnp.int32)
    entry = sub * 32 + piece - 1
    for j in range(16):
        chosen = jnp.sum(jnp.where(valid & (rank == j), entry, 0), axis=0, keepdims=True)
        table[j : j + 1, :] = jnp.clip(chosen, 0, 4095)
    to_index = pltpu.make_async_copy(table, index, loads.at[10])
    to_index.start()
    has = jnp.broadcast_to(note[:, 0:1] > 0, (128, 128))
    order = count(lower, has.astype(jnp.float32)).astype(jnp.int32)
    slot = jnp.where(has & (order == lane), 1.0, 0.0)[:, :16]
    rows = []
    for i in range(8):
        is_row = (note[:, i : i + 1] - 1 == lane).astype(jnp.float32)
        rows.append(
            lax.dot_general(
                slot, is_row, (((0,), (0,)), ((), ())), preferred_element_type=jnp.float32
            )
        )
    perm[...] = jnp.concatenate(rows, axis=0).T.astype(jnp.bfloat16)
    facing[...] = note.astype(jnp.float32).T
    local[7].wait()
    local[8].wait()
    to_index.wait()
    finish(first, 127 * 32, 3)

    def gather_second(target, base, at):
        found = [first[pl.ds(index[j, at], 1)] for j in range(16)]
        for j in range(16):
            target[pl.ds(base + j, 1)] = found[j]

    def device_at(step):
        group = (z_at + step[0]) % 4
        chip = ((y_at + step[1]) % 4) * 4 + (x_at + step[2]) % 4
        return group, chip * 2 + (core + step[3]) % 2

    def forward(group, member):
        at = group * 32 + member
        copy(
            second.at[pl.ds(at * 16, 16)], third.at[pl.ds(mine * 16, 16)], 2, group, member
        )

    before = None
    for step in STEPS:
        group, member = device_at(step)
        at = group * 32 + member
        gather_second(second, at * 16, at)
        if before is not None:
            forward(*before)
        before = (group, member)
    gather_second(third, mine * 16, mine)
    forward(*before)
    finish(third, 127 * 16, 5)

    arrived = third.reshape(8, 16, 16, 128)
    for part in range(16):
        field[part] = pick_rows(perm[...], arrived[:, part].reshape(128, 128))

    low = lane < 64
    sign = jnp.where(low, -1.0, 1.0)
    z_in = kept[Z_IN]

    def pair(axis, which):
        if axis == 0:
            return jnp.where(low, field[which], field[12 + which])
        found = pick_lanes(field[which], fixed[TAKE + 4 * (axis - 1)])
        for q in range(1, 4):
            found = found + pick_lanes(field[4 * q + which], fixed[TAKE + 4 * (axis - 1) + q])
        return found

    ask_rows = ask.reshape(256, 128)
    for axis in range(3):
        pressure = pair(axis, 0)
        normal = sign * pair(axis, 1 + axis)
        traces[6 + 2 * axis] = pressure
        traces[7 + 2 * axis] = normal
        turned = pltpu.roll(pressure + z_in * normal, 64, 1)
        traces[2 * axis] = jnp.where(low, z_in, turned)
        traces[2 * axis + 1] = jnp.where(low, turned, z_in)
        for face in (2 * axis, 2 * axis + 1):
            if face < 4:
                ask_rows[pl.ds(64 * face, 32, stride=2), :] = pick_rows(
                    moves[GIVE + face][:32], traces[face]
                )
            else:
                ask_rows[pl.ds(128 * (face - 4) + 1, 16, stride=8), :] = pick_rows(
                    moves[GIVE + face][:16], traces[face]
                )

    def swap(source, target, phase):
        for step in STEPS:
            group, member = device_at(step)
            copy(
                source.at[pl.ds((group * 32 + member) * 2, 2)],
                target.at[pl.ds(mine * 2, 2)],
                phase,
                group,
                member,
            )
        target[pl.ds(mine * 2, 2)] = source[pl.ds(mine * 2, 2)]

    swap(ask, ask_in, 3)

    scale = jnp.float32(-metric_scale) * kept[BULK]
    thin = jnp.float32(-metric_scale) * kept[THIN]
    derivative = gll_tables(NP - 1)[2]

    def along_x(which):
        straight = [field[4 * q + which] for q in range(4)]
        crossed = [pltpu.roll(part, 64, 1) for part in straight]
        sums = []
        for q in range(4):
            found = None
            for b in range(4):
                one = jnp.where(low, derivative[2 * q, 2 * b], derivative[2 * q + 1, 2 * b + 1])
                two = jnp.where(low, derivative[2 * q, 2 * b + 1], derivative[2 * q + 1, 2 * b])
                term = one.astype(jnp.float32) * straight[b] + two.astype(jnp.float32) * crossed[b]
                found = term if found is None else found + term
            sums.append(found)
        return sums

    side_x = along_x(1)
    grad_x = along_x(0)
    for q in range(4):
        side = side_x[q] + exact(field[4 * q + 2], inside[0])
        side = side + exact(field[4 * q + 3], inside[1])
        total[4 * q] = scale * side
        total[4 * q + 1] = thin * grad_x[q]
        total[4 * q + 2] = thin * exact(field[4 * q], inside[0])
        total[4 * q + 3] = thin * exact(field[4 * q], inside[1])

    finish(ask_in, 254, 7)
    asked = ask_in.reshape(256, 128)
    answer_rows = answer.reshape(256, 128)
    sub_f = sub.astype(jnp.float32)
    for spot in range(2):
        face = mine // 32 if spot == 0 else 4 + mine // 64
        to = facing[pl.ds(8 + face, 1), :] - 1.0
        chosen = jnp.where(to == sub_f, 1.0, 0.0).astype(jnp.bfloat16)
        answer_rows[pl.ds(spot, 128, stride=2), :] = pick_rows(
            chosen, asked[pl.ds(spot, 128, stride=2), :]
        )
    swap(answer, answer_in, 4)

    outside = [pick_rows(moves[NEAR + face], traces[face ^ 1]) for face in range(6)]

    finish(answer_in, 254, 9)
    answers = answer_in.reshape(256, 128)
    for face in range(6):
        if face < 4:
            brought = answers[pl.ds(64 * (face ^ 1), 32, stride=2), :]
            picked = pick_rows(moves[FAR + face][:, :32], brought)
        else:
            brought = answers[pl.ds(128 * ((face ^ 1) - 4) + 1, 16, stride=8), :]
            picked = pick_rows(moves[FAR + face][:, :16], brought)
        outside[face] = outside[face] + picked
    lift = jnp.float32(metric_scale / float(gll_tables(NP - 1)[1][0]))
    gains = []
    for axis in range(3):
        even, odd = outside[2 * axis], outside[2 * axis + 1]
        coming = jnp.where(low, even, odd)
        z_out = pltpu.roll(jnp.where(low, odd, even), 64, 1)
        code = kept[CODE + axis].astype(jnp.int32)
        coming = jnp.where(code % 2 == 1, pick_lanes(coming, fixed[TURN]), coming)
        coming = jnp.where(code // 2 % 2 == 1, pick_lanes(coming, fixed[TURN + 1]), coming)
        coming = jnp.where(code >= 4, pick_lanes(coming, fixed[TURN + 2]), coming)
        is_wall = kept[WALL + axis] == 1.0
        pressure = traces[6 + 2 * axis]
        normal = traces[7 + 2 * axis]
        z_out = jnp.where(is_wall, z_in, z_out)
        jump = jnp.where(is_wall, 2.0 * z_in * normal, coming - pressure + z_out * normal)
        jump = lift * jump / (z_in + z_out)
        gains.append(jnp.concatenate([kept[BULK] * jump, -sign * kept[THIN] * z_in * jump]))
    for q in range(4):
        if q == 0:
            along = jnp.where(jnp.concatenate([low, low]), gains[0], 0.0)
        elif q == 3:
            along = jnp.where(jnp.concatenate([low, low]), 0.0, gains[0])
        else:
            along = None
        lifted = [along] + [
            pick_lanes(gains[axis], fixed[LIFT + 4 * (axis - 1) + q]) for axis in (1, 2)
        ]
        part = total[4 * q] + lifted[1][:128] + lifted[2][:128]
        part_x = total[4 * q + 1]
        if along is not None:
            part = part + along[:128]
            part_x = part_x + along[128:]
        out_ref[pl.ds(4 * q, 128, stride=16), :] = part
        out_ref[pl.ds(4 * q + 1, 128, stride=16), :] = part_x
        out_ref[pl.ds(4 * q + 2, 128, stride=16), :] = total[4 * q + 2] + lifted[1][128:]
        out_ref[pl.ds(4 * q + 3, 128, stride=16), :] = total[4 * q + 3] + lifted[2][128:]
    finish(notes, 127, 0)
    finish(first, 127 * 32, 2)
    finish(third, 127 * 16, 4)
    finish(ask_in, 254, 6)
    finish(answer_in, 254, 8)


def body(old_state, dest_row, neighbours, orientation, wall_flags, bulk_modulus, density):
    view = old_state.reshape(256, 4, 4, 128).transpose(0, 2, 1, 3).reshape(4096, 1, 128)
    picks, inside = fixed_tables()
    f32, i32, bf16 = jnp.float32, jnp.int32, jnp.bfloat16
    halo = pltpu.VMEM((256, 1, 128), f32)
    result = pl.pallas_call(
        exchange_kernel,
        out_shape=jax.ShapeDtypeStruct((2048, 128), f32),
        in_specs=[pl.BlockSpec(memory_space=pl.ANY)] * 9,
        out_specs=pl.BlockSpec(memory_space=pltpu.VMEM),
        scratch_shapes=[
            pltpu.VMEM((4096, 1, 128), f32),
            pltpu.VMEM((2, 128), i32),
            pltpu.VMEM((6, 128), i32),
            pltpu.VMEM((6, 128), i32),
            pltpu.VMEM((6, 128), i32),
            pltpu.VMEM((1, 128), f32),
            pltpu.VMEM((1, 128), f32),
            pltpu.VMEM((19, 128, 128), bf16),
            pltpu.VMEM((2, 128, 128), f32),
            pltpu.VMEM((2, 128), i32),
            pltpu.SMEM((2, 128), i32),
            pltpu.VMEM((128, 1, 128), i32),
            pltpu.VMEM((128, 1, 128), i32),
            pltpu.VMEM((4096, 1, 128), f32),
            pltpu.VMEM((4096, 1, 128), f32),
            pltpu.VMEM((2048, 1, 128), f32),
            pltpu.VMEM((2048, 1, 128), f32),
            pltpu.VMEM((16, 128), i32),
            pltpu.SMEM((16, 128), i32),
            pltpu.VMEM((128, 128), bf16),
            pltpu.VMEM((128, 128), f32),
            pltpu.VMEM((128, 128), f32),
            pltpu.VMEM((18, 128, 128), bf16),
            pltpu.VMEM((KEPT, 128, 128), f32),
            pltpu.VMEM((16, 128, 128), f32),
            pltpu.VMEM((12, 128, 128), f32),
            halo,
            halo,
            halo,
            halo,
            pltpu.VMEM((16, 128, 128), f32),
            pltpu.SemaphoreType.DMA((10,)),
            pltpu.SemaphoreType.DMA((11,)),
            pltpu.SemaphoreType.REGULAR,
            pltpu.SemaphoreType.REGULAR,
        ],
        compiler_params=pltpu.CompilerParams(collective_id=0, has_side_effects=True),
    )(
        view,
        dest_row.reshape(2, 128),
        neighbours,
        orientation,
        wall_flags,
        bulk_modulus[None, :],
        density[None, :],
        jnp.asarray(picks, bf16),
        jnp.asarray(inside),
    )
    return result.reshape(128, 4, 4, 128).transpose(0, 2, 1, 3).reshape(128, 4, 512)


def solution(mesh):
    in_specs = (
        P(("grp", "dev"), None, None),
        P(("grp", "dev")),
        P(None, ("grp", "dev")),
        P(None, ("grp", "dev")),
        P(None, ("grp", "dev")),
        P(("grp", "dev")),
        P(("grp", "dev")),
    )
    out_specs = P(("grp", "dev"), None, None)
    return jax.shard_map(body, mesh=mesh, in_specs=in_specs, out_specs=out_specs, check_vma=False)
```

```python
import jax
import jax.numpy as jnp
import numpy as np
from jax import lax
from jax.experimental import pallas as pl
from jax.experimental.pallas import tpu as pltpu
from jax.sharding import PartitionSpec as P

NP = 8
MESH = pl.DeviceIdType.MESH
HIGHEST = lax.Precision.HIGHEST
HELD = 48

metric_scale = 0.25


def gll_tables(poly_order):
    num_points = poly_order + 1
    points = -np.cos(np.pi * np.arange(num_points) / poly_order)
    legendre = np.zeros((num_points, num_points))
    for sweeps in range(101):
        legendre[:, 0] = 1.0
        legendre[:, 1] = points
        for degree in range(2, num_points):
            legendre[:, degree] = (
                (2 * degree - 1) * points * legendre[:, degree - 1]
                - (degree - 1) * legendre[:, degree - 2]
            ) / degree
        if sweeps < 100:
            points = points - (points * legendre[:, poly_order] - legendre[:, poly_order - 1]) / (
                num_points * legendre[:, poly_order]
            )
    end_values = legendre[:, poly_order]
    weights = 2.0 / (poly_order * num_points * end_values**2)
    distance = points[:, None] - points[None, :] + np.eye(num_points)
    derivative = end_values[:, None] / end_values[None, :] / distance
    derivative = derivative * (1.0 - np.eye(num_points))
    derivative[0, 0] = -poly_order * num_points / 4.0
    derivative[poly_order, poly_order] = poly_order * num_points / 4.0
    return (points, weights, derivative)


def fixed_tables():
    derivative = gll_tables(NP - 1)[2]
    take = np.zeros((2, 4, 128, 128))
    for end in range(2):
        for first in range(8):
            for second in range(8):
                face_lane = 64 * end + 8 * first + second
                half, chunk = 64 * (first % 2), first // 2
                take[0, chunk, half + 56 * end + second, face_lane] = 1.0
                take[1, chunk, half + 8 * second + 7 * end, face_lane] = 1.0
    turns = np.zeros((3, 128, 128))
    for end in range(2):
        for first in range(8):
            for second in range(8):
                to = 64 * end + 8 * first + second
                turns[0, 64 * end + 8 * (7 - first) + second, to] = 1.0
                turns[1, 64 * end + 8 * first + 7 - second, to] = 1.0
                turns[2, 64 * end + 8 * second + first, to] = 1.0
    eye2, eye8 = np.eye(2), np.eye(8)
    inside = [
        np.kron(eye2, np.kron(derivative.T, eye8)),
        np.kron(eye2, np.kron(eye8, derivative.T)),
    ]
    lift = np.swapaxes(take, 2, 3)
    stack = [take.reshape(8, 128, 128), lift.reshape(8, 128, 128), turns]
    comes_from = np.full((128, 128), -1.0)
    for number, step in enumerate(NEARBY):
        for device in range(128):
            place = device // 32, device // 8 % 4, device // 2 % 4, device % 2
            back = [(at - by) % size for at, by, size in zip(place, step, (4, 4, 4, 2))]
            comes_from[number, device] = back[0] * 32 + back[1] * 8 + back[2] * 2 + back[3]
    return np.concatenate(stack), np.stack(inside + [comes_from]).astype(np.float32)


TAKE, LIFT, TURN = 0, 8, 16
NEAR, FAR, GIVE, ROUTE, OWNER = 0, 3, 6, 9, 12
CODE, WALL, Z_IN, BULK, THIN, SPOT, KEPT = 0, 3, 6, 7, 8, 9, 12

STEPS = sorted(
    [(a, b, c, d) for a in range(4) for b in range(4) for c in range(4) for d in range(2)][1:],
    key=lambda step: -sum(min(part, 4 - part) for part in step[:3]),
)
NEARBY = [(0, 0, 0, 0)] + STEPS[::-1][:31]


def my_place():
    group = lax.axis_index("grp")
    member = lax.axis_index("dev")
    return group, member // 8, (member // 2) % 4, member % 2


def chip_at(place, step):
    z_at, y_at, x_at, _ = place
    x_to = (x_at + step) % 4
    y_to = (y_at + step // 4 + step) % 4
    z_to = (z_at + step // 16 + step // 4 + step) % 4
    return z_to, y_to * 4 + x_to


def split3(value):
    high = value.astype(jnp.bfloat16)
    rest = value - high.astype(jnp.float32)
    middle = rest.astype(jnp.bfloat16)
    low = (rest - middle.astype(jnp.float32)).astype(jnp.bfloat16)
    return high, middle, low


def pick_rows(chosen, value):
    wide = value.shape[1]
    parts = jnp.concatenate(split3(value), axis=1)
    found = jnp.dot(chosen, parts, preferred_element_type=jnp.float32)
    return found[:, :wide] + found[:, wide : 2 * wide] + found[:, 2 * wide :]


def pick_lanes(value, chosen):
    tall = value.shape[0]
    parts = jnp.concatenate(split3(value), axis=0)
    found = jnp.dot(parts, chosen, preferred_element_type=jnp.float32)
    return found[:tall] + found[tall : 2 * tall] + found[2 * tall :]


def exact(left, right):
    return jnp.dot(left, right, precision=HIGHEST, preferred_element_type=jnp.float32)


def count(left, right):
    return jnp.dot(
        left.astype(jnp.bfloat16), right.astype(jnp.bfloat16), preferred_element_type=jnp.float32
    )


def order_slots(dest_row, stack, ranks):
    lane = lax.broadcasted_iota(jnp.int32, (128, 128), 1)
    sub = lax.broadcasted_iota(jnp.int32, (128, 128), 0)
    value = dest_row.astype(jnp.float32)
    stack[0:2, :] = value
    columns = stack[...].T
    rows = [value[0:1, :], value[1:2, :]]
    slots = []
    for half in range(2):
        mine = columns[:, half : half + 1]
        below = jnp.zeros((128, 128), jnp.float32)
        for other in range(2):
            tied = rows[other] == mine
            if other > half:
                less = rows[other] < mine
            elif other < half:
                less = (rows[other] < mine) | tied
            else:
                less = (rows[other] < mine) | (tied & (lane < sub))
            below = below + jnp.where(less, 1.0, 0.0)
        slots.append((mine, jnp.sum(below, axis=1, keepdims=True)))
    lane_f = lane.astype(jnp.float32)
    sub_f = sub.astype(jnp.float32)
    for half in range(2):
        found = jnp.zeros((1, 128), jnp.float32)
        for part in range(2):
            is_it = slots[part][1] == lane_f + 128.0 * half
            found = found + jnp.sum(
                jnp.where(is_it, sub_f + 128.0 * part, 0.0), axis=0, keepdims=True
            )
        ranks[half : half + 1, :] = jnp.clip(found.astype(jnp.int32), 0, 255)
    return rows, slots


def write_notes(rows, slots, near_rows, wall_rows, mine, note_out):
    lane = lax.broadcasted_iota(jnp.int32, (128, 128), 1)
    sub = lax.broadcasted_iota(jnp.int32, (128, 128), 0)
    lane_f = lane.astype(jnp.float32)
    sub_f = sub.astype(jnp.float32)
    note = jnp.zeros((128, 128), jnp.float32)
    heads = jnp.zeros((1, 128), jnp.float32)
    for half in range(2):
        row = rows[half].astype(jnp.int32)
        owner_row = jnp.where(row >= 0, row // 128, -1)
        to = jnp.where(owner_row == sub, 1.0, 0.0)
        mine_f, rank = slots[half]
        column = mine_f.astype(jnp.int32)
        rank_i = rank.astype(jnp.int32)
        owner = jnp.where(column >= 0, column // 128, -1).astype(jnp.float32)
        inside = (column % 128 + 1).astype(jnp.float32)
        ids = jnp.where((rank_i % 8) == lane, inside, 0.0)
        note = note + count(to, ids)
        heads = heads + jnp.sum(
            jnp.where(rank_i == 8 * (lane - 32), owner, 0.0), axis=0, keepdims=True
        )
    owners = near_rows // 128
    beside = jnp.where((owners != mine) & (wall_rows == 0), owners + 1, 0).astype(jnp.float32)
    beside = jnp.max(beside, axis=1, keepdims=True)
    beside = jnp.sum(
        jnp.where(lane_f[:6] == sub_f[:6] + 8.0, beside, 0.0), axis=0, keepdims=True
    )
    heads = jnp.where((lane[:1] >= 32) & (lane[:1] < 64), heads, 0.0)
    note_out.reshape(128, 128)[...] = (note + heads + beside).astype(jnp.int32)


def prepare(
    mine, near_rows, turn_rows, wall_rows, bulk_row, dens_row, comes_from, stack, moves, kept
):
    lane = lax.broadcasted_iota(jnp.int32, (128, 128), 1)
    sub = lax.broadcasted_iota(jnp.int32, (128, 128), 0)
    away_rows = jnp.where((near_rows // 128 != mine) & (wall_rows == 0), 1.0, 0.0)
    stack[0:6, :] = near_rows.astype(jnp.float32)
    stack[8:14, :] = turn_rows.astype(jnp.float32)
    stack[16:22, :] = wall_rows.astype(jnp.float32)
    stack[24:25, :] = bulk_row
    stack[25:26, :] = dens_row
    stack[26:32, :] = away_rows
    columns = stack[...].T
    give_rank = count(stack[24:32, :], (sub < lane).astype(jnp.float32))
    base = (mine * 128).astype(jnp.float32)
    lane_f = lane.astype(jnp.float32)
    sub_f = sub.astype(jnp.float32)
    owners = near_rows // 128
    beside = jnp.where(away_rows > 0.0, owners + 1, 0).astype(jnp.float32)
    beside = jnp.max(beside, axis=1, keepdims=True) - 1.0
    for face in range(6):
        axis, half = face // 2, face % 2
        near = columns[:, face : face + 1]
        away = columns[:, 26 + face : 27 + face]
        away_row = away_rows[face : face + 1, :]
        is_near = (near - base == lane_f) & (away == 0.0)
        before = jnp.where((near_rows[face : face + 1, :].astype(jnp.float32) < near), away_row, 0.0)
        take_rank = jnp.sum(before, axis=1, keepdims=True)
        is_far = jnp.where((take_rank == lane_f) & (away > 0.0), 1.0, 0.0)
        passed_by = jnp.where(comes_from == beside[face : face + 1, :], 1.0, 0.0)
        is_given = (give_rank[2 + face : 3 + face, :] == sub_f[:32]) & (away_row > 0.0)
        rows = pl.ds(128 * half, 128)
        moves[NEAR + axis, rows] = jnp.where(is_near, 1.0, 0.0).astype(jnp.bfloat16)
        moves[FAR + axis, rows] = count(is_far[:, :32], passed_by).astype(jnp.bfloat16)
        moves[GIVE + axis, pl.ds(32 * (1 - half), 32)] = jnp.where(is_given, 1.0, 0.0).astype(
            jnp.bfloat16
        )
        near_i = near.astype(jnp.int32)
        moves[OWNER + axis, rows] = jnp.where(near_i // 128 == lane, 1.0, 0.0).astype(jnp.bfloat16)
        kept[SPOT + axis, :, 64 * half : 64 * half + 64] = jnp.broadcast_to(
            (near_i % 128).astype(jnp.float32), (128, 64)
        )
    low = lane < 64
    for axis in range(3):
        kept[CODE + axis] = jnp.where(
            low, columns[:, 8 + 2 * axis : 9 + 2 * axis], columns[:, 9 + 2 * axis : 10 + 2 * axis]
        )
        kept[WALL + axis] = jnp.where(
            low, columns[:, 16 + 2 * axis : 17 + 2 * axis], columns[:, 17 + 2 * axis : 18 + 2 * axis]
        )
    bulk = jnp.broadcast_to(columns[:, 24:25], (128, 128))
    dens = jnp.broadcast_to(columns[:, 25:26], (128, 128))
    kept[Z_IN] = jnp.sqrt(bulk * dens)
    kept[BULK] = bulk
    kept[THIN] = 1.0 / dens


def exchange_kernel(
    state_ref, dest_ref, near_ref, turn_ref, wall_ref, bulk_ref, dens_ref, fixed_ref, inside_ref,
    out_ref, state, dest, near, turn, wall, bulk, dens, fixed, inside, ranks, slot_of, note_out,
    notes, sends, first, second, third, table, index, perm, stack, z_here, z_all, moves, kept, field,
    traces, ask, ask_in, answer, answer_in, total, sems, loads, met_y, met_z,
):
    place = my_place()
    z_at, y_at, x_at, core = place
    member_here = lax.axis_index("dev")
    mine = z_at * 32 + member_here
    barrier = pltpu.get_barrier_semaphore()

    def signal(sem, group, y_to, x_to, core_to):
        pl.semaphore_signal(
            sem, inc=1, device_id=(group, (y_to * 4 + x_to) * 2 + core_to), device_id_type=MESH
        )

    for step in range(1, 8):
        signal(barrier, z_at, y_at, (x_at + step // 2) % 4, (core + step) % 2)
    for step in range(1, 4):
        signal(barrier, z_at, (y_at + step) % 4, x_at, core)
        signal(barrier, (z_at + step) % 4, y_at, x_at, core)

    pairs = [
        (dest_ref, dest), (near_ref, near), (wall_ref, wall), (turn_ref, turn),
        (bulk_ref, bulk), (dens_ref, dens), (state_ref, state), (fixed_ref, fixed),
        (inside_ref, inside),
    ]
    local = [pltpu.make_async_copy(a, b, loads.at[n]) for n, (a, b) in enumerate(pairs)]
    for one in local:
        one.start()
    stack[...] = jnp.zeros((128, 128), jnp.float32)
    local[0].wait()
    rows, slots = order_slots(dest[...], stack, ranks)
    to_slots = pltpu.make_async_copy(ranks, slot_of, loads.at[9])
    to_slots.start()
    pl.semaphore_wait(barrier, 13)
    for step in range(1, 4):
        signal(met_y, z_at, (y_at + step) % 4, x_at, core)
    local[1].wait()
    local[2].wait()
    write_notes(rows, slots, near[...], wall[...], mine, note_out)
    pl.semaphore_wait(met_y, 3)
    for step in range(1, 4):
        signal(met_z, (z_at + step) % 4, y_at, x_at, core)
    to_slots.wait()
    local[6].wait()

    def gather_first(target, base, at):
        row, chunk = at // 16, at % 16
        found = []
        for k in range(32):
            slot = slot_of[k // 16, (k % 16) * 8 + row]
            found.append(state[pl.ds(slot * 16 + chunk, 1)])
        for k in range(32):
            target[pl.ds(base + k, 1)] = found[k]

    def to_device(step):
        chip_step = jnp.where(step > 63, step - 63, step)
        side = jnp.where(step == 0, 1 - core, step // 64)
        group, chip = chip_at(place, chip_step)
        return group, chip * 2 + side

    def copy(source, target, phase, group, member):
        pltpu.make_async_remote_copy(
            src_ref=source,
            dst_ref=target,
            send_sem=sems.at[2 * phase],
            recv_sem=sems.at[2 * phase + 1],
            device_id=(group, member),
            device_id_type=MESH,
        ).start()

    def finish(buffer, rows, which):
        view = buffer.at[pl.ds(0, rows)]
        pltpu.make_async_copy(view, view, sems.at[which]).wait()

    def fetch(step):
        group, member = to_device(step)
        at = group * 32 + member
        gather_first(sends, at * 32, at)

    def spread(step, leaves):
        group, member = to_device(step)
        at = group * 32 + member
        pltpu.make_async_remote_copy(
            src_ref=sends.at[pl.ds(at * 32, 32)],
            dst_ref=first.at[pl.ds(mine * 32, 32)],
            send_sem=sems.at[leaves],
            recv_sem=sems.at[16 + member % 2],
            device_id=(group, member),
            device_id_type=MESH,
        ).start()

    def tell(group, member):
        at = group * 32 + member
        copy(note_out.at[pl.ds(at, 1)], notes.at[pl.ds(mine, 1)], 0, group, member)

    fetch(0)
    fetch(1)
    pl.semaphore_wait(met_z, 3)
    spread(0, 2)
    tell(z_at, member_here + 1 - 2 * core)

    def early(leaves):
        def one(step, carry):
            fetch(step + 1)
            spread(step, leaves)
            group, chip = chip_at(place, step)
            tell(group, chip * 2)
            tell(group, chip * 2 + 1)
            return carry

        return one

    lax.fori_loop(1, HELD + 1, early(12), 0)
    lax.fori_loop(HELD + 1, 64, early(13), 0)

    def late(step, carry):
        spread(step, 14)
        fetch(step + 1)
        return carry

    finish(first, HELD * 32, 12)
    lax.fori_loop(64, 126, late, 0)
    spread(126, 14)
    gather_first(first, mine * 32, mine)
    notes[pl.ds(mine, 1)] = note_out[pl.ds(mine, 1)]

    local[3].wait()
    local[4].wait()
    local[5].wait()
    local[8].wait()
    z_here[...] = jnp.sqrt(bulk[...] * dens[...]).reshape(1, 1, 128)
    z_all[pl.ds(mine, 1)] = z_here[...]

    def tell_z(step, carry):
        group, chip = chip_at(place, step // 2)
        copy(z_here, z_all.at[pl.ds(mine, 1)], 5, group, chip * 2 + (core + step) % 2)
        return carry

    lax.fori_loop(1, 128, tell_z, 0)
    ask_in[...] = jnp.zeros((384, 1, 128), jnp.float32)
    prepare(
        mine, near[...], turn[...], wall[...], bulk[...], dens[...], inside[2, :32, :], stack,
        moves, kept,
    )
    finish(notes, 127, 1)
    note = notes.reshape(128, 128)[...]
    lane = lax.broadcasted_iota(jnp.int32, (128, 128), 1)
    sub = lax.broadcasted_iota(jnp.int32, (128, 128), 0)
    lower = (lane < sub).astype(jnp.float32)
    piece = jnp.zeros((128, 128), jnp.int32)
    for k in range(32):
        piece = piece + jnp.where(note[:, 32 + k : 33 + k] == lane, k + 1, 0)
    valid = piece > 0
    rank = count(lower, valid.astype(jnp.float32)).astype(jnp.int32)
    entry = sub * 32 + piece - 1
    for j in range(16):
        chosen = jnp.sum(jnp.where(valid & (rank == j), entry, 0), axis=0, keepdims=True)
        table[j : j + 1, :] = jnp.clip(chosen, 0, 4095)
    to_index = pltpu.make_async_copy(table, index, loads.at[10])
    to_index.start()
    has = jnp.broadcast_to(note[:, 0:1] > 0, (128, 128))
    order = count(lower, has.astype(jnp.float32)).astype(jnp.int32)
    slot = jnp.where(has & (order == lane), 1.0, 0.0)[:, :16]
    rows = []
    for i in range(8):
        is_row = (note[:, i : i + 1] - 1 == lane).astype(jnp.float32)
        rows.append(
            lax.dot_general(
                slot, is_row, (((0,), (0,)), ((), ())), preferred_element_type=jnp.float32
            )
        )
    perm[...] = jnp.concatenate(rows, axis=0).T.astype(jnp.bfloat16)
    facing = note.astype(jnp.float32).T
    for face in range(6):
        to = facing[8 + face : 9 + face, :] - 1.0
        chosen = jnp.where(to == sub.astype(jnp.float32), 1.0, 0.0).astype(jnp.bfloat16)
        moves[ROUTE + face // 2, pl.ds(128 * (1 - face % 2), 128)] = chosen
    local[7].wait()
    to_index.wait()
    finish(first, 127 * 32, 16 + core)

    def gather_second(target, base, at):
        found = [first[pl.ds(index[j, at], 1)] for j in range(16)]
        for j in range(16):
            target[pl.ds(base + j, 1)] = found[j]

    def device_at(step):
        group = (z_at + step[0]) % 4
        chip = ((y_at + step[1]) % 4) * 4 + (x_at + step[2]) % 4
        return group, chip * 2 + (core + step[3]) % 2

    def forward(group, member):
        at = group * 32 + member
        copy(
            second.at[pl.ds(at * 16, 16)], third.at[pl.ds(mine * 16, 16)], 2, group, member
        )

    before = None
    for step in STEPS:
        group, member = device_at(step)
        at = group * 32 + member
        gather_second(second, at * 16, at)
        if before is not None:
            forward(*before)
        before = (group, member)
    gather_second(third, mine * 16, mine)
    forward(*before)
    finish(third, 127 * 16, 5)

    arrived = third.reshape(8, 16, 16, 128)
    for part in range(16):
        field[part] = pick_rows(perm[...], arrived[:, part].reshape(128, 128))

    low = lane < 64
    sign = jnp.where(low, -1.0, 1.0)
    z_in = kept[Z_IN]

    def four(which):
        return jnp.concatenate([field[4 * q + which] for q in range(4)], axis=1)

    def taken(which, axes):
        table = [
            jnp.concatenate([fixed[TAKE + 4 * (axis - 1) + q] for q in range(4)], axis=0)
            for axis in axes
        ]
        return pick_lanes(four(which), jnp.concatenate(table, axis=1))

    both = taken(0, (1, 2))
    pressures = [jnp.where(low, field[0], field[12]), both[:, :128], both[:, 128:]]
    normals = [jnp.where(low, field[1], field[13]), taken(2, (1,)), taken(3, (2,))]
    ask_rows = ask.reshape(96, 128)
    for axis in range(3):
        normal = sign * normals[axis]
        traces[3 + axis] = pressures[axis]
        traces[6 + axis] = normal
        turned = pltpu.roll(pressures[axis] + z_in * normal, 64, 1)
        traces[axis] = turned
        found = pick_rows(moves[GIVE + axis, :64], turned)
        ask_rows[pl.ds(axis, 32, stride=3), :] = jnp.where(low[:32], found[:32], found[32:])

    def three(step, number, source, target, phase):
        group, member = device_at(step)
        at = group * 32 + member if number is None else number
        copy(
            source.at[pl.ds(at * 3, 3)], target.at[pl.ds(mine * 3, 3)], phase, group, member
        )

    for number in range(31, 0, -1):
        three(NEARBY[number], number, ask, ask_in, 3)
    ask_in[pl.ds(mine * 3, 3)] = ask[pl.ds(0, 3)]

    scale = jnp.float32(-metric_scale) * kept[BULK]
    thin = jnp.float32(-metric_scale) * kept[THIN]
    derivative = gll_tables(NP - 1)[2]

    def along_x(which):
        straight = [field[4 * q + which] for q in range(4)]
        crossed = [pltpu.roll(part, 64, 1) for part in straight]
        sums = []
        for q in range(4):
            found = None
            for b in range(4):
                one = jnp.where(low, derivative[2 * q, 2 * b], derivative[2 * q + 1, 2 * b + 1])
                two = jnp.where(low, derivative[2 * q, 2 * b + 1], derivative[2 * q + 1, 2 * b])
                term = one.astype(jnp.float32) * straight[b] + two.astype(jnp.float32) * crossed[b]
                found = term if found is None else found + term
            sums.append(found)
        return sums

    side_x = along_x(1)
    grad_x = along_x(0)
    for q in range(4):
        total[4 * q] = side_x[q]
        total[4 * q + 1] = thin * grad_x[q]

    finish(ask_in, 93, 7)
    asked = ask_in.reshape(384, 128)
    answer_rows = answer.reshape(384, 128)
    for axis in range(3):
        found = pick_rows(moves[ROUTE + axis], asked[pl.ds(axis, 128, stride=3), :])
        answer_rows[pl.ds(axis, 128, stride=3), :] = jnp.where(low, found[:128], found[128:])
    for step in STEPS:
        three(step, None, answer, answer_in, 4)
    answer_in[pl.ds(mine * 3, 3)] = answer[pl.ds(mine * 3, 3)]

    finish(z_all, 127, 11)
    z_table = z_all.reshape(128, 128)[...]
    lane_f = lane.astype(jnp.float32)
    for axis in range(3):
        found = pick_rows(moves[OWNER + axis], z_table)
        sides = []
        for half in range(2):
            spot = kept[SPOT + axis, :, 64 * half : 64 * half + 1]
            sides.append(
                jnp.sum(
                    jnp.where(lane_f == spot, found[128 * half : 128 * half + 128], 0.0),
                    axis=1,
                    keepdims=True,
                )
            )
        kept[SPOT + axis] = jnp.where(low, sides[0], sides[1])
        found = pick_rows(moves[NEAR + axis], traces[axis])
        traces[axis] = jnp.where(low, found[:128], found[128:])

    def stacked(which):
        return jnp.concatenate([field[4 * q + which] for q in range(4)], axis=0)

    side_y = exact(stacked(2), inside[0])
    side_z = exact(stacked(3), inside[1])
    grad_y = exact(stacked(0), inside[0])
    grad_z = exact(stacked(0), inside[1])
    for q in range(4):
        rows = slice(128 * q, 128 * q + 128)
        total[4 * q] = scale * (total[4 * q] + side_y[rows] + side_z[rows])
        total[4 * q + 2] = thin * grad_y[rows]
        total[4 * q + 3] = thin * grad_z[rows]

    finish(answer_in, 381, 9)
    answers = answer_in.reshape(384, 128)
    coming = []
    for axis in range(3):
        found = pick_rows(moves[FAR + axis], answers[pl.ds(axis, 128, stride=3), :])
        coming.append(traces[axis] + jnp.where(low, found[:128], found[128:]))
    coming = jnp.concatenate(coming, axis=0)
    code = jnp.concatenate([kept[CODE + axis] for axis in range(3)], axis=0).astype(jnp.int32)
    coming = jnp.where(code % 2 == 1, pick_lanes(coming, fixed[TURN]), coming)
    coming = jnp.where(code // 2 % 2 == 1, pick_lanes(coming, fixed[TURN + 1]), coming)
    coming = jnp.where(code >= 4, pick_lanes(coming, fixed[TURN + 2]), coming)
    lift = jnp.float32(metric_scale / float(gll_tables(NP - 1)[1][0]))
    gains = []
    for axis in range(3):
        is_wall = kept[WALL + axis] == 1.0
        normal = traces[6 + axis]
        z_out = jnp.where(is_wall, z_in, kept[SPOT + axis])
        other = coming[128 * axis : 128 * axis + 128]
        jump = jnp.where(
            is_wall, 2.0 * z_in * normal, other - traces[3 + axis] + z_out * normal
        )
        jump = lift * jump / (z_in + z_out)
        gains.append(jnp.concatenate([kept[BULK] * jump, -sign * kept[THIN] * z_in * jump]))
    lifted = []
    for axis in (1, 2):
        wide = jnp.concatenate([fixed[LIFT + 4 * (axis - 1) + q] for q in range(4)], axis=1)
        lifted.append(pick_lanes(gains[axis], wide))
    for q in range(4):
        lanes = slice(128 * q, 128 * q + 128)
        part = total[4 * q] + lifted[0][:128, lanes] + lifted[1][:128, lanes]
        part_x = total[4 * q + 1]
        if q in (0, 3):
            keep = low if q == 0 else lane >= 64
            part = part + jnp.where(keep, gains[0][:128], 0.0)
            part_x = part_x + jnp.where(keep, gains[0][128:], 0.0)
        out_ref[pl.ds(4 * q, 128, stride=16), :] = part
        out_ref[pl.ds(4 * q + 1, 128, stride=16), :] = part_x
        out_ref[pl.ds(4 * q + 2, 128, stride=16), :] = total[4 * q + 2] + lifted[0][128:, lanes]
        out_ref[pl.ds(4 * q + 3, 128, stride=16), :] = total[4 * q + 3] + lifted[1][128:, lanes]
    finish(notes, 127, 0)
    finish(first, 32, 2)
    finish(first, (63 - HELD) * 32, 13)
    finish(first, 63 * 32, 14)
    finish(z_all, 127, 10)
    finish(third, 127 * 16, 4)
    finish(ask_in, 93, 6)
    finish(answer_in, 381, 8)


def body(old_state, dest_row, neighbours, orientation, wall_flags, bulk_modulus, density):
    view = old_state.reshape(256, 4, 4, 128).transpose(0, 2, 1, 3).reshape(4096, 1, 128)
    picks, inside = fixed_tables()
    f32, i32, bf16 = jnp.float32, jnp.int32, jnp.bfloat16
    halo = pltpu.VMEM((384, 1, 128), f32)
    result = pl.pallas_call(
        exchange_kernel,
        out_shape=jax.ShapeDtypeStruct((2048, 128), f32),
        in_specs=[pl.BlockSpec(memory_space=pl.ANY)] * 9,
        out_specs=pl.BlockSpec(memory_space=pltpu.VMEM),
        scratch_shapes=[
            pltpu.VMEM((4096, 1, 128), f32),
            pltpu.VMEM((2, 128), i32),
            pltpu.VMEM((6, 128), i32),
            pltpu.VMEM((6, 128), i32),
            pltpu.VMEM((6, 128), i32),
            pltpu.VMEM((1, 128), f32),
            pltpu.VMEM((1, 128), f32),
            pltpu.VMEM((19, 128, 128), bf16),
            pltpu.VMEM((3, 128, 128), f32),
            pltpu.VMEM((2, 128), i32),
            pltpu.SMEM((2, 128), i32),
            pltpu.VMEM((128, 1, 128), i32),
            pltpu.VMEM((128, 1, 128), i32),
            pltpu.VMEM((4096, 1, 128), f32),
            pltpu.VMEM((4096, 1, 128), f32),
            pltpu.VMEM((2048, 1, 128), f32),
            pltpu.VMEM((2048, 1, 128), f32),
            pltpu.VMEM((16, 128), i32),
            pltpu.SMEM((16, 128), i32),
            pltpu.VMEM((128, 128), bf16),
            pltpu.VMEM((128, 128), f32),
            pltpu.VMEM((1, 1, 128), f32),
            pltpu.VMEM((128, 1, 128), f32),
            pltpu.VMEM((15, 256, 128), bf16),
            pltpu.VMEM((KEPT, 128, 128), f32),
            pltpu.VMEM((16, 128, 128), f32),
            pltpu.VMEM((9, 128, 128), f32),
            pltpu.VMEM((96, 1, 128), f32),
            halo,
            halo,
            halo,
            pltpu.VMEM((16, 128, 128), f32),
            pltpu.SemaphoreType.DMA((18,)),
            pltpu.SemaphoreType.DMA((11,)),
            pltpu.SemaphoreType.REGULAR,
            pltpu.SemaphoreType.REGULAR,
        ],
        compiler_params=pltpu.CompilerParams(collective_id=0, has_side_effects=True),
    )(
        view,
        dest_row.reshape(2, 128),
        neighbours,
        orientation,
        wall_flags,
        bulk_modulus[None, :],
        density[None, :],
        jnp.asarray(picks, bf16),
        jnp.asarray(inside),
    )
    return result.reshape(128, 4, 4, 128).transpose(0, 2, 1, 3).reshape(128, 4, 512)


def solution(mesh):
    in_specs = (
        P(("grp", "dev"), None, None),
        P(("grp", "dev")),
        P(None, ("grp", "dev")),
        P(None, ("grp", "dev")),
        P(None, ("grp", "dev")),
        P(("grp", "dev")),
        P(("grp", "dev")),
    )
    out_specs = P(("grp", "dev"), None, None)
    return jax.shard_map(body, mesh=mesh, in_specs=in_specs, out_specs=out_specs, check_vma=False)
```

```python
import jax
import jax.numpy as jnp
import numpy as np
from jax import lax
from jax.experimental import pallas as pl
from jax.experimental.pallas import tpu as pltpu
from jax.sharding import PartitionSpec as P

NP = 8
MESH = pl.DeviceIdType.MESH
HIGHEST = lax.Precision.HIGHEST

metric_scale = 0.25


def gll_tables(poly_order):
    num_points = poly_order + 1
    points = -np.cos(np.pi * np.arange(num_points) / poly_order)
    legendre = np.zeros((num_points, num_points))
    for sweeps in range(101):
        legendre[:, 0] = 1.0
        legendre[:, 1] = points
        for degree in range(2, num_points):
            legendre[:, degree] = (
                (2 * degree - 1) * points * legendre[:, degree - 1]
                - (degree - 1) * legendre[:, degree - 2]
            ) / degree
        if sweeps < 100:
            points = points - (points * legendre[:, poly_order] - legendre[:, poly_order - 1]) / (
                num_points * legendre[:, poly_order]
            )
    end_values = legendre[:, poly_order]
    weights = 2.0 / (poly_order * num_points * end_values**2)
    distance = points[:, None] - points[None, :] + np.eye(num_points)
    derivative = end_values[:, None] / end_values[None, :] / distance
    derivative = derivative * (1.0 - np.eye(num_points))
    derivative[0, 0] = -poly_order * num_points / 4.0
    derivative[poly_order, poly_order] = poly_order * num_points / 4.0
    return (points, weights, derivative)


def fixed_tables():
    derivative = gll_tables(NP - 1)[2]
    take = np.zeros((2, 4, 128, 128))
    for end in range(2):
        for first in range(8):
            for second in range(8):
                face_lane = 64 * end + 8 * first + second
                half, chunk = 64 * (first % 2), first // 2
                take[0, chunk, half + 56 * end + second, face_lane] = 1.0
                take[1, chunk, half + 8 * second + 7 * end, face_lane] = 1.0
    turns = np.zeros((3, 128, 128))
    for end in range(2):
        for first in range(8):
            for second in range(8):
                to = 64 * end + 8 * first + second
                turns[0, 64 * end + 8 * (7 - first) + second, to] = 1.0
                turns[1, 64 * end + 8 * first + 7 - second, to] = 1.0
                turns[2, 64 * end + 8 * second + first, to] = 1.0
    eye2, eye8 = np.eye(2), np.eye(8)
    inside = [
        np.kron(eye2, np.kron(derivative.T, eye8)),
        np.kron(eye2, np.kron(eye8, derivative.T)),
    ]
    lift = np.swapaxes(take, 2, 3)
    stack = [take.reshape(8, 128, 128), lift.reshape(8, 128, 128), turns]
    comes_from = np.full((128, 128), -1.0)
    for number, step in enumerate(NEARBY):
        for device in range(128):
            place = device // 32, device // 8 % 4, device // 2 % 4, device % 2
            back = [(at - by) % size for at, by, size in zip(place, step, (4, 4, 4, 2))]
            comes_from[number, device] = back[0] * 32 + back[1] * 8 + back[2] * 2 + back[3]
    return np.concatenate(stack), np.stack(inside + [comes_from]).astype(np.float32)


TAKE, LIFT, TURN = 0, 8, 16
NEAR, FAR, GIVE, ROUTE, OWNER = 0, 3, 6, 9, 12
CODE, WALL, Z_IN, BULK, THIN, SPOT, KEPT = 0, 3, 6, 7, 8, 9, 12

STEPS = sorted(
    [(a, b, c, d) for a in range(4) for b in range(4) for c in range(4) for d in range(2)][1:],
    key=lambda step: -sum(min(part, 4 - part) for part in step[:3]),
)
NEARBY = [(0, 0, 0, 0)] + STEPS[::-1][:31]


def my_place():
    group = lax.axis_index("grp")
    member = lax.axis_index("dev")
    return group, member // 8, (member // 2) % 4, member % 2


def chip_at(place, step):
    z_at, y_at, x_at, _ = place
    x_to = (x_at + step) % 4
    y_to = (y_at + step // 4 + step) % 4
    z_to = (z_at + step // 16 + step // 4 + step) % 4
    return z_to, y_to * 4 + x_to


def split3(value):
    high = value.astype(jnp.bfloat16)
    rest = value - high.astype(jnp.float32)
    middle = rest.astype(jnp.bfloat16)
    low = (rest - middle.astype(jnp.float32)).astype(jnp.bfloat16)
    return high, middle, low


def pick_rows(chosen, value):
    wide = value.shape[1]
    parts = jnp.concatenate(split3(value), axis=1)
    found = jnp.dot(chosen, parts, preferred_element_type=jnp.float32)
    return found[:, :wide] + found[:, wide : 2 * wide] + found[:, 2 * wide :]


def pick_lanes(value, chosen):
    tall = value.shape[0]
    parts = jnp.concatenate(split3(value), axis=0)
    found = jnp.dot(parts, chosen, preferred_element_type=jnp.float32)
    return found[:tall] + found[tall : 2 * tall] + found[2 * tall :]


def exact(left, right):
    return jnp.dot(left, right, precision=HIGHEST, preferred_element_type=jnp.float32)


def count(left, right):
    return jnp.dot(
        left.astype(jnp.bfloat16), right.astype(jnp.bfloat16), preferred_element_type=jnp.float32
    )


def order_slots(dest_row, stack, ranks):
    lane = lax.broadcasted_iota(jnp.int32, (128, 128), 1)
    sub = lax.broadcasted_iota(jnp.int32, (128, 128), 0)
    value = dest_row.astype(jnp.float32)
    stack[0:2, :] = value
    columns = stack[...].T
    rows = [value[0:1, :], value[1:2, :]]
    slots = []
    for half in range(2):
        mine = columns[:, half : half + 1]
        below = jnp.zeros((128, 128), jnp.float32)
        for other in range(2):
            tied = rows[other] == mine
            if other > half:
                less = rows[other] < mine
            elif other < half:
                less = (rows[other] < mine) | tied
            else:
                less = (rows[other] < mine) | (tied & (lane < sub))
            below = below + jnp.where(less, 1.0, 0.0)
        slots.append((mine, jnp.sum(below, axis=1, keepdims=True)))
    lane_f = lane.astype(jnp.float32)
    sub_f = sub.astype(jnp.float32)
    for half in range(2):
        found = jnp.zeros((1, 128), jnp.float32)
        for part in range(2):
            is_it = slots[part][1] == lane_f + 128.0 * half
            found = found + jnp.sum(
                jnp.where(is_it, sub_f + 128.0 * part, 0.0), axis=0, keepdims=True
            )
        ranks[half : half + 1, :] = jnp.clip(found.astype(jnp.int32), 0, 255)
    return rows, slots


def write_notes(rows, slots, near_rows, wall_rows, mine, note_out):
    lane = lax.broadcasted_iota(jnp.int32, (128, 128), 1)
    sub = lax.broadcasted_iota(jnp.int32, (128, 128), 0)
    lane_f = lane.astype(jnp.float32)
    sub_f = sub.astype(jnp.float32)
    note = jnp.zeros((128, 128), jnp.float32)
    heads = jnp.zeros((1, 128), jnp.float32)
    for half in range(2):
        row = rows[half].astype(jnp.int32)
        owner_row = jnp.where(row >= 0, row // 128, -1)
        to = jnp.where(owner_row == sub, 1.0, 0.0)
        mine_f, rank = slots[half]
        column = mine_f.astype(jnp.int32)
        rank_i = rank.astype(jnp.int32)
        owner = jnp.where(column >= 0, column // 128, -1).astype(jnp.float32)
        inside = (column % 128 + 1).astype(jnp.float32)
        ids = jnp.where((rank_i % 8) == lane, inside, 0.0)
        note = note + count(to, ids)
        heads = heads + jnp.sum(
            jnp.where(rank_i == 8 * (lane - 32), owner, 0.0), axis=0, keepdims=True
        )
    owners = near_rows // 128
    beside = jnp.where((owners != mine) & (wall_rows == 0), owners + 1, 0).astype(jnp.float32)
    beside = jnp.max(beside, axis=1, keepdims=True)
    beside = jnp.sum(
        jnp.where(lane_f[:6] == sub_f[:6] + 8.0, beside, 0.0), axis=0, keepdims=True
    )
    heads = jnp.where((lane[:1] >= 32) & (lane[:1] < 64), heads, 0.0)
    note_out.reshape(128, 128)[...] = (note + heads + beside).astype(jnp.int32)


def prepare(
    mine, near_rows, turn_rows, wall_rows, bulk_row, dens_row, comes_from, stack, moves, kept
):
    lane = lax.broadcasted_iota(jnp.int32, (128, 128), 1)
    sub = lax.broadcasted_iota(jnp.int32, (128, 128), 0)
    away_rows = jnp.where((near_rows // 128 != mine) & (wall_rows == 0), 1.0, 0.0)
    stack[0:6, :] = near_rows.astype(jnp.float32)
    stack[8:14, :] = turn_rows.astype(jnp.float32)
    stack[16:22, :] = wall_rows.astype(jnp.float32)
    stack[24:25, :] = bulk_row
    stack[25:26, :] = dens_row
    stack[26:32, :] = away_rows
    columns = stack[...].T
    give_rank = count(stack[24:32, :], (sub < lane).astype(jnp.float32))
    base = (mine * 128).astype(jnp.float32)
    lane_f = lane.astype(jnp.float32)
    sub_f = sub.astype(jnp.float32)
    owners = near_rows // 128
    beside = jnp.where(away_rows > 0.0, owners + 1, 0).astype(jnp.float32)
    beside = jnp.max(beside, axis=1, keepdims=True) - 1.0
    for face in range(6):
        axis, half = face // 2, face % 2
        near = columns[:, face : face + 1]
        away = columns[:, 26 + face : 27 + face]
        away_row = away_rows[face : face + 1, :]
        is_near = (near - base == lane_f) & (away == 0.0)
        before = jnp.where((near_rows[face : face + 1, :].astype(jnp.float32) < near), away_row, 0.0)
        take_rank = jnp.sum(before, axis=1, keepdims=True)
        is_far = jnp.where((take_rank == lane_f) & (away > 0.0), 1.0, 0.0)
        passed_by = jnp.where(comes_from == beside[face : face + 1, :], 1.0, 0.0)
        is_given = (give_rank[2 + face : 3 + face, :] == sub_f[:32]) & (away_row > 0.0)
        rows = pl.ds(128 * half, 128)
        moves[NEAR + axis, rows] = jnp.where(is_near, 1.0, 0.0).astype(jnp.bfloat16)
        moves[FAR + axis, rows] = count(is_far[:, :32], passed_by).astype(jnp.bfloat16)
        moves[GIVE + axis, pl.ds(32 * (1 - half), 32)] = jnp.where(is_given, 1.0, 0.0).astype(
            jnp.bfloat16
        )
        near_i = near.astype(jnp.int32)
        moves[OWNER + axis, rows] = jnp.where(near_i // 128 == lane, 1.0, 0.0).astype(jnp.bfloat16)
        kept[SPOT + axis, :, 64 * half : 64 * half + 64] = jnp.broadcast_to(
            (near_i % 128).astype(jnp.float32), (128, 64)
        )
    low = lane < 64
    for axis in range(3):
        kept[CODE + axis] = jnp.where(
            low, columns[:, 8 + 2 * axis : 9 + 2 * axis], columns[:, 9 + 2 * axis : 10 + 2 * axis]
        )
        kept[WALL + axis] = jnp.where(
            low, columns[:, 16 + 2 * axis : 17 + 2 * axis], columns[:, 17 + 2 * axis : 18 + 2 * axis]
        )
    bulk = jnp.broadcast_to(columns[:, 24:25], (128, 128))
    dens = jnp.broadcast_to(columns[:, 25:26], (128, 128))
    kept[Z_IN] = jnp.sqrt(bulk * dens)
    kept[BULK] = bulk
    kept[THIN] = 1.0 / dens


def exchange_kernel(
    state_ref, dest_ref, near_ref, turn_ref, wall_ref, bulk_ref, dens_ref, fixed_ref, inside_ref,
    out_ref, state, dest, near, turn, wall, bulk, dens, fixed, inside, ranks, slot_of, note_out,
    notes, sends, first, second, third, table, index, perm, stack, z_here, z_all, moves, kept, field,
    traces, ask, ask_in, answer, answer_in, total, sems, loads, met_y, met_z,
):
    place = my_place()
    z_at, y_at, x_at, core = place
    member_here = lax.axis_index("dev")
    mine = z_at * 32 + member_here
    barrier = pltpu.get_barrier_semaphore()

    def signal(sem, group, y_to, x_to, core_to):
        pl.semaphore_signal(
            sem, inc=1, device_id=(group, (y_to * 4 + x_to) * 2 + core_to), device_id_type=MESH
        )

    for step in range(1, 8):
        signal(barrier, z_at, y_at, (x_at + step // 2) % 4, (core + step) % 2)
    for step in range(1, 4):
        signal(barrier, z_at, (y_at + step) % 4, x_at, core)
        signal(barrier, (z_at + step) % 4, y_at, x_at, core)

    pairs = [
        (dest_ref, dest), (near_ref, near), (wall_ref, wall), (turn_ref, turn),
        (bulk_ref, bulk), (dens_ref, dens), (state_ref, state), (fixed_ref, fixed),
        (inside_ref, inside),
    ]
    local = [pltpu.make_async_copy(a, b, loads.at[n]) for n, (a, b) in enumerate(pairs)]
    for one in local:
        one.start()
    stack[...] = jnp.zeros((128, 128), jnp.float32)
    local[0].wait()
    rows, slots = order_slots(dest[...], stack, ranks)
    to_slots = pltpu.make_async_copy(ranks, slot_of, loads.at[9])
    to_slots.start()
    pl.semaphore_wait(barrier, 13)
    for step in range(1, 4):
        signal(met_y, z_at, (y_at + step) % 4, x_at, core)
    local[1].wait()
    local[2].wait()
    write_notes(rows, slots, near[...], wall[...], mine, note_out)
    pl.semaphore_wait(met_y, 3)
    for step in range(1, 4):
        signal(met_z, (z_at + step) % 4, y_at, x_at, core)
    to_slots.wait()
    local[6].wait()

    def gather_first(target, base, at):
        row, chunk = at // 16, at % 16
        found = []
        for k in range(32):
            slot = slot_of[k // 16, (k % 16) * 8 + row]
            found.append(state[pl.ds(slot * 16 + chunk, 1)])
        for k in range(32):
            target[pl.ds(base + k, 1)] = found[k]

    def to_device(step):
        chip_step = jnp.where(step > 63, step - 63, step)
        side = jnp.where(step == 0, 1 - core, step // 64)
        group, chip = chip_at(place, chip_step)
        return group, chip * 2 + side

    def copy(source, target, phase, group, member):
        pltpu.make_async_remote_copy(
            src_ref=source,
            dst_ref=target,
            send_sem=sems.at[2 * phase],
            recv_sem=sems.at[2 * phase + 1],
            device_id=(group, member),
            device_id_type=MESH,
        ).start()

    def finish(buffer, rows, which):
        view = buffer.at[pl.ds(0, rows)]
        pltpu.make_async_copy(view, view, sems.at[which]).wait()

    def fetch(step):
        group, member = to_device(step)
        at = group * 32 + member
        gather_first(sends, at * 32, at)

    def spread(step, leaves):
        group, member = to_device(step)
        at = group * 32 + member
        pltpu.make_async_remote_copy(
            src_ref=sends.at[pl.ds(at * 32, 32)],
            dst_ref=first.at[pl.ds(mine * 32, 32)],
            send_sem=sems.at[leaves],
            recv_sem=sems.at[16 + member % 2],
            device_id=(group, member),
            device_id_type=MESH,
        ).start()

    def tell(group, member):
        at = group * 32 + member
        copy(note_out.at[pl.ds(at, 1)], notes.at[pl.ds(mine, 1)], 0, group, member)

    fetch(0)
    fetch(1)
    pl.semaphore_wait(met_z, 3)
    spread(0, 2)
    tell(z_at, member_here + 1 - 2 * core)

    def early(step, carry):
        fetch(step + 1)
        spread(step, 12)
        group, chip = chip_at(place, step)
        tell(group, chip * 2)
        tell(group, chip * 2 + 1)
        return carry

    lax.fori_loop(1, 64, early, 0)

    def late(step, carry):
        spread(step, 14)
        fetch(step + 1)
        return carry

    local[3].wait()
    local[4].wait()
    local[5].wait()
    local[8].wait()
    z_here[...] = jnp.sqrt(bulk[...] * dens[...]).reshape(1, 1, 128)
    z_all[pl.ds(mine, 1)] = z_here[...]

    ask_in[...] = jnp.zeros((384, 1, 128), jnp.float32)
    finish(first, 63 * 32, 12)
    lax.fori_loop(64, 126, late, 0)
    spread(126, 14)
    gather_first(first, mine * 32, mine)
    notes[pl.ds(mine, 1)] = note_out[pl.ds(mine, 1)]

    finish(notes, 127, 1)
    note = notes.reshape(128, 128)[...]
    lane = lax.broadcasted_iota(jnp.int32, (128, 128), 1)
    sub = lax.broadcasted_iota(jnp.int32, (128, 128), 0)
    lower = (lane < sub).astype(jnp.float32)
    piece = jnp.zeros((128, 128), jnp.int32)
    for k in range(32):
        piece = piece + jnp.where(note[:, 32 + k : 33 + k] == lane, k + 1, 0)
    valid = piece > 0
    rank = count(lower, valid.astype(jnp.float32)).astype(jnp.int32)
    entry = sub * 32 + piece - 1
    for j in range(16):
        chosen = jnp.sum(jnp.where(valid & (rank == j), entry, 0), axis=0, keepdims=True)
        table[j : j + 1, :] = jnp.clip(chosen, 0, 4095)
    to_index = pltpu.make_async_copy(table, index, loads.at[10])
    to_index.start()
    has = jnp.broadcast_to(note[:, 0:1] > 0, (128, 128))
    order = count(lower, has.astype(jnp.float32)).astype(jnp.int32)
    slot = jnp.where(has & (order == lane), 1.0, 0.0)[:, :16]
    rows = []
    for i in range(8):
        is_row = (note[:, i : i + 1] - 1 == lane).astype(jnp.float32)
        rows.append(
            lax.dot_general(
                slot, is_row, (((0,), (0,)), ((), ())), preferred_element_type=jnp.float32
            )
        )
    perm[...] = jnp.concatenate(rows, axis=0).T.astype(jnp.bfloat16)
    facing = note.astype(jnp.float32).T
    for face in range(6):
        to = facing[8 + face : 9 + face, :] - 1.0
        chosen = jnp.where(to == sub.astype(jnp.float32), 1.0, 0.0).astype(jnp.bfloat16)
        moves[ROUTE + face // 2, pl.ds(128 * (1 - face % 2), 128)] = chosen
    local[7].wait()
    to_index.wait()
    finish(first, 127 * 32, 16 + core)

    def gather_second(target, base, at):
        found = [first[pl.ds(index[j, at], 1)] for j in range(16)]
        for j in range(16):
            target[pl.ds(base + j, 1)] = found[j]

    def device_at(step):
        group = (z_at + step[0]) % 4
        chip = ((y_at + step[1]) % 4) * 4 + (x_at + step[2]) % 4
        return group, chip * 2 + (core + step[3]) % 2

    def forward(group, member):
        at = group * 32 + member
        copy(
            second.at[pl.ds(at * 16, 16)], third.at[pl.ds(mine * 16, 16)], 2, group, member
        )

    before = None
    for step in STEPS:
        group, member = device_at(step)
        at = group * 32 + member
        gather_second(second, at * 16, at)
        if before is not None:
            forward(*before)
        before = (group, member)
    gather_second(third, mine * 16, mine)
    forward(*before)

    def tell_z(step, carry):
        group, chip = chip_at(place, step // 2)
        copy(z_here, z_all.at[pl.ds(mine, 1)], 5, group, chip * 2 + (core + step) % 2)
        return carry

    lax.fori_loop(1, 128, tell_z, 0)
    prepare(
        mine, near[...], turn[...], wall[...], bulk[...], dens[...], inside[2, :32, :], stack,
        moves, kept,
    )
    finish(third, 127 * 16, 5)

    arrived = third.reshape(8, 16, 16, 128)
    for part in range(16):
        field[part] = pick_rows(perm[...], arrived[:, part].reshape(128, 128))

    low = lane < 64
    sign = jnp.where(low, -1.0, 1.0)
    z_in = kept[Z_IN]

    def four(which):
        return jnp.concatenate([field[4 * q + which] for q in range(4)], axis=1)

    def taken(which, axes):
        table = [
            jnp.concatenate([fixed[TAKE + 4 * (axis - 1) + q] for q in range(4)], axis=0)
            for axis in axes
        ]
        return pick_lanes(four(which), jnp.concatenate(table, axis=1))

    both = taken(0, (1, 2))
    pressures = [jnp.where(low, field[0], field[12]), both[:, :128], both[:, 128:]]
    normals = [jnp.where(low, field[1], field[13]), taken(2, (1,)), taken(3, (2,))]
    ask_rows = ask.reshape(96, 128)
    for axis in range(3):
        normal = sign * normals[axis]
        traces[3 + axis] = pressures[axis]
        traces[6 + axis] = normal
        turned = pltpu.roll(pressures[axis] + z_in * normal, 64, 1)
        traces[axis] = turned
        found = pick_rows(moves[GIVE + axis, :64], turned)
        ask_rows[pl.ds(axis, 32, stride=3), :] = jnp.where(low[:32], found[:32], found[32:])

    def three(step, number, source, target, phase):
        group, member = device_at(step)
        at = group * 32 + member if number is None else number
        copy(
            source.at[pl.ds(at * 3, 3)], target.at[pl.ds(mine * 3, 3)], phase, group, member
        )

    for number in range(31, 0, -1):
        three(NEARBY[number], number, ask, ask_in, 3)
    ask_in[pl.ds(mine * 3, 3)] = ask[pl.ds(0, 3)]

    scale = jnp.float32(-metric_scale) * kept[BULK]
    thin = jnp.float32(-metric_scale) * kept[THIN]
    derivative = gll_tables(NP - 1)[2]

    def along_x(which):
        straight = [field[4 * q + which] for q in range(4)]
        crossed = [pltpu.roll(part, 64, 1) for part in straight]
        sums = []
        for q in range(4):
            found = None
            for b in range(4):
                one = jnp.where(low, derivative[2 * q, 2 * b], derivative[2 * q + 1, 2 * b + 1])
                two = jnp.where(low, derivative[2 * q, 2 * b + 1], derivative[2 * q + 1, 2 * b])
                term = one.astype(jnp.float32) * straight[b] + two.astype(jnp.float32) * crossed[b]
                found = term if found is None else found + term
            sums.append(found)
        return sums

    side_x = along_x(1)
    grad_x = along_x(0)
    for q in range(4):
        total[4 * q] = side_x[q]
        total[4 * q + 1] = thin * grad_x[q]

    finish(ask_in, 93, 7)
    asked = ask_in.reshape(384, 128)
    answer_rows = answer.reshape(384, 128)
    for axis in range(3):
        found = pick_rows(moves[ROUTE + axis], asked[pl.ds(axis, 128, stride=3), :])
        answer_rows[pl.ds(axis, 128, stride=3), :] = jnp.where(low, found[:128], found[128:])
    for step in STEPS:
        three(step, None, answer, answer_in, 4)
    answer_in[pl.ds(mine * 3, 3)] = answer[pl.ds(mine * 3, 3)]

    finish(z_all, 127, 11)
    z_table = z_all.reshape(128, 128)[...]
    lane_f = lane.astype(jnp.float32)
    for axis in range(3):
        found = pick_rows(moves[OWNER + axis], z_table)
        sides = []
        for half in range(2):
            spot = kept[SPOT + axis, :, 64 * half : 64 * half + 1]
            sides.append(
                jnp.sum(
                    jnp.where(lane_f == spot, found[128 * half : 128 * half + 128], 0.0),
                    axis=1,
                    keepdims=True,
                )
            )
        kept[SPOT + axis] = jnp.where(low, sides[0], sides[1])
        found = pick_rows(moves[NEAR + axis], traces[axis])
        traces[axis] = jnp.where(low, found[:128], found[128:])

    def stacked(which):
        return jnp.concatenate([field[4 * q + which] for q in range(4)], axis=0)

    side_y = exact(stacked(2), inside[0])
    side_z = exact(stacked(3), inside[1])
    grad_y = exact(stacked(0), inside[0])
    grad_z = exact(stacked(0), inside[1])
    for q in range(4):
        rows = slice(128 * q, 128 * q + 128)
        total[4 * q] = scale * (total[4 * q] + side_y[rows] + side_z[rows])
        total[4 * q + 2] = thin * grad_y[rows]
        total[4 * q + 3] = thin * grad_z[rows]

    finish(answer_in, 381, 9)
    answers = answer_in.reshape(384, 128)
    coming = []
    for axis in range(3):
        found = pick_rows(moves[FAR + axis], answers[pl.ds(axis, 128, stride=3), :])
        coming.append(traces[axis] + jnp.where(low, found[:128], found[128:]))
    coming = jnp.concatenate(coming, axis=0)
    code = jnp.concatenate([kept[CODE + axis] for axis in range(3)], axis=0).astype(jnp.int32)
    coming = jnp.where(code % 2 == 1, pick_lanes(coming, fixed[TURN]), coming)
    coming = jnp.where(code // 2 % 2 == 1, pick_lanes(coming, fixed[TURN + 1]), coming)
    coming = jnp.where(code >= 4, pick_lanes(coming, fixed[TURN + 2]), coming)
    lift = jnp.float32(metric_scale / float(gll_tables(NP - 1)[1][0]))
    gains = []
    for axis in range(3):
        is_wall = kept[WALL + axis] == 1.0
        normal = traces[6 + axis]
        z_out = jnp.where(is_wall, z_in, kept[SPOT + axis])
        other = coming[128 * axis : 128 * axis + 128]
        jump = jnp.where(
            is_wall, 2.0 * z_in * normal, other - traces[3 + axis] + z_out * normal
        )
        jump = lift * jump / (z_in + z_out)
        gains.append(jnp.concatenate([kept[BULK] * jump, -sign * kept[THIN] * z_in * jump]))
    lifted = []
    for axis in (1, 2):
        wide = jnp.concatenate([fixed[LIFT + 4 * (axis - 1) + q] for q in range(4)], axis=1)
        lifted.append(pick_lanes(gains[axis], wide))
    for q in range(4):
        lanes = slice(128 * q, 128 * q + 128)
        part = total[4 * q] + lifted[0][:128, lanes] + lifted[1][:128, lanes]
        part_x = total[4 * q + 1]
        if q in (0, 3):
            keep = low if q == 0 else lane >= 64
            part = part + jnp.where(keep, gains[0][:128], 0.0)
            part_x = part_x + jnp.where(keep, gains[0][128:], 0.0)
        out_ref[pl.ds(4 * q, 128, stride=16), :] = part
        out_ref[pl.ds(4 * q + 1, 128, stride=16), :] = part_x
        out_ref[pl.ds(4 * q + 2, 128, stride=16), :] = total[4 * q + 2] + lifted[0][128:, lanes]
        out_ref[pl.ds(4 * q + 3, 128, stride=16), :] = total[4 * q + 3] + lifted[1][128:, lanes]
    finish(notes, 127, 0)
    finish(first, 32, 2)
    finish(first, 63 * 32, 14)
    finish(z_all, 127, 10)
    finish(third, 127 * 16, 4)
    finish(ask_in, 93, 6)
    finish(answer_in, 381, 8)


def body(old_state, dest_row, neighbours, orientation, wall_flags, bulk_modulus, density):
    view = old_state.reshape(256, 4, 4, 128).transpose(0, 2, 1, 3).reshape(4096, 1, 128)
    picks, inside = fixed_tables()
    f32, i32, bf16 = jnp.float32, jnp.int32, jnp.bfloat16
    halo = pltpu.VMEM((384, 1, 128), f32)
    result = pl.pallas_call(
        exchange_kernel,
        out_shape=jax.ShapeDtypeStruct((2048, 128), f32),
        in_specs=[pl.BlockSpec(memory_space=pl.ANY)] * 9,
        out_specs=pl.BlockSpec(memory_space=pltpu.VMEM),
        scratch_shapes=[
            pltpu.VMEM((4096, 1, 128), f32),
            pltpu.VMEM((2, 128), i32),
            pltpu.VMEM((6, 128), i32),
            pltpu.VMEM((6, 128), i32),
            pltpu.VMEM((6, 128), i32),
            pltpu.VMEM((1, 128), f32),
            pltpu.VMEM((1, 128), f32),
            pltpu.VMEM((19, 128, 128), bf16),
            pltpu.VMEM((3, 128, 128), f32),
            pltpu.VMEM((2, 128), i32),
            pltpu.SMEM((2, 128), i32),
            pltpu.VMEM((128, 1, 128), i32),
            pltpu.VMEM((128, 1, 128), i32),
            pltpu.VMEM((4096, 1, 128), f32),
            pltpu.VMEM((4096, 1, 128), f32),
            pltpu.VMEM((2048, 1, 128), f32),
            pltpu.VMEM((2048, 1, 128), f32),
            pltpu.VMEM((16, 128), i32),
            pltpu.SMEM((16, 128), i32),
            pltpu.VMEM((128, 128), bf16),
            pltpu.VMEM((128, 128), f32),
            pltpu.VMEM((1, 1, 128), f32),
            pltpu.VMEM((128, 1, 128), f32),
            pltpu.VMEM((15, 256, 128), bf16),
            pltpu.VMEM((KEPT, 128, 128), f32),
            pltpu.VMEM((16, 128, 128), f32),
            pltpu.VMEM((9, 128, 128), f32),
            pltpu.VMEM((96, 1, 128), f32),
            halo,
            halo,
            halo,
            pltpu.VMEM((16, 128, 128), f32),
            pltpu.SemaphoreType.DMA((18,)),
            pltpu.SemaphoreType.DMA((11,)),
            pltpu.SemaphoreType.REGULAR,
            pltpu.SemaphoreType.REGULAR,
        ],
        compiler_params=pltpu.CompilerParams(collective_id=0, has_side_effects=True),
    )(
        view,
        dest_row.reshape(2, 128),
        neighbours,
        orientation,
        wall_flags,
        bulk_modulus[None, :],
        density[None, :],
        jnp.asarray(picks, bf16),
        jnp.asarray(inside),
    )
    return result.reshape(128, 4, 4, 128).transpose(0, 2, 1, 3).reshape(128, 4, 512)


def solution(mesh):
    in_specs = (
        P(("grp", "dev"), None, None),
        P(("grp", "dev")),
        P(None, ("grp", "dev")),
        P(None, ("grp", "dev")),
        P(None, ("grp", "dev")),
        P(("grp", "dev")),
        P(("grp", "dev")),
    )
    out_specs = P(("grp", "dev"), None, None)
    return jax.shard_map(body, mesh=mesh, in_specs=in_specs, out_specs=out_specs, check_vma=False)
```

```python
import jax
import jax.numpy as jnp
import numpy as np
from jax import lax
from jax.experimental import pallas as pl
from jax.experimental.pallas import tpu as pltpu
from jax.sharding import PartitionSpec as P

NP = 8
MESH = pl.DeviceIdType.MESH
HIGHEST = lax.Precision.HIGHEST

metric_scale = 0.25


def gll_tables(poly_order):
    num_points = poly_order + 1
    points = -np.cos(np.pi * np.arange(num_points) / poly_order)
    legendre = np.zeros((num_points, num_points))
    for sweeps in range(101):
        legendre[:, 0] = 1.0
        legendre[:, 1] = points
        for degree in range(2, num_points):
            legendre[:, degree] = (
                (2 * degree - 1) * points * legendre[:, degree - 1]
                - (degree - 1) * legendre[:, degree - 2]
            ) / degree
        if sweeps < 100:
            points = points - (points * legendre[:, poly_order] - legendre[:, poly_order - 1]) / (
                num_points * legendre[:, poly_order]
            )
    end_values = legendre[:, poly_order]
    weights = 2.0 / (poly_order * num_points * end_values**2)
    distance = points[:, None] - points[None, :] + np.eye(num_points)
    derivative = end_values[:, None] / end_values[None, :] / distance
    derivative = derivative * (1.0 - np.eye(num_points))
    derivative[0, 0] = -poly_order * num_points / 4.0
    derivative[poly_order, poly_order] = poly_order * num_points / 4.0
    return (points, weights, derivative)


def fixed_tables():
    derivative = gll_tables(NP - 1)[2]
    take = np.zeros((2, 4, 128, 128))
    for end in range(2):
        for first in range(8):
            for second in range(8):
                face_lane = 64 * end + 8 * first + second
                half, chunk = 64 * (first % 2), first // 2
                take[0, chunk, half + 56 * end + second, face_lane] = 1.0
                take[1, chunk, half + 8 * second + 7 * end, face_lane] = 1.0
    turns = np.zeros((3, 128, 128))
    for end in range(2):
        for first in range(8):
            for second in range(8):
                to = 64 * end + 8 * first + second
                turns[0, 64 * end + 8 * (7 - first) + second, to] = 1.0
                turns[1, 64 * end + 8 * first + 7 - second, to] = 1.0
                turns[2, 64 * end + 8 * second + first, to] = 1.0
    eye2, eye8 = np.eye(2), np.eye(8)
    inside = [
        np.kron(eye2, np.kron(derivative.T, eye8)),
        np.kron(eye2, np.kron(eye8, derivative.T)),
    ]
    lift = np.swapaxes(take, 2, 3)
    stack = [take.reshape(8, 128, 128), lift.reshape(8, 128, 128), turns]
    comes_from = np.full((128, 128), -1.0)
    for number, step in enumerate(NEARBY):
        for device in range(128):
            place = device // 32, device // 8 % 4, device // 2 % 4, device % 2
            back = [(at - by) % size for at, by, size in zip(place, step, (4, 4, 4, 2))]
            comes_from[number, device] = back[0] * 32 + back[1] * 8 + back[2] * 2 + back[3]
    return np.concatenate(stack), np.stack(inside + [comes_from]).astype(np.float32)


TAKE, LIFT, TURN = 0, 8, 16
NEAR, FAR, GIVE, ROUTE, OWNER = 0, 3, 6, 9, 12
CODE, WALL, Z_IN, BULK, THIN, SPOT, KEPT = 0, 3, 6, 7, 8, 9, 12

STEPS = sorted(
    [(a, b, c, d) for a in range(4) for b in range(4) for c in range(4) for d in range(2)][1:],
    key=lambda step: -sum(min(part, 4 - part) for part in step[:3]),
)
NEARBY = [(0, 0, 0, 0)] + STEPS[::-1][:31]


def my_place():
    group = lax.axis_index("grp")
    member = lax.axis_index("dev")
    return group, member // 8, (member // 2) % 4, member % 2


def chip_at(place, step):
    z_at, y_at, x_at, _ = place
    step = step * 37 % 64
    x_to = (x_at + step) % 4
    y_to = (y_at + step // 4) % 4
    z_to = (z_at + step // 16) % 4
    return z_to, y_to * 4 + x_to


def split3(value):
    high = value.astype(jnp.bfloat16)
    rest = value - high.astype(jnp.float32)
    middle = rest.astype(jnp.bfloat16)
    low = (rest - middle.astype(jnp.float32)).astype(jnp.bfloat16)
    return high, middle, low


def pick_rows(chosen, value):
    wide = value.shape[1]
    parts = jnp.concatenate(split3(value), axis=1)
    found = jnp.dot(chosen, parts, preferred_element_type=jnp.float32)
    return found[:, :wide] + found[:, wide : 2 * wide] + found[:, 2 * wide :]


def pick_lanes(value, chosen):
    tall = value.shape[0]
    parts = jnp.concatenate(split3(value), axis=0)
    found = jnp.dot(parts, chosen, preferred_element_type=jnp.float32)
    return found[:tall] + found[tall : 2 * tall] + found[2 * tall :]


def exact(left, right):
    return jnp.dot(left, right, precision=HIGHEST, preferred_element_type=jnp.float32)


def count(left, right):
    return jnp.dot(
        left.astype(jnp.bfloat16), right.astype(jnp.bfloat16), preferred_element_type=jnp.float32
    )


def order_slots(dest_row, stack, ranks):
    lane = lax.broadcasted_iota(jnp.int32, (128, 128), 1)
    sub = lax.broadcasted_iota(jnp.int32, (128, 128), 0)
    value = dest_row.astype(jnp.float32)
    stack[0:2, :] = value
    columns = stack[...].T
    rows = [value[0:1, :], value[1:2, :]]
    slots = []
    for half in range(2):
        mine = columns[:, half : half + 1]
        below = jnp.zeros((128, 128), jnp.float32)
        for other in range(2):
            tied = rows[other] == mine
            if other > half:
                less = rows[other] < mine
            elif other < half:
                less = (rows[other] < mine) | tied
            else:
                less = (rows[other] < mine) | (tied & (lane < sub))
            below = below + jnp.where(less, 1.0, 0.0)
        slots.append((mine, jnp.sum(below, axis=1, keepdims=True)))
    lane_f = lane.astype(jnp.float32)
    sub_f = sub.astype(jnp.float32)
    for half in range(2):
        found = jnp.zeros((1, 128), jnp.float32)
        for part in range(2):
            is_it = slots[part][1] == lane_f + 128.0 * half
            found = found + jnp.sum(
                jnp.where(is_it, sub_f + 128.0 * part, 0.0), axis=0, keepdims=True
            )
        ranks[half : half + 1, :] = jnp.clip(found.astype(jnp.int32), 0, 255)
    return rows, slots


def write_notes(rows, slots, near_rows, wall_rows, mine, note_out):
    lane = lax.broadcasted_iota(jnp.int32, (128, 128), 1)
    sub = lax.broadcasted_iota(jnp.int32, (128, 128), 0)
    lane_f = lane.astype(jnp.float32)
    sub_f = sub.astype(jnp.float32)
    note = jnp.zeros((128, 128), jnp.float32)
    heads = jnp.zeros((1, 128), jnp.float32)
    for half in range(2):
        row = rows[half].astype(jnp.int32)
        owner_row = jnp.where(row >= 0, row // 128, -1)
        to = jnp.where(owner_row == sub, 1.0, 0.0)
        mine_f, rank = slots[half]
        column = mine_f.astype(jnp.int32)
        rank_i = rank.astype(jnp.int32)
        owner = jnp.where(column >= 0, column // 128, -1).astype(jnp.float32)
        inside = (column % 128 + 1).astype(jnp.float32)
        ids = jnp.where((rank_i % 8) == lane, inside, 0.0)
        note = note + count(to, ids)
        heads = heads + jnp.sum(
            jnp.where(rank_i == 8 * (lane - 32), owner, 0.0), axis=0, keepdims=True
        )
    owners = near_rows // 128
    beside = jnp.where((owners != mine) & (wall_rows == 0), owners + 1, 0).astype(jnp.float32)
    beside = jnp.max(beside, axis=1, keepdims=True)
    beside = jnp.sum(
        jnp.where(lane_f[:6] == sub_f[:6] + 8.0, beside, 0.0), axis=0, keepdims=True
    )
    heads = jnp.where((lane[:1] >= 32) & (lane[:1] < 64), heads, 0.0)
    note_out.reshape(128, 128)[...] = (note + heads + beside).astype(jnp.int32)


def prepare(
    mine, near_rows, turn_rows, wall_rows, bulk_row, dens_row, comes_from, stack, moves, kept
):
    lane = lax.broadcasted_iota(jnp.int32, (128, 128), 1)
    sub = lax.broadcasted_iota(jnp.int32, (128, 128), 0)
    away_rows = jnp.where((near_rows // 128 != mine) & (wall_rows == 0), 1.0, 0.0)
    stack[0:6, :] = near_rows.astype(jnp.float32)
    stack[8:14, :] = turn_rows.astype(jnp.float32)
    stack[16:22, :] = wall_rows.astype(jnp.float32)
    stack[24:25, :] = bulk_row
    stack[25:26, :] = dens_row
    stack[26:32, :] = away_rows
    columns = stack[...].T
    give_rank = count(stack[24:32, :], (sub < lane).astype(jnp.float32))
    base = (mine * 128).astype(jnp.float32)
    lane_f = lane.astype(jnp.float32)
    sub_f = sub.astype(jnp.float32)
    owners = near_rows // 128
    beside = jnp.where(away_rows > 0.0, owners + 1, 0).astype(jnp.float32)
    beside = jnp.max(beside, axis=1, keepdims=True) - 1.0
    for face in range(6):
        axis, half = face // 2, face % 2
        near = columns[:, face : face + 1]
        away = columns[:, 26 + face : 27 + face]
        away_row = away_rows[face : face + 1, :]
        is_near = (near - base == lane_f) & (away == 0.0)
        before = jnp.where((near_rows[face : face + 1, :].astype(jnp.float32) < near), away_row, 0.0)
        take_rank = jnp.sum(before, axis=1, keepdims=True)
        is_far = jnp.where((take_rank == lane_f) & (away > 0.0), 1.0, 0.0)
        passed_by = jnp.where(comes_from == beside[face : face + 1, :], 1.0, 0.0)
        is_given = (give_rank[2 + face : 3 + face, :] == sub_f[:32]) & (away_row > 0.0)
        rows = pl.ds(128 * half, 128)
        moves[NEAR + axis, rows] = jnp.where(is_near, 1.0, 0.0).astype(jnp.bfloat16)
        moves[FAR + axis, rows] = count(is_far[:, :32], passed_by).astype(jnp.bfloat16)
        moves[GIVE + axis, pl.ds(32 * (1 - half), 32)] = jnp.where(is_given, 1.0, 0.0).astype(
            jnp.bfloat16
        )
        near_i = near.astype(jnp.int32)
        moves[OWNER + axis, rows] = jnp.where(near_i // 128 == lane, 1.0, 0.0).astype(jnp.bfloat16)
        kept[SPOT + axis, :, 64 * half : 64 * half + 64] = jnp.broadcast_to(
            (near_i % 128).astype(jnp.float32), (128, 64)
        )
    low = lane < 64
    for axis in range(3):
        kept[CODE + axis] = jnp.where(
            low, columns[:, 8 + 2 * axis : 9 + 2 * axis], columns[:, 9 + 2 * axis : 10 + 2 * axis]
        )
        kept[WALL + axis] = jnp.where(
            low, columns[:, 16 + 2 * axis : 17 + 2 * axis], columns[:, 17 + 2 * axis : 18 + 2 * axis]
        )
    bulk = jnp.broadcast_to(columns[:, 24:25], (128, 128))
    dens = jnp.broadcast_to(columns[:, 25:26], (128, 128))
    kept[Z_IN] = jnp.sqrt(bulk * dens)
    kept[BULK] = bulk
    kept[THIN] = 1.0 / dens


def exchange_kernel(
    state_ref, dest_ref, near_ref, turn_ref, wall_ref, bulk_ref, dens_ref, fixed_ref, inside_ref,
    out_ref, state, dest, near, turn, wall, bulk, dens, fixed, inside, ranks, slot_of, note_out,
    notes, sends, first, second, third, table, index, perm, stack, z_here, z_all, moves, kept, field,
    traces, ask, ask_in, answer, answer_in, total, sems, loads, met_y, met_z,
):
    place = my_place()
    z_at, y_at, x_at, core = place
    member_here = lax.axis_index("dev")
    mine = z_at * 32 + member_here
    barrier = pltpu.get_barrier_semaphore()

    def signal(sem, group, y_to, x_to, core_to):
        pl.semaphore_signal(
            sem, inc=1, device_id=(group, (y_to * 4 + x_to) * 2 + core_to), device_id_type=MESH
        )

    for step in range(1, 8):
        signal(barrier, z_at, y_at, (x_at + step // 2) % 4, (core + step) % 2)
    for step in range(1, 4):
        signal(barrier, z_at, (y_at + step) % 4, x_at, core)
        signal(barrier, (z_at + step) % 4, y_at, x_at, core)

    pairs = [
        (dest_ref, dest), (near_ref, near), (wall_ref, wall), (turn_ref, turn),
        (bulk_ref, bulk), (dens_ref, dens), (state_ref, state), (fixed_ref, fixed),
        (inside_ref, inside),
    ]
    local = [pltpu.make_async_copy(a, b, loads.at[n]) for n, (a, b) in enumerate(pairs)]
    for one in local:
        one.start()
    stack[...] = jnp.zeros((128, 128), jnp.float32)
    local[0].wait()
    rows, slots = order_slots(dest[...], stack, ranks)
    to_slots = pltpu.make_async_copy(ranks, slot_of, loads.at[9])
    to_slots.start()
    pl.semaphore_wait(barrier, 13)
    for step in range(1, 4):
        signal(met_y, z_at, (y_at + step) % 4, x_at, core)
    local[1].wait()
    local[2].wait()
    write_notes(rows, slots, near[...], wall[...], mine, note_out)
    pl.semaphore_wait(met_y, 3)
    for step in range(1, 4):
        signal(met_z, (z_at + step) % 4, y_at, x_at, core)
    to_slots.wait()
    local[6].wait()

    def gather_first(target, base, at):
        row, chunk = at // 16, at % 16
        found = []
        for k in range(32):
            slot = slot_of[k // 16, (k % 16) * 8 + row]
            found.append(state[pl.ds(slot * 16 + chunk, 1)])
        for k in range(32):
            target[pl.ds(base + k, 1)] = found[k]

    def to_device(step):
        chip_step = jnp.where(step > 63, step - 63, step)
        side = jnp.where(step == 0, 1 - core, step // 64)
        group, chip = chip_at(place, chip_step)
        return group, chip * 2 + side

    def copy(source, target, phase, group, member):
        pltpu.make_async_remote_copy(
            src_ref=source,
            dst_ref=target,
            send_sem=sems.at[2 * phase],
            recv_sem=sems.at[2 * phase + 1],
            device_id=(group, member),
            device_id_type=MESH,
        ).start()

    def finish(buffer, rows, which):
        view = buffer.at[pl.ds(0, rows)]
        pltpu.make_async_copy(view, view, sems.at[which]).wait()

    def fetch(step):
        group, member = to_device(step)
        at = group * 32 + member
        gather_first(sends, at * 32, at)

    def spread(step, leaves):
        group, member = to_device(step)
        at = group * 32 + member
        pltpu.make_async_remote_copy(
            src_ref=sends.at[pl.ds(at * 32, 32)],
            dst_ref=first.at[pl.ds(mine * 32, 32)],
            send_sem=sems.at[leaves],
            recv_sem=sems.at[16 + member % 2],
            device_id=(group, member),
            device_id_type=MESH,
        ).start()

    def tell(group, member):
        at = group * 32 + member
        copy(note_out.at[pl.ds(at, 1)], notes.at[pl.ds(mine, 1)], 0, group, member)

    fetch(0)
    fetch(1)
    pl.semaphore_wait(met_z, 3)
    spread(0, 2)
    tell(z_at, member_here + 1 - 2 * core)

    def early(step, carry):
        fetch(step + 1)
        spread(step, 12)
        group, chip = chip_at(place, step)
        tell(group, chip * 2)
        tell(group, chip * 2 + 1)
        return carry

    lax.fori_loop(1, 64, early, 0, unroll=3)

    def late(step, carry):
        spread(step, 14)
        fetch(step + 1)
        return carry

    local[3].wait()
    local[4].wait()
    local[5].wait()
    local[8].wait()
    z_here[...] = jnp.sqrt(bulk[...] * dens[...]).reshape(1, 1, 128)
    z_all[pl.ds(mine, 1)] = z_here[...]

    ask_in[...] = jnp.zeros((384, 1, 128), jnp.float32)
    finish(first, 63 * 32, 12)
    lax.fori_loop(64, 126, late, 0, unroll=2)
    spread(126, 14)
    gather_first(first, mine * 32, mine)
    notes[pl.ds(mine, 1)] = note_out[pl.ds(mine, 1)]

    finish(notes, 127, 1)
    note = notes.reshape(128, 128)[...]
    lane = lax.broadcasted_iota(jnp.int32, (128, 128), 1)
    sub = lax.broadcasted_iota(jnp.int32, (128, 128), 0)
    lower = (lane < sub).astype(jnp.float32)
    piece = jnp.zeros((128, 128), jnp.int32)
    for k in range(32):
        piece = piece + jnp.where(note[:, 32 + k : 33 + k] == lane, k + 1, 0)
    valid = piece > 0
    rank = count(lower, valid.astype(jnp.float32)).astype(jnp.int32)
    entry = sub * 32 + piece - 1
    for j in range(16):
        chosen = jnp.sum(jnp.where(valid & (rank == j), entry, 0), axis=0, keepdims=True)
        table[j : j + 1, :] = jnp.clip(chosen, 0, 4095)
    to_index = pltpu.make_async_copy(table, index, loads.at[10])
    to_index.start()
    has = jnp.broadcast_to(note[:, 0:1] > 0, (128, 128))
    order = count(lower, has.astype(jnp.float32)).astype(jnp.int32)
    slot = jnp.where(has & (order == lane), 1.0, 0.0)[:, :16]
    rows = []
    for i in range(8):
        is_row = (note[:, i : i + 1] - 1 == lane).astype(jnp.float32)
        rows.append(
            lax.dot_general(
                slot, is_row, (((0,), (0,)), ((), ())), preferred_element_type=jnp.float32
            )
        )
    perm[...] = jnp.concatenate(rows, axis=0).T.astype(jnp.bfloat16)
    facing = note.astype(jnp.float32).T
    for face in range(6):
        to = facing[8 + face : 9 + face, :] - 1.0
        chosen = jnp.where(to == sub.astype(jnp.float32), 1.0, 0.0).astype(jnp.bfloat16)
        moves[ROUTE + face // 2, pl.ds(128 * (1 - face % 2), 128)] = chosen
    local[7].wait()
    to_index.wait()
    finish(first, 127 * 32, 16 + core)

    def gather_second(target, base, at):
        found = [first[pl.ds(index[j, at], 1)] for j in range(16)]
        for j in range(16):
            target[pl.ds(base + j, 1)] = found[j]

    def device_at(step):
        group = (z_at + step[0]) % 4
        chip = ((y_at + step[1]) % 4) * 4 + (x_at + step[2]) % 4
        return group, chip * 2 + (core + step[3]) % 2

    def forward(group, member):
        at = group * 32 + member
        copy(
            second.at[pl.ds(at * 16, 16)], third.at[pl.ds(mine * 16, 16)], 2, group, member
        )

    before = None
    for step in STEPS:
        group, member = device_at(step)
        at = group * 32 + member
        gather_second(second, at * 16, at)
        if before is not None:
            forward(*before)
        before = (group, member)
    gather_second(third, mine * 16, mine)
    forward(*before)

    for step in STEPS:
        copy(z_here, z_all.at[pl.ds(mine, 1)], 5, *device_at(step))
    prepare(
        mine, near[...], turn[...], wall[...], bulk[...], dens[...], inside[2, :32, :], stack,
        moves, kept,
    )
    finish(third, 127 * 16, 5)

    arrived = third.reshape(8, 16, 16, 128)
    for part in range(16):
        field[part] = pick_rows(perm[...], arrived[:, part].reshape(128, 128))

    low = lane < 64
    sign = jnp.where(low, -1.0, 1.0)
    z_in = kept[Z_IN]

    def four(which):
        return jnp.concatenate([field[4 * q + which] for q in range(4)], axis=1)

    def taken(which, axes):
        table = [
            jnp.concatenate([fixed[TAKE + 4 * (axis - 1) + q] for q in range(4)], axis=0)
            for axis in axes
        ]
        return pick_lanes(four(which), jnp.concatenate(table, axis=1))

    both = taken(0, (1, 2))
    pressures = [jnp.where(low, field[0], field[12]), both[:, :128], both[:, 128:]]
    normals = [jnp.where(low, field[1], field[13]), taken(2, (1,)), taken(3, (2,))]
    ask_rows = ask.reshape(96, 128)
    for axis in range(3):
        normal = sign * normals[axis]
        traces[3 + axis] = pressures[axis]
        traces[6 + axis] = normal
        turned = pltpu.roll(pressures[axis] + z_in * normal, 64, 1)
        traces[axis] = turned
        found = pick_rows(moves[GIVE + axis, :64], turned)
        ask_rows[pl.ds(axis, 32, stride=3), :] = jnp.where(low[:32], found[:32], found[32:])

    def three(step, number, source, target, phase):
        group, member = device_at(step)
        at = group * 32 + member if number is None else number
        copy(
            source.at[pl.ds(at * 3, 3)], target.at[pl.ds(mine * 3, 3)], phase, group, member
        )

    for number in range(31, 0, -1):
        three(NEARBY[number], number, ask, ask_in, 3)
    ask_in[pl.ds(mine * 3, 3)] = ask[pl.ds(0, 3)]

    scale = jnp.float32(-metric_scale) * kept[BULK]
    thin = jnp.float32(-metric_scale) * kept[THIN]
    derivative = gll_tables(NP - 1)[2]

    def along_x(which):
        straight = [field[4 * q + which] for q in range(4)]
        crossed = [pltpu.roll(part, 64, 1) for part in straight]
        sums = []
        for q in range(4):
            found = None
            for b in range(4):
                one = jnp.where(low, derivative[2 * q, 2 * b], derivative[2 * q + 1, 2 * b + 1])
                two = jnp.where(low, derivative[2 * q, 2 * b + 1], derivative[2 * q + 1, 2 * b])
                term = one.astype(jnp.float32) * straight[b] + two.astype(jnp.float32) * crossed[b]
                found = term if found is None else found + term
            sums.append(found)
        return sums

    finish(ask_in, 93, 7)
    asked = ask_in.reshape(384, 128)
    answer_rows = answer.reshape(384, 128)
    for axis in range(3):
        found = pick_rows(moves[ROUTE + axis], asked[pl.ds(axis, 128, stride=3), :])
        answer_rows[pl.ds(axis, 128, stride=3), :] = jnp.where(low, found[:128], found[128:])
    for step in STEPS:
        three(step, None, answer, answer_in, 4)
    answer_in[pl.ds(mine * 3, 3)] = answer[pl.ds(mine * 3, 3)]

    finish(z_all, 127, 11)
    z_table = z_all.reshape(128, 128)[...]
    lane_f = lane.astype(jnp.float32)
    for axis in range(3):
        found = pick_rows(moves[OWNER + axis], z_table)
        sides = []
        for half in range(2):
            spot = kept[SPOT + axis, :, 64 * half : 64 * half + 1]
            sides.append(
                jnp.sum(
                    jnp.where(lane_f == spot, found[128 * half : 128 * half + 128], 0.0),
                    axis=1,
                    keepdims=True,
                )
            )
        kept[SPOT + axis] = jnp.where(low, sides[0], sides[1])
        found = pick_rows(moves[NEAR + axis], traces[axis])
        traces[axis] = jnp.where(low, found[:128], found[128:])

    def stacked(which):
        return jnp.concatenate([field[4 * q + which] for q in range(4)], axis=0)

    side_x = along_x(1)
    grad_x = along_x(0)
    for q in range(4):
        total[4 * q] = side_x[q]
        total[4 * q + 1] = thin * grad_x[q]

    side_y = exact(stacked(2), inside[0])
    side_z = exact(stacked(3), inside[1])
    grad_y = exact(stacked(0), inside[0])
    grad_z = exact(stacked(0), inside[1])
    for q in range(4):
        rows = slice(128 * q, 128 * q + 128)
        total[4 * q] = scale * (total[4 * q] + side_y[rows] + side_z[rows])
        total[4 * q + 2] = thin * grad_y[rows]
        total[4 * q + 3] = thin * grad_z[rows]

    finish(answer_in, 381, 9)
    answers = answer_in.reshape(384, 128)
    coming = []
    for axis in range(3):
        found = pick_rows(moves[FAR + axis], answers[pl.ds(axis, 128, stride=3), :])
        coming.append(traces[axis] + jnp.where(low, found[:128], found[128:]))
    coming = jnp.concatenate(coming, axis=0)
    code = jnp.concatenate([kept[CODE + axis] for axis in range(3)], axis=0).astype(jnp.int32)
    coming = jnp.where(code % 2 == 1, pick_lanes(coming, fixed[TURN]), coming)
    coming = jnp.where(code // 2 % 2 == 1, pick_lanes(coming, fixed[TURN + 1]), coming)
    coming = jnp.where(code >= 4, pick_lanes(coming, fixed[TURN + 2]), coming)
    lift = jnp.float32(metric_scale / float(gll_tables(NP - 1)[1][0]))
    gains = []
    for axis in range(3):
        is_wall = kept[WALL + axis] == 1.0
        normal = traces[6 + axis]
        z_out = jnp.where(is_wall, z_in, kept[SPOT + axis])
        other = coming[128 * axis : 128 * axis + 128]
        jump = jnp.where(
            is_wall, 2.0 * z_in * normal, other - traces[3 + axis] + z_out * normal
        )
        jump = lift * jump / (z_in + z_out)
        gains.append(jnp.concatenate([kept[BULK] * jump, -sign * kept[THIN] * z_in * jump]))
    lifted = []
    for axis in (1, 2):
        wide = jnp.concatenate([fixed[LIFT + 4 * (axis - 1) + q] for q in range(4)], axis=1)
        lifted.append(pick_lanes(gains[axis], wide))
    for q in range(4):
        lanes = slice(128 * q, 128 * q + 128)
        part = total[4 * q] + lifted[0][:128, lanes] + lifted[1][:128, lanes]
        part_x = total[4 * q + 1]
        if q in (0, 3):
            keep = low if q == 0 else lane >= 64
            part = part + jnp.where(keep, gains[0][:128], 0.0)
            part_x = part_x + jnp.where(keep, gains[0][128:], 0.0)
        out_ref[pl.ds(4 * q, 128, stride=16), :] = part
        out_ref[pl.ds(4 * q + 1, 128, stride=16), :] = part_x
        out_ref[pl.ds(4 * q + 2, 128, stride=16), :] = total[4 * q + 2] + lifted[0][128:, lanes]
        out_ref[pl.ds(4 * q + 3, 128, stride=16), :] = total[4 * q + 3] + lifted[1][128:, lanes]
    finish(notes, 127, 0)
    finish(first, 32, 2)
    finish(first, 63 * 32, 14)
    finish(z_all, 127, 10)
    finish(third, 127 * 16, 4)
    finish(ask_in, 93, 6)
    finish(answer_in, 381, 8)


def write_kernel(in_ref, out_ref, rows, sems):
    parts = [pl.ds(512 * n, 512) for n in range(4)]
    for n, part in enumerate(parts):
        pltpu.make_async_copy(in_ref.at[part], rows.at[part], sems.at[n]).start()
    for n, part in enumerate(parts):
        pltpu.make_async_copy(in_ref.at[part], rows.at[part], sems.at[n]).wait()
        pltpu.make_async_copy(rows.at[part], out_ref.at[part], sems.at[4 + n]).start()
    for n, part in enumerate(parts):
        pltpu.make_async_copy(rows.at[part], out_ref.at[part], sems.at[4 + n]).wait()


def body(old_state, dest_row, neighbours, orientation, wall_flags, bulk_modulus, density):
    view = old_state.reshape(256, 4, 4, 128).transpose(0, 2, 1, 3).reshape(4096, 1, 128)
    picks, inside = fixed_tables()
    f32, i32, bf16 = jnp.float32, jnp.int32, jnp.bfloat16
    halo = pltpu.VMEM((384, 1, 128), f32)
    result = pl.pallas_call(
        exchange_kernel,
        out_shape=jax.ShapeDtypeStruct((2048, 128), f32),
        in_specs=[pl.BlockSpec(memory_space=pl.ANY)] * 9,
        out_specs=pl.BlockSpec(memory_space=pltpu.VMEM),
        scratch_shapes=[
            pltpu.VMEM((4096, 1, 128), f32),
            pltpu.VMEM((2, 128), i32),
            pltpu.VMEM((6, 128), i32),
            pltpu.VMEM((6, 128), i32),
            pltpu.VMEM((6, 128), i32),
            pltpu.VMEM((1, 128), f32),
            pltpu.VMEM((1, 128), f32),
            pltpu.VMEM((19, 128, 128), bf16),
            pltpu.VMEM((3, 128, 128), f32),
            pltpu.VMEM((2, 128), i32),
            pltpu.SMEM((2, 128), i32),
            pltpu.VMEM((128, 1, 128), i32),
            pltpu.VMEM((128, 1, 128), i32),
            pltpu.VMEM((4096, 1, 128), f32),
            pltpu.VMEM((4096, 1, 128), f32),
            pltpu.VMEM((2048, 1, 128), f32),
            pltpu.VMEM((2048, 1, 128), f32),
            pltpu.VMEM((16, 128), i32),
            pltpu.SMEM((16, 128), i32),
            pltpu.VMEM((128, 128), bf16),
            pltpu.VMEM((128, 128), f32),
            pltpu.VMEM((1, 1, 128), f32),
            pltpu.VMEM((128, 1, 128), f32),
            pltpu.VMEM((15, 256, 128), bf16),
            pltpu.VMEM((KEPT, 128, 128), f32),
            pltpu.VMEM((16, 128, 128), f32),
            pltpu.VMEM((9, 128, 128), f32),
            pltpu.VMEM((96, 1, 128), f32),
            halo,
            halo,
            halo,
            pltpu.VMEM((16, 128, 128), f32),
            pltpu.SemaphoreType.DMA((18,)),
            pltpu.SemaphoreType.DMA((11,)),
            pltpu.SemaphoreType.REGULAR,
            pltpu.SemaphoreType.REGULAR,
        ],
        compiler_params=pltpu.CompilerParams(collective_id=0, has_side_effects=True),
    )(
        view,
        dest_row.reshape(2, 128),
        neighbours,
        orientation,
        wall_flags,
        bulk_modulus[None, :],
        density[None, :],
        jnp.asarray(picks, bf16),
        jnp.asarray(inside),
    )
    result = pl.pallas_call(
        write_kernel,
        out_shape=jax.ShapeDtypeStruct((2048, 128), f32),
        in_specs=[pl.BlockSpec(memory_space=pl.ANY)],
        out_specs=pl.BlockSpec(memory_space=pl.ANY),
        scratch_shapes=[pltpu.VMEM((2048, 128), f32), pltpu.SemaphoreType.DMA((8,))],
    )(result)
    return result.reshape(128, 4, 4, 128).transpose(0, 2, 1, 3).reshape(128, 4, 512)


def solution(mesh):
    in_specs = (
        P(("grp", "dev"), None, None),
        P(("grp", "dev")),
        P(None, ("grp", "dev")),
        P(None, ("grp", "dev")),
        P(None, ("grp", "dev")),
        P(("grp", "dev")),
        P(("grp", "dev")),
    )
    out_specs = P(("grp", "dev"), None, None)
    return jax.shard_map(body, mesh=mesh, in_specs=in_specs, out_specs=out_specs, check_vma=False)
```

```python
import jax
import jax.numpy as jnp
import numpy as np
from jax import lax
from jax.experimental import pallas as pl
from jax.experimental.pallas import tpu as pltpu
from jax.sharding import PartitionSpec as P

NP = 8
MESH = pl.DeviceIdType.MESH
HIGHEST = lax.Precision.HIGHEST

metric_scale = 0.25


def gll_tables(poly_order):
    num_points = poly_order + 1
    points = -np.cos(np.pi * np.arange(num_points) / poly_order)
    legendre = np.zeros((num_points, num_points))
    for sweeps in range(101):
        legendre[:, 0] = 1.0
        legendre[:, 1] = points
        for degree in range(2, num_points):
            legendre[:, degree] = (
                (2 * degree - 1) * points * legendre[:, degree - 1]
                - (degree - 1) * legendre[:, degree - 2]
            ) / degree
        if sweeps < 100:
            points = points - (points * legendre[:, poly_order] - legendre[:, poly_order - 1]) / (
                num_points * legendre[:, poly_order]
            )
    end_values = legendre[:, poly_order]
    weights = 2.0 / (poly_order * num_points * end_values**2)
    distance = points[:, None] - points[None, :] + np.eye(num_points)
    derivative = end_values[:, None] / end_values[None, :] / distance
    derivative = derivative * (1.0 - np.eye(num_points))
    derivative[0, 0] = -poly_order * num_points / 4.0
    derivative[poly_order, poly_order] = poly_order * num_points / 4.0
    return (points, weights, derivative)


def fixed_tables():
    derivative = gll_tables(NP - 1)[2]
    take = np.zeros((2, 4, 128, 128))
    for end in range(2):
        for first in range(8):
            for second in range(8):
                face_lane = 64 * end + 8 * first + second
                half, chunk = 64 * (first % 2), first // 2
                take[0, chunk, half + 56 * end + second, face_lane] = 1.0
                take[1, chunk, half + 8 * second + 7 * end, face_lane] = 1.0
    turns = np.zeros((3, 128, 128))
    for end in range(2):
        for first in range(8):
            for second in range(8):
                to = 64 * end + 8 * first + second
                turns[0, 64 * end + 8 * (7 - first) + second, to] = 1.0
                turns[1, 64 * end + 8 * first + 7 - second, to] = 1.0
                turns[2, 64 * end + 8 * second + first, to] = 1.0
    eye2, eye8 = np.eye(2), np.eye(8)
    inside = [
        np.kron(eye2, np.kron(derivative.T, eye8)),
        np.kron(eye2, np.kron(eye8, derivative.T)),
    ]
    lift = np.swapaxes(take, 2, 3)
    stack = [take.reshape(8, 128, 128), lift.reshape(8, 128, 128), turns]
    comes_from = np.full((128, 128), -1.0)
    for number, step in enumerate(NEARBY):
        for device in range(128):
            place = device // 32, device // 8 % 4, device // 2 % 4, device % 2
            back = [(at - by) % size for at, by, size in zip(place, step, (4, 4, 4, 2))]
            comes_from[number, device] = back[0] * 32 + back[1] * 8 + back[2] * 2 + back[3]
    return np.concatenate(stack), np.stack(inside + [comes_from]).astype(np.float32)


TAKE, LIFT, TURN = 0, 8, 16
NEAR, FAR, GIVE, ROUTE, OWNER = 0, 3, 6, 9, 12
CODE, WALL, Z_IN, BULK, THIN, SPOT, KEPT = 0, 3, 6, 7, 8, 9, 12

STEPS = sorted(
    [(a, b, c, d) for a in range(4) for b in range(4) for c in range(4) for d in range(2)][1:],
    key=lambda step: -sum(min(part, 4 - part) for part in step[:3]),
)
NEARBY = [(0, 0, 0, 0)] + STEPS[::-1][:31]


def my_place():
    group = lax.axis_index("grp")
    member = lax.axis_index("dev")
    return group, member // 8, (member // 2) % 4, member % 2


def chip_at(place, step):
    z_at, y_at, x_at, _ = place
    step = step * 27 % 64
    x_to = (x_at + step) % 4
    y_to = (y_at + step // 4) % 4
    z_to = (z_at + step // 16) % 4
    return z_to, y_to * 4 + x_to


def split3(value):
    high = value.astype(jnp.bfloat16)
    rest = value - high.astype(jnp.float32)
    middle = rest.astype(jnp.bfloat16)
    low = (rest - middle.astype(jnp.float32)).astype(jnp.bfloat16)
    return high, middle, low


def pick_rows(chosen, value):
    wide = value.shape[1]
    parts = jnp.concatenate(split3(value), axis=1)
    found = jnp.dot(chosen, parts, preferred_element_type=jnp.float32)
    return found[:, :wide] + found[:, wide : 2 * wide] + found[:, 2 * wide :]


def pick_lanes(value, chosen):
    tall = value.shape[0]
    parts = jnp.concatenate(split3(value), axis=0)
    found = jnp.dot(parts, chosen, preferred_element_type=jnp.float32)
    return found[:tall] + found[tall : 2 * tall] + found[2 * tall :]


def exact(left, right):
    return jnp.dot(left, right, precision=HIGHEST, preferred_element_type=jnp.float32)


def count(left, right):
    return jnp.dot(
        left.astype(jnp.bfloat16), right.astype(jnp.bfloat16), preferred_element_type=jnp.float32
    )


def order_slots(dest_row, stack, ranks):
    lane = lax.broadcasted_iota(jnp.int32, (128, 128), 1)
    sub = lax.broadcasted_iota(jnp.int32, (128, 128), 0)
    value = dest_row.astype(jnp.float32)
    stack[0:2, :] = value
    columns = stack[...].T
    rows = [value[0:1, :], value[1:2, :]]
    slots = []
    for half in range(2):
        mine = columns[:, half : half + 1]
        below = jnp.zeros((128, 128), jnp.float32)
        for other in range(2):
            tied = rows[other] == mine
            if other > half:
                less = rows[other] < mine
            elif other < half:
                less = (rows[other] < mine) | tied
            else:
                less = (rows[other] < mine) | (tied & (lane < sub))
            below = below + jnp.where(less, 1.0, 0.0)
        slots.append((mine, jnp.sum(below, axis=1, keepdims=True)))
    lane_f = lane.astype(jnp.float32)
    sub_f = sub.astype(jnp.float32)
    for half in range(2):
        found = jnp.zeros((1, 128), jnp.float32)
        for part in range(2):
            is_it = slots[part][1] == lane_f + 128.0 * half
            found = found + jnp.sum(
                jnp.where(is_it, sub_f + 128.0 * part, 0.0), axis=0, keepdims=True
            )
        ranks[half : half + 1, :] = jnp.clip(found.astype(jnp.int32), 0, 255)
    return rows, slots


def write_notes(rows, slots, near_rows, wall_rows, mine, note_out):
    lane = lax.broadcasted_iota(jnp.int32, (128, 128), 1)
    sub = lax.broadcasted_iota(jnp.int32, (128, 128), 0)
    lane_f = lane.astype(jnp.float32)
    sub_f = sub.astype(jnp.float32)
    note = jnp.zeros((128, 128), jnp.float32)
    heads = jnp.zeros((1, 128), jnp.float32)
    for half in range(2):
        row = rows[half].astype(jnp.int32)
        owner_row = jnp.where(row >= 0, row // 128, -1)
        to = jnp.where(owner_row == sub, 1.0, 0.0)
        mine_f, rank = slots[half]
        column = mine_f.astype(jnp.int32)
        rank_i = rank.astype(jnp.int32)
        owner = jnp.where(column >= 0, column // 128, -1).astype(jnp.float32)
        inside = (column % 128 + 1).astype(jnp.float32)
        ids = jnp.where((rank_i % 8) == lane, inside, 0.0)
        note = note + count(to, ids)
        heads = heads + jnp.sum(
            jnp.where(rank_i == 8 * (lane - 32), owner, 0.0), axis=0, keepdims=True
        )
    owners = near_rows // 128
    beside = jnp.where((owners != mine) & (wall_rows == 0), owners + 1, 0).astype(jnp.float32)
    beside = jnp.max(beside, axis=1, keepdims=True)
    beside = jnp.sum(
        jnp.where(lane_f[:6] == sub_f[:6] + 8.0, beside, 0.0), axis=0, keepdims=True
    )
    heads = jnp.where((lane[:1] >= 32) & (lane[:1] < 64), heads, 0.0)
    note_out.reshape(128, 128)[...] = (note + heads + beside).astype(jnp.int32)


def prepare(
    mine, near_rows, turn_rows, wall_rows, bulk_row, dens_row, comes_from, stack, moves, kept
):
    lane = lax.broadcasted_iota(jnp.int32, (128, 128), 1)
    sub = lax.broadcasted_iota(jnp.int32, (128, 128), 0)
    away_rows = jnp.where((near_rows // 128 != mine) & (wall_rows == 0), 1.0, 0.0)
    stack[0:6, :] = near_rows.astype(jnp.float32)
    stack[8:14, :] = turn_rows.astype(jnp.float32)
    stack[16:22, :] = wall_rows.astype(jnp.float32)
    stack[24:25, :] = bulk_row
    stack[25:26, :] = dens_row
    stack[26:32, :] = away_rows
    columns = stack[...].T
    give_rank = count(stack[24:32, :], (sub < lane).astype(jnp.float32))
    base = (mine * 128).astype(jnp.float32)
    lane_f = lane.astype(jnp.float32)
    sub_f = sub.astype(jnp.float32)
    owners = near_rows // 128
    beside = jnp.where(away_rows > 0.0, owners + 1, 0).astype(jnp.float32)
    beside = jnp.max(beside, axis=1, keepdims=True) - 1.0
    for face in range(6):
        axis, half = face // 2, face % 2
        near = columns[:, face : face + 1]
        away = columns[:, 26 + face : 27 + face]
        away_row = away_rows[face : face + 1, :]
        is_near = (near - base == lane_f) & (away == 0.0)
        before = jnp.where((near_rows[face : face + 1, :].astype(jnp.float32) < near), away_row, 0.0)
        take_rank = jnp.sum(before, axis=1, keepdims=True)
        is_far = jnp.where((take_rank == lane_f) & (away > 0.0), 1.0, 0.0)
        passed_by = jnp.where(comes_from == beside[face : face + 1, :], 1.0, 0.0)
        is_given = (give_rank[2 + face : 3 + face, :] == sub_f[:32]) & (away_row > 0.0)
        rows = pl.ds(128 * half, 128)
        moves[NEAR + axis, rows] = jnp.where(is_near, 1.0, 0.0).astype(jnp.bfloat16)
        moves[FAR + axis, rows] = count(is_far[:, :32], passed_by).astype(jnp.bfloat16)
        moves[GIVE + axis, pl.ds(32 * (1 - half), 32)] = jnp.where(is_given, 1.0, 0.0).astype(
            jnp.bfloat16
        )
        near_i = near.astype(jnp.int32)
        moves[OWNER + axis, rows] = jnp.where(near_i // 128 == lane, 1.0, 0.0).astype(jnp.bfloat16)
        kept[SPOT + axis, :, 64 * half : 64 * half + 64] = jnp.broadcast_to(
            (near_i % 128).astype(jnp.float32), (128, 64)
        )
    low = lane < 64
    for axis in range(3):
        kept[CODE + axis] = jnp.where(
            low, columns[:, 8 + 2 * axis : 9 + 2 * axis], columns[:, 9 + 2 * axis : 10 + 2 * axis]
        )
        kept[WALL + axis] = jnp.where(
            low, columns[:, 16 + 2 * axis : 17 + 2 * axis], columns[:, 17 + 2 * axis : 18 + 2 * axis]
        )
    bulk = jnp.broadcast_to(columns[:, 24:25], (128, 128))
    dens = jnp.broadcast_to(columns[:, 25:26], (128, 128))
    kept[Z_IN] = jnp.sqrt(bulk * dens)
    kept[BULK] = bulk
    kept[THIN] = 1.0 / dens


def exchange_kernel(
    state_ref, dest_ref, near_ref, turn_ref, wall_ref, bulk_ref, dens_ref, fixed_ref, inside_ref,
    out_ref, state, dest, near, turn, wall, bulk, dens, fixed, inside, ranks, slot_of, note_out,
    notes, sends, first, second, third, table, index, perm, stack, z_here, z_all, moves, kept, field,
    traces, ask, ask_in, answer, answer_in, total, sems, loads, met_y, met_z,
):
    place = my_place()
    z_at, y_at, x_at, core = place
    member_here = lax.axis_index("dev")
    mine = z_at * 32 + member_here
    barrier = pltpu.get_barrier_semaphore()

    def signal(sem, group, y_to, x_to, core_to):
        pl.semaphore_signal(
            sem, inc=1, device_id=(group, (y_to * 4 + x_to) * 2 + core_to), device_id_type=MESH
        )

    for step in range(1, 8):
        signal(barrier, z_at, y_at, (x_at + step // 2) % 4, (core + step) % 2)
    for step in range(1, 4):
        signal(barrier, z_at, (y_at + step) % 4, x_at, core)
        signal(barrier, (z_at + step) % 4, y_at, x_at, core)

    pairs = [
        (dest_ref, dest), (near_ref, near), (wall_ref, wall), (turn_ref, turn),
        (bulk_ref, bulk), (dens_ref, dens), (state_ref, state), (fixed_ref, fixed),
        (inside_ref, inside),
    ]
    local = [pltpu.make_async_copy(a, b, loads.at[n]) for n, (a, b) in enumerate(pairs)]
    for one in local:
        one.start()
    stack[...] = jnp.zeros((128, 128), jnp.float32)
    local[0].wait()
    rows, slots = order_slots(dest[...], stack, ranks)
    to_slots = pltpu.make_async_copy(ranks, slot_of, loads.at[9])
    to_slots.start()
    pl.semaphore_wait(barrier, 13)
    for step in range(1, 4):
        signal(met_y, z_at, (y_at + step) % 4, x_at, core)
    local[1].wait()
    local[2].wait()
    write_notes(rows, slots, near[...], wall[...], mine, note_out)
    pl.semaphore_wait(met_y, 3)
    for step in range(1, 4):
        signal(met_z, (z_at + step) % 4, y_at, x_at, core)
    to_slots.wait()
    local[6].wait()

    def gather_first(target, base, at):
        row, chunk = at // 16, at % 16
        found = []
        for k in range(32):
            slot = slot_of[k // 16, (k % 16) * 8 + row]
            found.append(state[pl.ds(slot * 16 + chunk, 1)])
        for k in range(32):
            target[pl.ds(base + k, 1)] = found[k]

    def to_device(step):
        chip_step = jnp.where(step > 63, step - 63, step)
        side = jnp.where(step == 0, 1 - core, step // 64)
        group, chip = chip_at(place, chip_step)
        return group, chip * 2 + side

    def copy(source, target, phase, group, member):
        pltpu.make_async_remote_copy(
            src_ref=source,
            dst_ref=target,
            send_sem=sems.at[2 * phase],
            recv_sem=sems.at[2 * phase + 1],
            device_id=(group, member),
            device_id_type=MESH,
        ).start()

    def finish(buffer, rows, which):
        view = buffer.at[pl.ds(0, rows)]
        pltpu.make_async_copy(view, view, sems.at[which]).wait()

    def fetch(step):
        group, member = to_device(step)
        at = group * 32 + member
        gather_first(sends, at * 32, at)

    def spread(step, leaves):
        group, member = to_device(step)
        at = group * 32 + member
        pltpu.make_async_remote_copy(
            src_ref=sends.at[pl.ds(at * 32, 32)],
            dst_ref=first.at[pl.ds(mine * 32, 32)],
            send_sem=sems.at[leaves],
            recv_sem=sems.at[16 + member % 2],
            device_id=(group, member),
            device_id_type=MESH,
        ).start()

    def tell(group, member):
        at = group * 32 + member
        copy(note_out.at[pl.ds(at, 1)], notes.at[pl.ds(mine, 1)], 0, group, member)

    fetch(0)
    fetch(1)
    pl.semaphore_wait(met_z, 3)
    spread(0, 2)
    tell(z_at, member_here + 1 - 2 * core)

    def early(step, carry):
        fetch(step + 1)
        spread(step, 12)
        group, chip = chip_at(place, step)
        tell(group, chip * 2)
        tell(group, chip * 2 + 1)
        return carry

    lax.fori_loop(1, 64, early, 0, unroll=3)

    def late(step, carry):
        spread(step, 14)
        fetch(step + 1)
        return carry

    local[3].wait()
    local[4].wait()
    local[5].wait()
    local[8].wait()
    z_here[...] = jnp.sqrt(bulk[...] * dens[...]).reshape(1, 1, 128)
    z_all[pl.ds(mine, 1)] = z_here[...]

    ask_in[...] = jnp.zeros((384, 1, 128), jnp.float32)
    finish(first, 63 * 32, 12)
    lax.fori_loop(64, 126, late, 0, unroll=2)
    spread(126, 14)
    gather_first(first, mine * 32, mine)
    notes[pl.ds(mine, 1)] = note_out[pl.ds(mine, 1)]

    finish(notes, 127, 1)
    note = notes.reshape(128, 128)[...]
    lane = lax.broadcasted_iota(jnp.int32, (128, 128), 1)
    sub = lax.broadcasted_iota(jnp.int32, (128, 128), 0)
    lower = (lane < sub).astype(jnp.float32)
    piece = jnp.zeros((128, 128), jnp.int32)
    for k in range(32):
        piece = piece + jnp.where(note[:, 32 + k : 33 + k] == lane, k + 1, 0)
    valid = piece > 0
    rank = count(lower, valid.astype(jnp.float32)).astype(jnp.int32)
    entry = sub * 32 + piece - 1
    for j in range(16):
        chosen = jnp.sum(jnp.where(valid & (rank == j), entry, 0), axis=0, keepdims=True)
        table[j : j + 1, :] = jnp.clip(chosen, 0, 4095)
    to_index = pltpu.make_async_copy(table, index, loads.at[10])
    to_index.start()
    has = jnp.broadcast_to(note[:, 0:1] > 0, (128, 128))
    order = count(lower, has.astype(jnp.float32)).astype(jnp.int32)
    slot = jnp.where(has & (order == lane), 1.0, 0.0)[:, :16]
    rows = []
    for i in range(8):
        is_row = (note[:, i : i + 1] - 1 == lane).astype(jnp.float32)
        rows.append(
            lax.dot_general(
                slot, is_row, (((0,), (0,)), ((), ())), preferred_element_type=jnp.float32
            )
        )
    perm[...] = jnp.concatenate(rows, axis=0).T.astype(jnp.bfloat16)
    facing = note.astype(jnp.float32).T
    for face in range(6):
        to = facing[8 + face : 9 + face, :] - 1.0
        chosen = jnp.where(to == sub.astype(jnp.float32), 1.0, 0.0).astype(jnp.bfloat16)
        moves[ROUTE + face // 2, pl.ds(128 * (1 - face % 2), 128)] = chosen
    local[7].wait()
    to_index.wait()
    finish(first, 127 * 32, 16 + core)

    def gather_second(target, base, at):
        found = [first[pl.ds(index[j, at], 1)] for j in range(16)]
        for j in range(16):
            target[pl.ds(base + j, 1)] = found[j]

    def device_at(step):
        group = (z_at + step[0]) % 4
        chip = ((y_at + step[1]) % 4) * 4 + (x_at + step[2]) % 4
        return group, chip * 2 + (core + step[3]) % 2

    def forward(group, member):
        at = group * 32 + member
        copy(
            second.at[pl.ds(at * 16, 16)], third.at[pl.ds(mine * 16, 16)], 2, group, member
        )

    before = None
    for step in STEPS:
        group, member = device_at(step)
        at = group * 32 + member
        gather_second(second, at * 16, at)
        if before is not None:
            forward(*before)
        before = (group, member)
    gather_second(third, mine * 16, mine)
    forward(*before)

    for step in STEPS:
        copy(z_here, z_all.at[pl.ds(mine, 1)], 5, *device_at(step))
    prepare(
        mine, near[...], turn[...], wall[...], bulk[...], dens[...], inside[2, :32, :], stack,
        moves, kept,
    )
    finish(third, 127 * 16, 5)

    arrived = third.reshape(8, 16, 16, 128)
    for part in range(16):
        field[part] = pick_rows(perm[...], arrived[:, part].reshape(128, 128))

    low = lane < 64
    sign = jnp.where(low, -1.0, 1.0)
    z_in = kept[Z_IN]

    def four(which):
        return jnp.concatenate([field[4 * q + which] for q in range(4)], axis=1)

    def taken(which, axes):
        table = [
            jnp.concatenate([fixed[TAKE + 4 * (axis - 1) + q] for q in range(4)], axis=0)
            for axis in axes
        ]
        return pick_lanes(four(which), jnp.concatenate(table, axis=1))

    both = taken(0, (1, 2))
    pressures = [jnp.where(low, field[0], field[12]), both[:, :128], both[:, 128:]]
    normals = [jnp.where(low, field[1], field[13]), taken(2, (1,)), taken(3, (2,))]
    ask_rows = ask.reshape(96, 128)
    for axis in range(3):
        normal = sign * normals[axis]
        traces[3 + axis] = pressures[axis]
        traces[6 + axis] = normal
        turned = pltpu.roll(pressures[axis] + z_in * normal, 64, 1)
        traces[axis] = turned
        found = pick_rows(moves[GIVE + axis, :64], turned)
        ask_rows[pl.ds(axis, 32, stride=3), :] = jnp.where(low[:32], found[:32], found[32:])

    def three(step, number, source, target, phase):
        group, member = device_at(step)
        at = group * 32 + member if number is None else number
        copy(
            source.at[pl.ds(at * 3, 3)], target.at[pl.ds(mine * 3, 3)], phase, group, member
        )

    for number in range(31, 0, -1):
        three(NEARBY[number], number, ask, ask_in, 3)
    ask_in[pl.ds(mine * 3, 3)] = ask[pl.ds(0, 3)]

    scale = jnp.float32(-metric_scale) * kept[BULK]
    thin = jnp.float32(-metric_scale) * kept[THIN]
    derivative = gll_tables(NP - 1)[2]

    def along_x(which):
        straight = [field[4 * q + which] for q in range(4)]
        crossed = [pltpu.roll(part, 64, 1) for part in straight]
        sums = []
        for q in range(4):
            found = None
            for b in range(4):
                one = jnp.where(low, derivative[2 * q, 2 * b], derivative[2 * q + 1, 2 * b + 1])
                two = jnp.where(low, derivative[2 * q, 2 * b + 1], derivative[2 * q + 1, 2 * b])
                term = one.astype(jnp.float32) * straight[b] + two.astype(jnp.float32) * crossed[b]
                found = term if found is None else found + term
            sums.append(found)
        return sums

    finish(ask_in, 93, 7)
    asked = ask_in.reshape(384, 128)
    answer_rows = answer.reshape(384, 128)
    for axis in range(3):
        found = pick_rows(moves[ROUTE + axis], asked[pl.ds(axis, 128, stride=3), :])
        answer_rows[pl.ds(axis, 128, stride=3), :] = jnp.where(low, found[:128], found[128:])
    for step in STEPS:
        three(step, None, answer, answer_in, 4)
    answer_in[pl.ds(mine * 3, 3)] = answer[pl.ds(mine * 3, 3)]

    finish(z_all, 127, 11)
    z_table = z_all.reshape(128, 128)[...]
    lane_f = lane.astype(jnp.float32)
    for axis in range(3):
        found = pick_rows(moves[OWNER + axis], z_table)
        sides = []
        for half in range(2):
            spot = kept[SPOT + axis, :, 64 * half : 64 * half + 1]
            sides.append(
                jnp.sum(
                    jnp.where(lane_f == spot, found[128 * half : 128 * half + 128], 0.0),
                    axis=1,
                    keepdims=True,
                )
            )
        kept[SPOT + axis] = jnp.where(low, sides[0], sides[1])
        found = pick_rows(moves[NEAR + axis], traces[axis])
        traces[axis] = jnp.where(low, found[:128], found[128:])

    def stacked(which):
        return jnp.concatenate([field[4 * q + which] for q in range(4)], axis=0)

    side_x = along_x(1)
    grad_x = along_x(0)
    for q in range(4):
        total[4 * q] = side_x[q]
        total[4 * q + 1] = thin * grad_x[q]

    side_y = exact(stacked(2), inside[0])
    side_z = exact(stacked(3), inside[1])
    grad_y = exact(stacked(0), inside[0])
    grad_z = exact(stacked(0), inside[1])
    for q in range(4):
        rows = slice(128 * q, 128 * q + 128)
        total[4 * q] = scale * (total[4 * q] + side_y[rows] + side_z[rows])
        total[4 * q + 2] = thin * grad_y[rows]
        total[4 * q + 3] = thin * grad_z[rows]

    finish(answer_in, 381, 9)
    answers = answer_in.reshape(384, 128)
    coming = []
    for axis in range(3):
        found = pick_rows(moves[FAR + axis], answers[pl.ds(axis, 128, stride=3), :])
        coming.append(traces[axis] + jnp.where(low, found[:128], found[128:]))
    coming = jnp.concatenate(coming, axis=0)
    code = jnp.concatenate([kept[CODE + axis] for axis in range(3)], axis=0).astype(jnp.int32)
    coming = jnp.where(code % 2 == 1, pick_lanes(coming, fixed[TURN]), coming)
    coming = jnp.where(code // 2 % 2 == 1, pick_lanes(coming, fixed[TURN + 1]), coming)
    coming = jnp.where(code >= 4, pick_lanes(coming, fixed[TURN + 2]), coming)
    lift = jnp.float32(metric_scale / float(gll_tables(NP - 1)[1][0]))
    gains = []
    for axis in range(3):
        is_wall = kept[WALL + axis] == 1.0
        normal = traces[6 + axis]
        z_out = jnp.where(is_wall, z_in, kept[SPOT + axis])
        other = coming[128 * axis : 128 * axis + 128]
        jump = jnp.where(
            is_wall, 2.0 * z_in * normal, other - traces[3 + axis] + z_out * normal
        )
        jump = lift * jump / (z_in + z_out)
        gains.append(jnp.concatenate([kept[BULK] * jump, -sign * kept[THIN] * z_in * jump]))
    lifted = []
    for axis in (1, 2):
        wide = jnp.concatenate([fixed[LIFT + 4 * (axis - 1) + q] for q in range(4)], axis=1)
        lifted.append(pick_lanes(gains[axis], wide))
    for q in range(4):
        lanes = slice(128 * q, 128 * q + 128)
        part = total[4 * q] + lifted[0][:128, lanes] + lifted[1][:128, lanes]
        part_x = total[4 * q + 1]
        if q in (0, 3):
            keep = low if q == 0 else lane >= 64
            part = part + jnp.where(keep, gains[0][:128], 0.0)
            part_x = part_x + jnp.where(keep, gains[0][128:], 0.0)
        out_ref[pl.ds(4 * q, 128, stride=16), :] = part
        out_ref[pl.ds(4 * q + 1, 128, stride=16), :] = part_x
        out_ref[pl.ds(4 * q + 2, 128, stride=16), :] = total[4 * q + 2] + lifted[0][128:, lanes]
        out_ref[pl.ds(4 * q + 3, 128, stride=16), :] = total[4 * q + 3] + lifted[1][128:, lanes]
    finish(notes, 127, 0)
    finish(first, 32, 2)
    finish(first, 63 * 32, 14)
    finish(z_all, 127, 10)
    finish(third, 127 * 16, 4)
    finish(ask_in, 93, 6)
    finish(answer_in, 381, 8)


def write_kernel(in_ref, out_ref, rows, sems):
    parts = [pl.ds(512 * n, 512) for n in range(4)]
    for n, part in enumerate(parts):
        pltpu.make_async_copy(in_ref.at[part], rows.at[part], sems.at[n]).start()
    for n, part in enumerate(parts):
        pltpu.make_async_copy(in_ref.at[part], rows.at[part], sems.at[n]).wait()
        pltpu.make_async_copy(rows.at[part], out_ref.at[part], sems.at[4 + n]).start()
    for n, part in enumerate(parts):
        pltpu.make_async_copy(rows.at[part], out_ref.at[part], sems.at[4 + n]).wait()


def body(old_state, dest_row, neighbours, orientation, wall_flags, bulk_modulus, density):
    view = old_state.reshape(256, 4, 4, 128).transpose(0, 2, 1, 3).reshape(4096, 1, 128)
    picks, inside = fixed_tables()
    f32, i32, bf16 = jnp.float32, jnp.int32, jnp.bfloat16
    halo = pltpu.VMEM((384, 1, 128), f32)
    result = pl.pallas_call(
        exchange_kernel,
        out_shape=jax.ShapeDtypeStruct((2048, 128), f32),
        in_specs=[pl.BlockSpec(memory_space=pl.ANY)] * 9,
        out_specs=pl.BlockSpec(memory_space=pltpu.VMEM),
        scratch_shapes=[
            pltpu.VMEM((4096, 1, 128), f32),
            pltpu.VMEM((2, 128), i32),
            pltpu.VMEM((6, 128), i32),
            pltpu.VMEM((6, 128), i32),
            pltpu.VMEM((6, 128), i32),
            pltpu.VMEM((1, 128), f32),
            pltpu.VMEM((1, 128), f32),
            pltpu.VMEM((19, 128, 128), bf16),
            pltpu.VMEM((3, 128, 128), f32),
            pltpu.VMEM((2, 128), i32),
            pltpu.SMEM((2, 128), i32),
            pltpu.VMEM((128, 1, 128), i32),
            pltpu.VMEM((128, 1, 128), i32),
            pltpu.VMEM((4096, 1, 128), f32),
            pltpu.VMEM((4096, 1, 128), f32),
            pltpu.VMEM((2048, 1, 128), f32),
            pltpu.VMEM((2048, 1, 128), f32),
            pltpu.VMEM((16, 128), i32),
            pltpu.SMEM((16, 128), i32),
            pltpu.VMEM((128, 128), bf16),
            pltpu.VMEM((128, 128), f32),
            pltpu.VMEM((1, 1, 128), f32),
            pltpu.VMEM((128, 1, 128), f32),
            pltpu.VMEM((15, 256, 128), bf16),
            pltpu.VMEM((KEPT, 128, 128), f32),
            pltpu.VMEM((16, 128, 128), f32),
            pltpu.VMEM((9, 128, 128), f32),
            pltpu.VMEM((96, 1, 128), f32),
            halo,
            halo,
            halo,
            pltpu.VMEM((16, 128, 128), f32),
            pltpu.SemaphoreType.DMA((18,)),
            pltpu.SemaphoreType.DMA((11,)),
            pltpu.SemaphoreType.REGULAR,
            pltpu.SemaphoreType.REGULAR,
        ],
        compiler_params=pltpu.CompilerParams(collective_id=0, has_side_effects=True),
    )(
        view,
        dest_row.reshape(2, 128),
        neighbours,
        orientation,
        wall_flags,
        bulk_modulus[None, :],
        density[None, :],
        jnp.asarray(picks, bf16),
        jnp.asarray(inside),
    )
    result = pl.pallas_call(
        write_kernel,
        out_shape=jax.ShapeDtypeStruct((2048, 128), f32),
        in_specs=[pl.BlockSpec(memory_space=pl.ANY)],
        out_specs=pl.BlockSpec(memory_space=pl.ANY),
        scratch_shapes=[pltpu.VMEM((2048, 128), f32), pltpu.SemaphoreType.DMA((8,))],
    )(result)
    return result.reshape(128, 4, 4, 128).transpose(0, 2, 1, 3).reshape(128, 4, 512)


def solution(mesh):
    in_specs = (
        P(("grp", "dev"), None, None),
        P(("grp", "dev")),
        P(None, ("grp", "dev")),
        P(None, ("grp", "dev")),
        P(None, ("grp", "dev")),
        P(("grp", "dev")),
        P(("grp", "dev")),
    )
    out_specs = P(("grp", "dev"), None, None)
    return jax.shard_map(body, mesh=mesh, in_specs=in_specs, out_specs=out_specs, check_vma=False)
```

```python
import jax
import jax.numpy as jnp
import numpy as np
from jax import lax
from jax.experimental import pallas as pl
from jax.experimental.pallas import tpu as pltpu
from jax.sharding import PartitionSpec as P

NP = 8
MESH = pl.DeviceIdType.MESH
HIGHEST = lax.Precision.HIGHEST

metric_scale = 0.25


def gll_tables(poly_order):
    num_points = poly_order + 1
    points = -np.cos(np.pi * np.arange(num_points) / poly_order)
    legendre = np.zeros((num_points, num_points))
    for sweeps in range(101):
        legendre[:, 0] = 1.0
        legendre[:, 1] = points
        for degree in range(2, num_points):
            legendre[:, degree] = (
                (2 * degree - 1) * points * legendre[:, degree - 1]
                - (degree - 1) * legendre[:, degree - 2]
            ) / degree
        if sweeps < 100:
            points = points - (points * legendre[:, poly_order] - legendre[:, poly_order - 1]) / (
                num_points * legendre[:, poly_order]
            )
    end_values = legendre[:, poly_order]
    weights = 2.0 / (poly_order * num_points * end_values**2)
    distance = points[:, None] - points[None, :] + np.eye(num_points)
    derivative = end_values[:, None] / end_values[None, :] / distance
    derivative = derivative * (1.0 - np.eye(num_points))
    derivative[0, 0] = -poly_order * num_points / 4.0
    derivative[poly_order, poly_order] = poly_order * num_points / 4.0
    return (points, weights, derivative)


def fixed_tables():
    derivative = gll_tables(NP - 1)[2]
    take = np.zeros((2, 4, 128, 128))
    for end in range(2):
        for first in range(8):
            for second in range(8):
                face_lane = 64 * end + 8 * first + second
                half, chunk = 64 * (first % 2), first // 2
                take[0, chunk, half + 56 * end + second, face_lane] = 1.0
                take[1, chunk, half + 8 * second + 7 * end, face_lane] = 1.0
    turns = np.zeros((3, 128, 128))
    for end in range(2):
        for first in range(8):
            for second in range(8):
                to = 64 * end + 8 * first + second
                turns[0, 64 * end + 8 * (7 - first) + second, to] = 1.0
                turns[1, 64 * end + 8 * first + 7 - second, to] = 1.0
                turns[2, 64 * end + 8 * second + first, to] = 1.0
    eye2, eye8 = np.eye(2), np.eye(8)
    inside = [
        np.kron(eye2, np.kron(derivative.T, eye8)),
        np.kron(eye2, np.kron(eye8, derivative.T)),
    ]
    lift = np.swapaxes(take, 2, 3)
    stack = [take.reshape(8, 128, 128), lift.reshape(8, 128, 128), turns]
    comes_from = np.full((128, 128), -1.0)
    for number, step in enumerate(NEARBY):
        for device in range(128):
            place = device // 32, device // 8 % 4, device // 2 % 4, device % 2
            back = [(at - by) % size for at, by, size in zip(place, step, (4, 4, 4, 2))]
            comes_from[number, device] = back[0] * 32 + back[1] * 8 + back[2] * 2 + back[3]
    return np.concatenate(stack), np.stack(inside + [comes_from]).astype(np.float32)


TAKE, LIFT, TURN = 0, 8, 16
NEAR, FAR, GIVE, ROUTE, OWNER = 0, 3, 6, 9, 12
CODE, WALL, Z_IN, BULK, THIN, SPOT, KEPT = 0, 3, 6, 7, 8, 9, 12

STEPS = sorted(
    [(a, b, c, d) for a in range(4) for b in range(4) for c in range(4) for d in range(2)][1:],
    key=lambda step: -sum(min(part, 4 - part) for part in step[:3]),
)
NEARBY = [(0, 0, 0, 0)] + STEPS[::-1][:31]


def my_place():
    group = lax.axis_index("grp")
    member = lax.axis_index("dev")
    return group, member // 8, (member // 2) % 4, member % 2


def chip_at(place, step):
    z_at, y_at, x_at, _ = place
    step = step * 27 % 64
    x_to = (x_at + step) % 4
    y_to = (y_at + step // 4) % 4
    z_to = (z_at + step // 16) % 4
    return z_to, y_to * 4 + x_to


def split3(value):
    high = value.astype(jnp.bfloat16)
    rest = value - high.astype(jnp.float32)
    middle = rest.astype(jnp.bfloat16)
    low = (rest - middle.astype(jnp.float32)).astype(jnp.bfloat16)
    return high, middle, low


def pick_rows(chosen, value):
    wide = value.shape[1]
    parts = jnp.concatenate(split3(value), axis=1)
    found = jnp.dot(chosen, parts, preferred_element_type=jnp.float32)
    return found[:, :wide] + found[:, wide : 2 * wide] + found[:, 2 * wide :]


def pick_lanes(value, chosen):
    tall = value.shape[0]
    parts = jnp.concatenate(split3(value), axis=0)
    found = jnp.dot(parts, chosen, preferred_element_type=jnp.float32)
    return found[:tall] + found[tall : 2 * tall] + found[2 * tall :]


def exact(left, right):
    return jnp.dot(left, right, precision=HIGHEST, preferred_element_type=jnp.float32)


def count(left, right):
    return jnp.dot(
        left.astype(jnp.bfloat16), right.astype(jnp.bfloat16), preferred_element_type=jnp.float32
    )


def order_slots(dest_row, stack, ranks):
    lane = lax.broadcasted_iota(jnp.int32, (128, 128), 1)
    sub = lax.broadcasted_iota(jnp.int32, (128, 128), 0)
    value = dest_row.astype(jnp.float32)
    stack[0:2, :] = value
    columns = stack[...].T
    rows = [value[0:1, :], value[1:2, :]]
    slots = []
    for half in range(2):
        mine = columns[:, half : half + 1]
        below = jnp.zeros((128, 128), jnp.float32)
        for other in range(2):
            tied = rows[other] == mine
            if other > half:
                less = rows[other] < mine
            elif other < half:
                less = (rows[other] < mine) | tied
            else:
                less = (rows[other] < mine) | (tied & (lane < sub))
            below = below + jnp.where(less, 1.0, 0.0)
        slots.append((mine, jnp.sum(below, axis=1, keepdims=True)))
    lane_f = lane.astype(jnp.float32)
    sub_f = sub.astype(jnp.float32)
    for half in range(2):
        found = jnp.zeros((1, 128), jnp.float32)
        for part in range(2):
            is_it = slots[part][1] == lane_f + 128.0 * half
            found = found + jnp.sum(
                jnp.where(is_it, sub_f + 128.0 * part, 0.0), axis=0, keepdims=True
            )
        ranks[half : half + 1, :] = jnp.clip(found.astype(jnp.int32), 0, 255)
    return rows, slots


def write_notes(rows, slots, near_rows, wall_rows, mine, note_out):
    lane = lax.broadcasted_iota(jnp.int32, (128, 128), 1)
    sub = lax.broadcasted_iota(jnp.int32, (128, 128), 0)
    lane_f = lane.astype(jnp.float32)
    sub_f = sub.astype(jnp.float32)
    note = jnp.zeros((128, 128), jnp.float32)
    heads = jnp.zeros((1, 128), jnp.float32)
    for half in range(2):
        row = rows[half].astype(jnp.int32)
        owner_row = jnp.where(row >= 0, row // 128, -1)
        to = jnp.where(owner_row == sub, 1.0, 0.0)
        mine_f, rank = slots[half]
        column = mine_f.astype(jnp.int32)
        rank_i = rank.astype(jnp.int32)
        owner = jnp.where(column >= 0, column // 128, -1).astype(jnp.float32)
        inside = (column % 128 + 1).astype(jnp.float32)
        ids = jnp.where((rank_i % 8) == lane, inside, 0.0)
        note = note + count(to, ids)
        heads = heads + jnp.sum(
            jnp.where(rank_i == 8 * (lane - 32), owner, 0.0), axis=0, keepdims=True
        )
    owners = near_rows // 128
    beside = jnp.where((owners != mine) & (wall_rows == 0), owners + 1, 0).astype(jnp.float32)
    beside = jnp.max(beside, axis=1, keepdims=True)
    beside = jnp.sum(
        jnp.where(lane_f[:6] == sub_f[:6] + 8.0, beside, 0.0), axis=0, keepdims=True
    )
    heads = jnp.where((lane[:1] >= 32) & (lane[:1] < 64), heads, 0.0)
    note_out.reshape(128, 128)[...] = (note + heads + beside).astype(jnp.int32)


def prepare(
    mine, near_rows, turn_rows, wall_rows, bulk_row, dens_row, comes_from, stack, moves, kept
):
    lane = lax.broadcasted_iota(jnp.int32, (128, 128), 1)
    sub = lax.broadcasted_iota(jnp.int32, (128, 128), 0)
    away_rows = jnp.where((near_rows // 128 != mine) & (wall_rows == 0), 1.0, 0.0)
    stack[0:6, :] = near_rows.astype(jnp.float32)
    stack[8:14, :] = turn_rows.astype(jnp.float32)
    stack[16:22, :] = wall_rows.astype(jnp.float32)
    stack[24:25, :] = bulk_row
    stack[25:26, :] = dens_row
    stack[26:32, :] = away_rows
    columns = stack[...].T
    give_rank = count(stack[24:32, :], (sub < lane).astype(jnp.float32))
    base = (mine * 128).astype(jnp.float32)
    lane_f = lane.astype(jnp.float32)
    sub_f = sub.astype(jnp.float32)
    owners = near_rows // 128
    beside = jnp.where(away_rows > 0.0, owners + 1, 0).astype(jnp.float32)
    beside = jnp.max(beside, axis=1, keepdims=True) - 1.0
    for face in range(6):
        axis, half = face // 2, face % 2
        near = columns[:, face : face + 1]
        away = columns[:, 26 + face : 27 + face]
        away_row = away_rows[face : face + 1, :]
        is_near = (near - base == lane_f) & (away == 0.0)
        before = jnp.where((near_rows[face : face + 1, :].astype(jnp.float32) < near), away_row, 0.0)
        take_rank = jnp.sum(before, axis=1, keepdims=True)
        is_far = jnp.where((take_rank == lane_f) & (away > 0.0), 1.0, 0.0)
        passed_by = jnp.where(comes_from == beside[face : face + 1, :], 1.0, 0.0)
        is_given = (give_rank[2 + face : 3 + face, :] == sub_f[:32]) & (away_row > 0.0)
        rows = pl.ds(128 * half, 128)
        moves[NEAR + axis, rows] = jnp.where(is_near, 1.0, 0.0).astype(jnp.bfloat16)
        moves[FAR + axis, rows] = count(is_far[:, :32], passed_by).astype(jnp.bfloat16)
        moves[GIVE + axis, pl.ds(32 * (1 - half), 32)] = jnp.where(is_given, 1.0, 0.0).astype(
            jnp.bfloat16
        )
        near_i = near.astype(jnp.int32)
        moves[OWNER + axis, rows] = jnp.where(near_i // 128 == lane, 1.0, 0.0).astype(jnp.bfloat16)
        kept[SPOT + axis, :, 64 * half : 64 * half + 64] = jnp.broadcast_to(
            (near_i % 128).astype(jnp.float32), (128, 64)
        )
    low = lane < 64
    for axis in range(3):
        kept[CODE + axis] = jnp.where(
            low, columns[:, 8 + 2 * axis : 9 + 2 * axis], columns[:, 9 + 2 * axis : 10 + 2 * axis]
        )
        kept[WALL + axis] = jnp.where(
            low, columns[:, 16 + 2 * axis : 17 + 2 * axis], columns[:, 17 + 2 * axis : 18 + 2 * axis]
        )
    bulk = jnp.broadcast_to(columns[:, 24:25], (128, 128))
    dens = jnp.broadcast_to(columns[:, 25:26], (128, 128))
    kept[Z_IN] = jnp.sqrt(bulk * dens)
    kept[BULK] = bulk
    kept[THIN] = 1.0 / dens


def exchange_kernel(
    state_ref, dest_ref, near_ref, turn_ref, wall_ref, bulk_ref, dens_ref, fixed_ref, inside_ref,
    out_ref, state, dest, near, turn, wall, bulk, dens, fixed, inside, ranks, slot_of, note_out,
    notes, sends, first, second, third, table, index, perm, stack, z_here, z_all, moves, kept, field,
    traces, ask, ask_in, answer, answer_in, total, sems, loads, met_y, met_z,
):
    place = my_place()
    z_at, y_at, x_at, core = place
    member_here = lax.axis_index("dev")
    mine = z_at * 32 + member_here
    barrier = pltpu.get_barrier_semaphore()

    def signal(sem, group, y_to, x_to, core_to):
        pl.semaphore_signal(
            sem, inc=1, device_id=(group, (y_to * 4 + x_to) * 2 + core_to), device_id_type=MESH
        )

    for step in range(1, 8):
        signal(barrier, z_at, y_at, (x_at + step // 2) % 4, (core + step) % 2)
    for step in range(1, 4):
        signal(barrier, z_at, (y_at + step) % 4, x_at, core)
        signal(barrier, (z_at + step) % 4, y_at, x_at, core)

    pairs = [
        (dest_ref, dest), (near_ref, near), (wall_ref, wall), (turn_ref, turn),
        (bulk_ref, bulk), (dens_ref, dens), (state_ref, state), (fixed_ref, fixed),
        (inside_ref, inside),
    ]
    local = [pltpu.make_async_copy(a, b, loads.at[n]) for n, (a, b) in enumerate(pairs)]
    for one in local:
        one.start()
    stack[...] = jnp.zeros((128, 128), jnp.float32)
    local[0].wait()
    rows, slots = order_slots(dest[...], stack, ranks)
    to_slots = pltpu.make_async_copy(ranks, slot_of, loads.at[9])
    to_slots.start()
    pl.semaphore_wait(barrier, 13)
    for step in range(1, 4):
        signal(met_y, z_at, (y_at + step) % 4, x_at, core)
    local[1].wait()
    local[2].wait()
    write_notes(rows, slots, near[...], wall[...], mine, note_out)
    pl.semaphore_wait(met_y, 3)
    for step in range(1, 4):
        signal(met_z, (z_at + step) % 4, y_at, x_at, core)
    to_slots.wait()
    local[6].wait()

    def gather_first(target, base, at):
        row, chunk = at // 16, at % 16
        found = []
        for k in range(32):
            slot = slot_of[k // 16, (k % 16) * 8 + row]
            found.append(state[pl.ds(slot * 16 + chunk, 1)])
        for k in range(32):
            target[pl.ds(base + k, 1)] = found[k]

    def to_device(step):
        chip_step = jnp.where(step > 63, step - 63, step)
        side = jnp.where(step == 0, 1 - core, step // 64)
        group, chip = chip_at(place, chip_step)
        return group, chip * 2 + side

    def copy(source, target, phase, group, member):
        pltpu.make_async_remote_copy(
            src_ref=source,
            dst_ref=target,
            send_sem=sems.at[2 * phase],
            recv_sem=sems.at[2 * phase + 1],
            device_id=(group, member),
            device_id_type=MESH,
        ).start()

    def finish(buffer, rows, which):
        view = buffer.at[pl.ds(0, rows)]
        pltpu.make_async_copy(view, view, sems.at[which]).wait()

    def fetch(step):
        group, member = to_device(step)
        at = group * 32 + member
        gather_first(sends, at * 32, at)

    def spread(step, leaves):
        group, member = to_device(step)
        at = group * 32 + member
        pltpu.make_async_remote_copy(
            src_ref=sends.at[pl.ds(at * 32, 32)],
            dst_ref=first.at[pl.ds(mine * 32, 32)],
            send_sem=sems.at[leaves],
            recv_sem=sems.at[16 + member % 2],
            device_id=(group, member),
            device_id_type=MESH,
        ).start()

    def tell(group, member):
        at = group * 32 + member
        copy(note_out.at[pl.ds(at, 1)], notes.at[pl.ds(mine, 1)], 0, group, member)

    fetch(0)
    fetch(1)
    pl.semaphore_wait(met_z, 3)
    spread(0, 2)
    tell(z_at, member_here + 1 - 2 * core)

    def early(step, carry):
        fetch(step + 1)
        spread(step, 12)
        group, chip = chip_at(place, step)
        tell(group, chip * 2)
        tell(group, chip * 2 + 1)
        return carry

    lax.fori_loop(1, 64, early, 0, unroll=3)

    def late(step, carry):
        spread(step, 14)
        fetch(step + 1)
        return carry

    local[3].wait()
    local[4].wait()
    local[5].wait()
    local[8].wait()
    z_here[...] = jnp.sqrt(bulk[...] * dens[...]).reshape(1, 1, 128)
    z_all[pl.ds(mine, 1)] = z_here[...]

    ask_in[...] = jnp.zeros((384, 1, 128), jnp.float32)
    finish(first, 63 * 32, 12)
    lax.fori_loop(64, 126, late, 0, unroll=2)
    spread(126, 14)
    gather_first(first, mine * 32, mine)
    notes[pl.ds(mine, 1)] = note_out[pl.ds(mine, 1)]

    finish(notes, 127, 1)
    note = notes.reshape(128, 128)[...]
    lane = lax.broadcasted_iota(jnp.int32, (128, 128), 1)
    sub = lax.broadcasted_iota(jnp.int32, (128, 128), 0)
    lower = (lane < sub).astype(jnp.float32)
    piece = jnp.zeros((128, 128), jnp.int32)
    for k in range(32):
        piece = piece + jnp.where(note[:, 32 + k : 33 + k] == lane, k + 1, 0)
    valid = piece > 0
    rank = count(lower, valid.astype(jnp.float32)).astype(jnp.int32)
    entry = sub * 32 + piece - 1
    for j in range(16):
        chosen = jnp.sum(jnp.where(valid & (rank == j), entry, 0), axis=0, keepdims=True)
        table[j : j + 1, :] = jnp.clip(chosen, 0, 4095)
    to_index = pltpu.make_async_copy(table, index, loads.at[10])
    to_index.start()
    has = jnp.broadcast_to(note[:, 0:1] > 0, (128, 128))
    order = count(lower, has.astype(jnp.float32)).astype(jnp.int32)
    slot = jnp.where(has & (order == lane), 1.0, 0.0)[:, :16]
    rows = []
    for i in range(8):
        is_row = (note[:, i : i + 1] - 1 == lane).astype(jnp.float32)
        rows.append(
            lax.dot_general(
                slot, is_row, (((0,), (0,)), ((), ())), preferred_element_type=jnp.float32
            )
        )
    perm[...] = jnp.concatenate(rows, axis=0).T.astype(jnp.bfloat16)
    facing = note.astype(jnp.float32).T
    for face in range(6):
        to = facing[8 + face : 9 + face, :] - 1.0
        chosen = jnp.where(to == sub.astype(jnp.float32), 1.0, 0.0).astype(jnp.bfloat16)
        moves[ROUTE + face // 2, pl.ds(128 * (1 - face % 2), 128)] = chosen
    local[7].wait()
    to_index.wait()
    finish(first, 127 * 32, 16 + core)

    def gather_second(target, base, at):
        found = [first[pl.ds(index[j, at], 1)] for j in range(16)]
        for j in range(16):
            target[pl.ds(base + j, 1)] = found[j]

    def device_at(step):
        group = (z_at + step[0]) % 4
        chip = ((y_at + step[1]) % 4) * 4 + (x_at + step[2]) % 4
        return group, chip * 2 + (core + step[3]) % 2

    def forward(group, member):
        at = group * 32 + member
        copy(
            second.at[pl.ds(at * 16, 16)], third.at[pl.ds(mine * 16, 16)], 2, group, member
        )

    before = None
    for step in STEPS:
        group, member = device_at(step)
        at = group * 32 + member
        gather_second(second, at * 16, at)
        if before is not None:
            forward(*before)
        before = (group, member)
    gather_second(third, mine * 16, mine)
    forward(*before)

    for step in STEPS:
        copy(z_here, z_all.at[pl.ds(mine, 1)], 5, *device_at(step))
    prepare(
        mine, near[...], turn[...], wall[...], bulk[...], dens[...], inside[2, :32, :], stack,
        moves, kept,
    )
    finish(third, 127 * 16, 5)

    arrived = third.reshape(8, 16, 16, 128)
    for part in range(16):
        field[part] = pick_rows(perm[...], arrived[:, part].reshape(128, 128))

    low = lane < 64
    sign = jnp.where(low, -1.0, 1.0)
    z_in = kept[Z_IN]

    def four(which):
        return jnp.concatenate([field[4 * q + which] for q in range(4)], axis=1)

    def taken(which, axes):
        table = [
            jnp.concatenate([fixed[TAKE + 4 * (axis - 1) + q] for q in range(4)], axis=0)
            for axis in axes
        ]
        return pick_lanes(four(which), jnp.concatenate(table, axis=1))

    both = taken(0, (1, 2))
    pressures = [jnp.where(low, field[0], field[12]), both[:, :128], both[:, 128:]]
    normals = [jnp.where(low, field[1], field[13]), taken(2, (1,)), taken(3, (2,))]
    ask_rows = ask.reshape(96, 128)
    for axis in range(3):
        normal = sign * normals[axis]
        traces[3 + axis] = pressures[axis]
        traces[6 + axis] = normal
        turned = pltpu.roll(pressures[axis] + z_in * normal, 64, 1)
        traces[axis] = turned
        found = pick_rows(moves[GIVE + axis, :64], turned)
        ask_rows[pl.ds(axis, 32, stride=3), :] = jnp.where(low[:32], found[:32], found[32:])

    def three(step, number, source, target, phase):
        group, member = device_at(step)
        at = group * 32 + member if number is None else number
        copy(
            source.at[pl.ds(at * 3, 3)], target.at[pl.ds(mine * 3, 3)], phase, group, member
        )

    for number in range(31, 0, -1):
        three(NEARBY[number], number, ask, ask_in, 3)
    ask_in[pl.ds(mine * 3, 3)] = ask[pl.ds(0, 3)]

    scale = jnp.float32(-metric_scale) * kept[BULK]
    thin = jnp.float32(-metric_scale) * kept[THIN]
    derivative = gll_tables(NP - 1)[2]

    def along_x(which):
        straight = [field[4 * q + which] for q in range(4)]
        crossed = [pltpu.roll(part, 64, 1) for part in straight]
        sums = []
        for q in range(4):
            found = None
            for b in range(4):
                one = jnp.where(low, derivative[2 * q, 2 * b], derivative[2 * q + 1, 2 * b + 1])
                two = jnp.where(low, derivative[2 * q, 2 * b + 1], derivative[2 * q + 1, 2 * b])
                term = one.astype(jnp.float32) * straight[b] + two.astype(jnp.float32) * crossed[b]
                found = term if found is None else found + term
            sums.append(found)
        return sums

    finish(ask_in, 93, 7)
    asked = ask_in.reshape(384, 128)
    answer_rows = answer.reshape(384, 128)
    for axis in range(3):
        found = pick_rows(moves[ROUTE + axis], asked[pl.ds(axis, 128, stride=3), :])
        answer_rows[pl.ds(axis, 128, stride=3), :] = jnp.where(low, found[:128], found[128:])
    for step in STEPS:
        three(step, None, answer, answer_in, 4)
    answer_in[pl.ds(mine * 3, 3)] = answer[pl.ds(mine * 3, 3)]

    finish(z_all, 127, 11)
    z_table = z_all.reshape(128, 128)[...]
    lane_f = lane.astype(jnp.float32)
    for axis in range(3):
        found = pick_rows(moves[OWNER + axis], z_table)
        sides = []
        for half in range(2):
            spot = kept[SPOT + axis, :, 64 * half : 64 * half + 1]
            sides.append(
                jnp.sum(
                    jnp.where(lane_f == spot, found[128 * half : 128 * half + 128], 0.0),
                    axis=1,
                    keepdims=True,
                )
            )
        kept[SPOT + axis] = jnp.where(low, sides[0], sides[1])
        found = pick_rows(moves[NEAR + axis], traces[axis])
        traces[axis] = jnp.where(low, found[:128], found[128:])

    def stacked(which):
        return jnp.concatenate([field[4 * q + which] for q in range(4)], axis=0)

    side_x = along_x(1)
    grad_x = along_x(0)
    for q in range(4):
        total[4 * q] = side_x[q]
        total[4 * q + 1] = thin * grad_x[q]

    side_y = exact(stacked(2), inside[0])
    side_z = exact(stacked(3), inside[1])
    grad_y = exact(stacked(0), inside[0])
    grad_z = exact(stacked(0), inside[1])
    for q in range(4):
        rows = slice(128 * q, 128 * q + 128)
        total[4 * q] = scale * (total[4 * q] + side_y[rows] + side_z[rows])
        total[4 * q + 2] = thin * grad_y[rows]
        total[4 * q + 3] = thin * grad_z[rows]

    finish(answer_in, 381, 9)
    answers = answer_in.reshape(384, 128)
    coming = []
    for axis in range(3):
        found = pick_rows(moves[FAR + axis], answers[pl.ds(axis, 128, stride=3), :])
        coming.append(traces[axis] + jnp.where(low, found[:128], found[128:]))
    parts = jnp.concatenate(
        [part.astype(jnp.float32) for part in split3(jnp.concatenate(coming, axis=0))], axis=0
    )
    code = jnp.concatenate([kept[CODE + axis] for axis in range(3)] * 3, axis=0).astype(jnp.int32)
    for number, turns in enumerate((code % 2 == 1, code // 2 % 2 == 1, code >= 4)):
        found = jnp.dot(
            parts.astype(jnp.bfloat16), fixed[TURN + number], preferred_element_type=jnp.float32
        )
        parts = jnp.where(turns, found, parts)
    coming = parts[:384] + parts[384:768] + parts[768:]
    lift = jnp.float32(metric_scale / float(gll_tables(NP - 1)[1][0]))
    gains = []
    for axis in range(3):
        is_wall = kept[WALL + axis] == 1.0
        normal = traces[6 + axis]
        z_out = jnp.where(is_wall, z_in, kept[SPOT + axis])
        other = coming[128 * axis : 128 * axis + 128]
        jump = jnp.where(
            is_wall, 2.0 * z_in * normal, other - traces[3 + axis] + z_out * normal
        )
        jump = lift * jump / (z_in + z_out)
        gains.append(jnp.concatenate([kept[BULK] * jump, -sign * kept[THIN] * z_in * jump]))
    lifted = []
    for axis in (1, 2):
        wide = jnp.concatenate([fixed[LIFT + 4 * (axis - 1) + q] for q in range(4)], axis=1)
        lifted.append(pick_lanes(gains[axis], wide))
    for q in range(4):
        lanes = slice(128 * q, 128 * q + 128)
        part = total[4 * q] + lifted[0][:128, lanes] + lifted[1][:128, lanes]
        part_x = total[4 * q + 1]
        if q in (0, 3):
            keep = low if q == 0 else lane >= 64
            part = part + jnp.where(keep, gains[0][:128], 0.0)
            part_x = part_x + jnp.where(keep, gains[0][128:], 0.0)
        out_ref[pl.ds(4 * q, 128, stride=16), :] = part
        out_ref[pl.ds(4 * q + 1, 128, stride=16), :] = part_x
        out_ref[pl.ds(4 * q + 2, 128, stride=16), :] = total[4 * q + 2] + lifted[0][128:, lanes]
        out_ref[pl.ds(4 * q + 3, 128, stride=16), :] = total[4 * q + 3] + lifted[1][128:, lanes]
    finish(notes, 127, 0)
    finish(first, 32, 2)
    finish(first, 63 * 32, 14)
    finish(z_all, 127, 10)
    finish(third, 127 * 16, 4)
    finish(ask_in, 93, 6)
    finish(answer_in, 381, 8)


def write_kernel(in_ref, out_ref, rows, sems):
    parts = [pl.ds(512 * n, 512) for n in range(4)]
    for n, part in enumerate(parts):
        pltpu.make_async_copy(in_ref.at[part], rows.at[part], sems.at[n]).start()
    for n, part in enumerate(parts):
        pltpu.make_async_copy(in_ref.at[part], rows.at[part], sems.at[n]).wait()
        pltpu.make_async_copy(rows.at[part], out_ref.at[part], sems.at[4 + n]).start()
    for n, part in enumerate(parts):
        pltpu.make_async_copy(rows.at[part], out_ref.at[part], sems.at[4 + n]).wait()


def body(old_state, dest_row, neighbours, orientation, wall_flags, bulk_modulus, density):
    view = old_state.reshape(256, 4, 4, 128).transpose(0, 2, 1, 3).reshape(4096, 1, 128)
    picks, inside = fixed_tables()
    f32, i32, bf16 = jnp.float32, jnp.int32, jnp.bfloat16
    halo = pltpu.VMEM((384, 1, 128), f32)
    result = pl.pallas_call(
        exchange_kernel,
        out_shape=jax.ShapeDtypeStruct((2048, 128), f32),
        in_specs=[pl.BlockSpec(memory_space=pl.ANY)] * 9,
        out_specs=pl.BlockSpec(memory_space=pltpu.VMEM),
        scratch_shapes=[
            pltpu.VMEM((4096, 1, 128), f32),
            pltpu.VMEM((2, 128), i32),
            pltpu.VMEM((6, 128), i32),
            pltpu.VMEM((6, 128), i32),
            pltpu.VMEM((6, 128), i32),
            pltpu.VMEM((1, 128), f32),
            pltpu.VMEM((1, 128), f32),
            pltpu.VMEM((19, 128, 128), bf16),
            pltpu.VMEM((3, 128, 128), f32),
            pltpu.VMEM((2, 128), i32),
            pltpu.SMEM((2, 128), i32),
            pltpu.VMEM((128, 1, 128), i32),
            pltpu.VMEM((128, 1, 128), i32),
            pltpu.VMEM((4096, 1, 128), f32),
            pltpu.VMEM((4096, 1, 128), f32),
            pltpu.VMEM((2048, 1, 128), f32),
            pltpu.VMEM((2048, 1, 128), f32),
            pltpu.VMEM((16, 128), i32),
            pltpu.SMEM((16, 128), i32),
            pltpu.VMEM((128, 128), bf16),
            pltpu.VMEM((128, 128), f32),
            pltpu.VMEM((1, 1, 128), f32),
            pltpu.VMEM((128, 1, 128), f32),
            pltpu.VMEM((15, 256, 128), bf16),
            pltpu.VMEM((KEPT, 128, 128), f32),
            pltpu.VMEM((16, 128, 128), f32),
            pltpu.VMEM((9, 128, 128), f32),
            pltpu.VMEM((96, 1, 128), f32),
            halo,
            halo,
            halo,
            pltpu.VMEM((16, 128, 128), f32),
            pltpu.SemaphoreType.DMA((18,)),
            pltpu.SemaphoreType.DMA((11,)),
            pltpu.SemaphoreType.REGULAR,
            pltpu.SemaphoreType.REGULAR,
        ],
        compiler_params=pltpu.CompilerParams(collective_id=0, has_side_effects=True),
    )(
        view,
        dest_row.reshape(2, 128),
        neighbours,
        orientation,
        wall_flags,
        bulk_modulus[None, :],
        density[None, :],
        jnp.asarray(picks, bf16),
        jnp.asarray(inside),
    )
    result = pl.pallas_call(
        write_kernel,
        out_shape=jax.ShapeDtypeStruct((2048, 128), f32),
        in_specs=[pl.BlockSpec(memory_space=pl.ANY)],
        out_specs=pl.BlockSpec(memory_space=pl.ANY),
        scratch_shapes=[pltpu.VMEM((2048, 128), f32), pltpu.SemaphoreType.DMA((8,))],
    )(result)
    return result.reshape(128, 4, 4, 128).transpose(0, 2, 1, 3).reshape(128, 4, 512)


def solution(mesh):
    in_specs = (
        P(("grp", "dev"), None, None),
        P(("grp", "dev")),
        P(None, ("grp", "dev")),
        P(None, ("grp", "dev")),
        P(None, ("grp", "dev")),
        P(("grp", "dev")),
        P(("grp", "dev")),
    )
    out_specs = P(("grp", "dev"), None, None)
    return jax.shard_map(body, mesh=mesh, in_specs=in_specs, out_specs=out_specs, check_vma=False)
```
